128 devices in a mesh: dep: 8 (over x_lo, z), res: 16 (over y, x_hi, core).
Axes of the slice: x: 4 (x_hi: 2, x_lo: 2; x = x_hi * 2 + x_lo), y: 4, z: 4, core: 2. Of those that a mesh axis runs over, the one named last changes fastest.
Arguments:
- homolog_representation: bfloat16 [512, 512, 256], P('dep', 'res'), may hold values from -6 to 6
- presence_indicator: int32 [512, 512], P('dep', 'res'), may hold values from 0 to 1, as said below
- pairwise_delta_sensitivity: bfloat16 [512, 512, 128], P('res', 'dep'), may hold values from -192 to 192
- upstream_sensitivity: bfloat16 [512, 512, 256], P('dep', 'res'), may hold values from -6 to 6
- asking_matrix: bfloat16 [256, 256], replicated, may hold values from -8.25 to 8.25
- lookup_matrix: bfloat16 [256, 256], replicated, may hold values from -0.25 to 0.25
- content_matrix: bfloat16 [256, 256], replicated, may hold values from -0.375 to 0.375
- sigmoid_matrix: bfloat16 [256, 256], replicated, may hold values from -0.375 to 0.375
- emission_matrix: bfloat16 [256, 256], replicated, may hold values from -0.375 to 0.375
- lhs_projection_matrix: bfloat16 [256, 32], replicated, may hold values from -0.375 to 0.375
- rhs_projection_matrix: bfloat16 [256, 32], replicated, may hold values from -0.375 to 0.375
- pairwise_projection_matrix: bfloat16 [1024, 128], replicated, may hold values from -0.1875 to 0.1875
Outputs:
- alignment_gradient: bfloat16 [512, 512, 256], P('dep', 'res')
- intermediate_sensitivity: bfloat16 [512, 512, 256], P('dep', 'res')
The draws below stay inside these ranges and needn't reach their ends.
Inputs may be any that keep to these rules, and one draw needn't show every extreme that they name: `presence_indicator`: every residue of sequence 0 is present.
All inputs are finite; a program needn't handle non-finite values.
Results may differ from the reference program's by a relative error of at most 0.018.
The reference program's roundings to bfloat16 on the way count: a program that leaves them out, or rounds other values in their place, can miss the bound.
Values may be sent and summed in bfloat16 or wider, within the bound.
A program may use at most 320 MiB of HBM per device.

```python
import math
import jax
import jax.numpy as jnp
from jax import lax

FEATURE_DEPTH = 256
H = 8
DH = 32
PROJ_WIDTH = 32
CZ = 128
RES_DEV = 32
NUM_HOMOLOGS = 512
NUM_POSITIONS = 512


def shared_keys(key):
    bound_number = 4.0 / math.sqrt(FEATURE_DEPTH)
    starting_point = jax.random.normal(jax.random.fold_in(key, 101), (FEATURE_DEPTH, FEATURE_DEPTH), jnp.float32) / math.sqrt(FEATURE_DEPTH)
    random_perturbation = jax.random.normal(jax.random.fold_in(key, 202), (FEATURE_DEPTH, FEATURE_DEPTH), jnp.float32) / math.sqrt(FEATURE_DEPTH)
    return (jnp.clip(starting_point, -bound_number, bound_number), jnp.clip(random_perturbation, -bound_number, bound_number))


def draw_lookup_matrix(key, part):
    starting_point, random_perturbation = shared_keys(key)
    return starting_point.astype(jnp.bfloat16)


def draw_asking_matrix(key, part):
    starting_point, random_perturbation = shared_keys(key)
    blended_tensor = random_perturbation
    return blended_tensor.astype(jnp.bfloat16)


def draw_presence_indicator(key, part):
    seq_rows = lax.broadcasted_iota(jnp.int32, (NUM_HOMOLOGS, NUM_POSITIONS), 0)
    cutoff = 900 - 600 * seq_rows // NUM_HOMOLOGS
    drawn = jax.random.randint(key, (NUM_HOMOLOGS, NUM_POSITIONS), 0, 1000, dtype=jnp.int32)
    return jnp.where((drawn < cutoff) | (seq_rows == 0), 1, 0).astype(jnp.int32)


def levels(rng, dims, pieces, least, top_value):
    def one(axis_at, blocks):
        draws = jax.random.uniform(jax.random.fold_in(jax.random.fold_in(rng, 6), axis_at), (blocks,), jnp.float32, least / len(pieces), top_value / len(pieces))
        return jnp.repeat(jnp.exp(draws), dims[axis_at] // blocks).reshape((-1,) + (1,) * (len(dims) - axis_at - 1))

    gain = one(*pieces[0])
    for cut in pieces[1:]:
        gain = gain * one(*cut)
    return gain


def bell_draw(own_key, dims, deviation, reach, pieces=(), kind=jnp.bfloat16):
    result = deviation * jax.random.normal(own_key, dims, jnp.float32)
    if pieces:
        result = result * levels(own_key, dims, pieces, -0.22, 0.18)
    return jnp.clip(result, -reach, reach).astype(kind)


def setup_inputs(seed: int = 0) -> dict:
    key_list = jax.random.split(jax.random.key(seed), 13)
    homolog_representation = bell_draw(key_list[0], (NUM_HOMOLOGS, NUM_POSITIONS, FEATURE_DEPTH), 1.0, 6.0, ((0, 8), (1, 16)))
    presence_indicator = draw_presence_indicator(jax.random.fold_in(key_list[12], 71), 0)
    pairwise_delta_sensitivity = bell_draw(key_list[2], (NUM_POSITIONS, NUM_POSITIONS, CZ), (NUM_HOMOLOGS / 16), 192.0, ((0, 16), (1, 8)))
    upstream_sensitivity = bell_draw(key_list[3], (NUM_HOMOLOGS, NUM_POSITIONS, FEATURE_DEPTH), 1.0, 6.0, ((0, 8), (1, 16)))
    asking_matrix = draw_asking_matrix(jax.random.fold_in(key_list[12], 71), 0)
    lookup_matrix = draw_lookup_matrix(jax.random.fold_in(key_list[12], 71), 0)
    content_matrix = bell_draw(key_list[6], (FEATURE_DEPTH, FEATURE_DEPTH), FEATURE_DEPTH ** -0.5, 0.375)
    sigmoid_matrix = bell_draw(key_list[7], (FEATURE_DEPTH, FEATURE_DEPTH), FEATURE_DEPTH ** -0.5, 0.375)
    emission_matrix = bell_draw(key_list[8], (FEATURE_DEPTH, FEATURE_DEPTH), FEATURE_DEPTH ** -0.5, 0.375)
    lhs_projection_matrix = bell_draw(key_list[9], (FEATURE_DEPTH, PROJ_WIDTH), FEATURE_DEPTH ** -0.5, 0.375)
    rhs_projection_matrix = bell_draw(key_list[10], (FEATURE_DEPTH, PROJ_WIDTH), FEATURE_DEPTH ** -0.5, 0.375)
    pairwise_projection_matrix = bell_draw(key_list[11], (PROJ_WIDTH * PROJ_WIDTH, CZ), (PROJ_WIDTH * PROJ_WIDTH) ** -0.5, 0.1875)
    return dict(homolog_representation=homolog_representation, presence_indicator=presence_indicator, pairwise_delta_sensitivity=pairwise_delta_sensitivity, upstream_sensitivity=upstream_sensitivity, asking_matrix=asking_matrix, lookup_matrix=lookup_matrix, content_matrix=content_matrix, sigmoid_matrix=sigmoid_matrix, emission_matrix=emission_matrix, lhs_projection_matrix=lhs_projection_matrix, rhs_projection_matrix=rhs_projection_matrix, pairwise_projection_matrix=pairwise_projection_matrix)


epsilon = 1e-05
big_penalty = 1000000000.0

def normalize(values):
    center = values - lax.optimization_barrier(jnp.mean(values, -1, keepdims=True))
    inverse_scale = lax.rsqrt(lax.optimization_barrier(jnp.mean(center * center, -1, keepdims=True)) + epsilon)
    return (center * inverse_scale, inverse_scale)

def attend_column(column, livecol, asking_matrix, lookup_matrix, content_matrix, sigmoid_matrix, emission_matrix):
    standardized_tensor, unused_inv = normalize(column.astype(jnp.float32))
    normed_b = standardized_tensor.astype(jnp.bfloat16)
    extent_along = column.shape[0]
    query = (jnp.dot(normed_b, asking_matrix, preferred_element_type=jnp.float32) * DH ** (-0.5)).astype(jnp.bfloat16).reshape(extent_along, H, DH)
    keyed = jnp.dot(normed_b, lookup_matrix, preferred_element_type=jnp.float32).astype(jnp.bfloat16).reshape(extent_along, H, DH)
    content_projected = jnp.dot(normed_b, content_matrix, preferred_element_type=jnp.float32).astype(jnp.bfloat16).reshape(extent_along, H, DH)
    gating = jax.nn.sigmoid(jnp.dot(normed_b, sigmoid_matrix, preferred_element_type=jnp.float32))
    scores = jnp.einsum('shd,thd->hst', query.astype(jnp.float32), keyed.astype(jnp.float32), precision=lax.Precision.HIGHEST)
    scores = scores + ((livecol - 1.0) * big_penalty)[None, None, :]
    peak_score = lax.optimization_barrier(jnp.max(scores, -1, keepdims=True))
    powers = jnp.exp(scores - peak_score)
    attention_probabilities = (powers / lax.optimization_barrier(jnp.sum(powers, -1, keepdims=True))).astype(jnp.bfloat16)
    blended_tensor = jnp.einsum('wvx,xwj->vwj', attention_probabilities.astype(jnp.float32), content_projected.astype(jnp.float32), precision=lax.Precision.HIGHEST).reshape(extent_along, FEATURE_DEPTH)
    gated = (gating * blended_tensor).astype(jnp.bfloat16)
    update = jnp.dot(gated, emission_matrix, preferred_element_type=jnp.float32)
    return (column.astype(jnp.float32) + update).astype(jnp.bfloat16)

def vertical_attention_whole(block_cols, live_cols, parameter_collection):

    def per_column(column_pair):
        return attend_column(column_pair[0], column_pair[1], *parameter_collection)
    results = lax.map(per_column, (jnp.swapaxes(block_cols, 0, 1), jnp.swapaxes(live_cols, 0, 1)))
    return jnp.swapaxes(results, 0, 1)

def outer_product_backward(refreshed_result, live_homologs, pairwise_delta_sensitivity, upstream_sensitivity, lhs_projection_matrix, rhs_projection_matrix, pairwise_projection_matrix):
    standardized_tensor, inverse_scale = normalize(refreshed_result.astype(jnp.float32))
    flattened_tensor = standardized_tensor.astype(jnp.bfloat16).reshape(-1, FEATURE_DEPTH)
    left = (jnp.dot(flattened_tensor, lhs_projection_matrix, preferred_element_type=jnp.float32).reshape(NUM_HOMOLOGS, NUM_POSITIONS, PROJ_WIDTH) * live_homologs[..., None]).astype(jnp.bfloat16)
    right = (jnp.dot(flattened_tensor, rhs_projection_matrix, preferred_element_type=jnp.float32).reshape(NUM_HOMOLOGS, NUM_POSITIONS, PROJ_WIDTH) * live_homologs[..., None]).astype(jnp.bfloat16)
    counts = jnp.dot(live_homologs.T, live_homologs, precision=lax.Precision.HIGHEST)
    recip = 1.0 / (0.001 + counts)
    blocks = NUM_POSITIONS // RES_DEV
    right_full = right.astype(jnp.float32)

    def step_block(carry, items):
        cot_rows, left_rows, recip_rows = items
        projected = lax.dot_general(cot_rows.reshape(-1, CZ), pairwise_projection_matrix, (((1,), (1,)), ((), ())), preferred_element_type=jnp.float32)
        outer_cot = (projected.reshape(RES_DEV, NUM_POSITIONS, PROJ_WIDTH, PROJ_WIDTH) * recip_rows[:, :, None, None]).astype(jnp.bfloat16).astype(jnp.float32)
        left_part = jnp.einsum('ijce,sje->sic', outer_cot, right_full, precision=lax.Precision.HIGHEST)
        carry = carry + jnp.einsum('ijce,sic->sje', outer_cot, left_rows.astype(jnp.float32), precision=lax.Precision.HIGHEST)
        return (carry, left_part)
    cot_blocks = pairwise_delta_sensitivity.reshape(blocks, RES_DEV, NUM_POSITIONS, CZ)
    left_blocks = jnp.swapaxes(left.reshape(NUM_HOMOLOGS, blocks, RES_DEV, PROJ_WIDTH), 0, 1)
    recip_blocks = recip.reshape(blocks, RES_DEV, NUM_POSITIONS)
    right_grad, left_parts = lax.scan(step_block, jnp.zeros((NUM_HOMOLOGS, NUM_POSITIONS, PROJ_WIDTH), jnp.float32), (cot_blocks, left_blocks, recip_blocks))
    left_grad = jnp.swapaxes(left_parts, 0, 1).reshape(NUM_HOMOLOGS, NUM_POSITIONS, PROJ_WIDTH)
    left_b = (left_grad * live_homologs[..., None]).astype(jnp.bfloat16).reshape(-1, PROJ_WIDTH)
    rhs_projected_tensor = (right_grad * live_homologs[..., None]).astype(jnp.bfloat16).reshape(-1, PROJ_WIDTH)
    tensor_contraction = (((1,), (1,)), ((), ()))
    layernorm_sensitivity = lax.dot_general(left_b, lhs_projection_matrix, tensor_contraction, preferred_element_type=jnp.float32)
    layernorm_sensitivity = (layernorm_sensitivity + lax.dot_general(rhs_projected_tensor, rhs_projection_matrix, tensor_contraction, preferred_element_type=jnp.float32)).reshape(NUM_HOMOLOGS, NUM_POSITIONS, FEATURE_DEPTH)
    first_mean = lax.optimization_barrier(jnp.mean(layernorm_sensitivity, -1, keepdims=True))
    second_mean = lax.optimization_barrier(jnp.mean(layernorm_sensitivity * standardized_tensor, -1, keepdims=True))
    middle_state = inverse_scale * (layernorm_sensitivity - first_mean - standardized_tensor * second_mean) + upstream_sensitivity.astype(jnp.float32)
    return middle_state.astype(jnp.bfloat16)

def reference(homolog_representation, presence_indicator, pairwise_delta_sensitivity, upstream_sensitivity, asking_matrix, lookup_matrix, content_matrix, sigmoid_matrix, emission_matrix, lhs_projection_matrix, rhs_projection_matrix, pairwise_projection_matrix):
    parameter_collection = (asking_matrix, lookup_matrix, content_matrix, sigmoid_matrix, emission_matrix)
    live_homologs = presence_indicator.astype(jnp.float32)
    refreshed_result = vertical_attention_whole(homolog_representation, live_homologs, parameter_collection)
    intermediate_sensitivity = outer_product_backward(refreshed_result, live_homologs, pairwise_delta_sensitivity, upstream_sensitivity, lhs_projection_matrix, rhs_projection_matrix, pairwise_projection_matrix)

    def vertical_sensitivity(items):
        column, livecol, cotan = items
        pullback_function = jax.vjp(lambda entry: attend_column(entry, livecol, *parameter_collection), column)[1]
        return pullback_function(cotan)[0]
    sensitivity_collection = lax.map(vertical_sensitivity, (jnp.swapaxes(homolog_representation, 0, 1), jnp.swapaxes(live_homologs, 0, 1), jnp.swapaxes(intermediate_sensitivity, 0, 1)))
    alignment_gradient = jnp.swapaxes(sensitivity_collection, 0, 1)
    return (alignment_gradient, intermediate_sensitivity)
```

```python
import jax
import jax.numpy as jnp
from jax import lax
from jax.experimental import pallas as pl
from jax.experimental.pallas import tpu as pltpu
from jax.sharding import PartitionSpec as P

F = 256
H = 8
DH = 32
N = 512
CW = 32
CZ = 128
EPS = 1e-05
BIG = 1e9
f32 = jnp.float32
bf16 = jnp.bfloat16
SCALE = DH ** (-0.5)
NT = (((1,), (1,)), ((), ()))


def mm(a, b):
    return jnp.dot(a, b, preferred_element_type=f32)


def mmt(a, b):
    return lax.dot_general(a, b, NT, preferred_element_type=f32)


def norm(v, axis):
    c = v - jnp.mean(v, axis, keepdims=True)
    inv = lax.rsqrt(jnp.mean(c * c, axis, keepdims=True) + EPS)
    return c * inv, inv


def spread(rows, h, extra):
    top = (h % 4) * DH
    parts = []
    if top:
        parts.append(jnp.zeros((top, N), bf16))
    parts.append(rows)
    if top < 96:
        parts.append(jnp.zeros((96 - top, N), bf16))
    parts.append(extra)
    return jnp.concatenate(parts, axis=0)


def fwd_kernel(x_ref, live_ref, wq, wk, wv, wg, we, wl, wr,
               p_ref, o_ref, g_ref, a_ref, l_ref, r_ref,
               wt, wlt, bias_s):
    k = pl.program_id(0)

    @pl.when(k == 0)
    def _():
        for n, w in enumerate((wq, wv, wg, we)):
            wt[n] = w[...].T
        wlt[0] = wl[...].T
        wlt[1] = wr[...].T
        b = (live_ref[...] - 1.0) * BIG
        b = jnp.concatenate([b, jnp.zeros((120, N), f32)], axis=0)
        bias_s[...] = b.T.astype(bf16)

    xin = x_ref[...].reshape(N, F)
    xhat, _ = norm(xin.astype(f32), 1)
    xb = xhat.astype(bf16)
    xbt = xb.T
    qt = (mm(wt[0], xbt) * SCALE).astype(bf16)
    vt = mm(wt[1], xbt).astype(bf16)
    kk = mm(xb, wk[...]).astype(bf16)
    gt = jax.nn.sigmoid(mm(wt[2], xbt))
    g_ref[0] = gt
    extra = (lax.broadcasted_iota(jnp.int32, (128, N), 0) == k).astype(f32).astype(bf16)
    bias = bias_s[...]
    for h in range(H):
        grp = h // 4
        lhs = jnp.concatenate([kk[:, 128 * grp:128 * grp + 128], bias], axis=1)
        st = mm(lhs, spread(qt[DH * h:DH * h + DH], h, extra))
        m = jnp.max(st, 0, keepdims=True)
        e = jnp.exp(st - m)
        s = jnp.sum(e, 0, keepdims=True)
        p = (e * (1.0 / s)).astype(bf16)
        p_ref[0, h] = p
        o_ref[0, pl.ds(DH * h, DH), :] = mm(vt[DH * h:DH * h + DH], p)
    gated = (gt * o_ref[0]).astype(bf16)
    up = mm(wt[3], gated)
    after = (xin.T.astype(f32) + up).astype(bf16)
    a_ref[0] = after
    yhat, _ = norm(after.astype(f32), 0)
    yb = yhat.astype(bf16)
    live = live_ref[pl.ds(k, 1), :]
    l_ref[0] = (mm(wlt[0], yb) * live).astype(bf16)
    r_ref[0] = (mm(wlt[1], yb) * live).astype(bf16)


def mid_kernel(a_ref, up_ref, lg_ref, rg_ref, wl, wr, it_ref, i_ref):
    yhat, inv = norm(a_ref[0].astype(f32), 0)
    dy = mm(wl[...], lg_ref[0]) + mm(wr[...], rg_ref[0])
    m1 = jnp.mean(dy, 0, keepdims=True)
    m2 = jnp.mean(dy * yhat, 0, keepdims=True)
    upt = up_ref[...].reshape(N, F).T.astype(f32)
    out = (inv * (dy - m1 - yhat * m2) + upt).astype(bf16)
    it_ref[0] = out
    i_ref[...] = out.T.reshape(i_ref.shape)


def bwd_kernel(x_ref, d_ref, p_ref, o_ref, g_ref, wq, wk, wv, wg, we,
               out_ref, wkt, acc_k, acc_v, acc_q):
    @pl.when(pl.program_id(0) == 0)
    def _():
        wkt[...] = wk[...].T

    xin = x_ref[...].reshape(N, F)
    xhat, _ = norm(xin.astype(f32), 1)
    xb = xhat.astype(bf16)
    xbt = xb.T
    q = (mm(xb, wq[...]) * SCALE).astype(bf16)
    v = mm(xb, wv[...]).astype(bf16)
    kt = mm(wkt[...], xbt).astype(bf16)
    gt = g_ref[0]
    ot = o_ref[0]
    dt = d_ref[0]
    dg = mm(we[...], dt).astype(bf16).astype(f32)
    dot_ = (dg * gt).astype(bf16)
    dpre = (dg * ot * gt * (1.0 - gt)).astype(bf16)
    do = dot_.T
    prod = dot_.astype(f32) * ot
    row = lax.broadcasted_iota(jnp.int32, (128, N), 0)
    col = lax.broadcasted_iota(jnp.int32, (N, 128), 1)
    ones = (col < 2).astype(f32).astype(bf16)
    lane = lax.broadcasted_iota(jnp.int32, (N, F), 1) // DH
    dk = jnp.zeros((N, F), f32)
    dv = jnp.zeros((N, F), f32)
    for h in range(H):
        grp = h // 4
        sl = slice(DH * h, DH * h + DH)
        dd = -jnp.sum(prod[sl], 0, keepdims=True)
        hi = dd.astype(bf16).astype(f32)
        lo = dd - hi
        extra = jnp.where(row == 0, hi, jnp.where(row == 1, lo, 0.0)).astype(bf16)
        lhs = jnp.concatenate([v[:, 128 * grp:128 * grp + 128], ones], axis=1)
        dp = mm(lhs, spread(dot_[sl], h, extra))
        p = p_ref[0, h]
        ds = (p.astype(f32) * dp).astype(bf16)
        mask = lane == h
        zero = jnp.zeros((), bf16)
        dv = dv + mm(p, jnp.where(mask, do, zero))
        dk = dk + mm(ds, jnp.where(mask, q, zero))
        acc_q[sl, :] = mm(kt[sl], ds)
    dq = (acc_q[...].astype(bf16).astype(f32) * SCALE).astype(bf16)
    dx = (mm(wq[...], dq) + mm(wg[...], dpre)
          + mmt(wk[...], dk.astype(bf16)) + mmt(wv[...], dv.astype(bf16)))
    dx = dx.astype(bf16).astype(f32)
    xt = xin.T.astype(f32)
    xh, inv = norm(xt, 0)
    m1 = jnp.mean(dx, 0, keepdims=True)
    m2 = jnp.mean(dx * xh, 0, keepdims=True)
    dln = (inv * (dx - m1 - xh * m2)).astype(bf16)
    out = (dt.astype(f32) + dln.astype(f32)).astype(bf16)
    out_ref[...] = out.T.reshape(out_ref.shape)


def whole(shape):
    return pl.BlockSpec(shape, lambda k: (0,) * len(shape))


def percol(shape):
    return pl.BlockSpec((1, *shape), lambda k: (k,) + (0,) * len(shape))


COLS = pl.BlockSpec((8, 1, 64, F), lambda k: (0, k, 0, 0))
PARAMS = pltpu.CompilerParams(vmem_limit_bytes=60 * 1024 * 1024, dimension_semantics=("arbitrary",))


def fwd(x, livet, wq, wk, wv, wg, we, wl, wr):
    C = x.shape[1]
    sd = jax.ShapeDtypeStruct
    return pl.pallas_call(
        fwd_kernel,
        grid=(C,),
        in_specs=[COLS, whole((8, N))] + [whole((F, F))] * 5 + [whole((F, CW))] * 2,
        out_specs=[percol((H, N, N)), percol((F, N)), percol((F, N)), percol((F, N)), percol((CW, N)), percol((CW, N))],
        out_shape=[sd((C, H, N, N), bf16), sd((C, F, N), f32), sd((C, F, N), f32), sd((C, F, N), bf16), sd((C, CW, N), bf16), sd((C, CW, N), bf16)],
        scratch_shapes=[pltpu.VMEM((4, F, F), bf16), pltpu.VMEM((2, CW, F), bf16), pltpu.VMEM((N, 128), bf16)],
        compiler_params=PARAMS,
        name="attention_forward",
        cost_estimate=pl.CostEstimate(flops=20_000_000_000, bytes_accessed=30_000_000, transcendentals=8_000_000),
    )(x, livet, wq, wk, wv, wg, we, wl, wr)


def mid(at, up, lg, rg, wl, wr):
    C = at.shape[0]
    sd = jax.ShapeDtypeStruct
    return pl.pallas_call(
        mid_kernel,
        grid=(C,),
        in_specs=[percol((F, N)), COLS, percol((CW, N)), percol((CW, N)), whole((F, CW)), whole((F, CW))],
        out_specs=[percol((F, N)), COLS],
        out_shape=[sd((C, F, N), bf16), sd((8, C, 64, F), bf16)],
        compiler_params=PARAMS,
        name="middle",
        cost_estimate=pl.CostEstimate(flops=500_000_000, bytes_accessed=5_000_000, transcendentals=0),
    )(at, up, lg, rg, wl, wr)


def bwd(x, dt, p, o, g, wq, wk, wv, wg, we):
    C = x.shape[1]
    sd = jax.ShapeDtypeStruct
    return pl.pallas_call(
        bwd_kernel,
        grid=(C,),
        in_specs=[COLS, percol((F, N)), percol((H, N, N)), percol((F, N)), percol((F, N))] + [whole((F, F))] * 5,
        out_specs=COLS,
        out_shape=sd((8, C, 64, F), bf16),
        scratch_shapes=[pltpu.VMEM((F, F), bf16), pltpu.VMEM((N, F), f32), pltpu.VMEM((N, F), f32), pltpu.VMEM((F, N), f32)],
        compiler_params=PARAMS,
        name="attention_backward",
        cost_estimate=pl.CostEstimate(flops=40_000_000_000, bytes_accessed=30_000_000, transcendentals=0),
    )(x, dt, p, o, g, wq, wk, wv, wg, we)


def outer_kernel(pd_ref, rc_ref, w_ref, oc1_ref, oc2_ref, perm):
    @pl.when(pl.program_id(0) == 0)
    def _():
        a = lax.broadcasted_iota(jnp.int32, (1024, 1024), 0)
        b = lax.broadcasted_iota(jnp.int32, (1024, 1024), 1)
        hit = ((a // CW) == (b % CW)) & ((a % CW) == (b // CW))
        perm[...] = hit.astype(f32).astype(bf16)

    z = (mmt(w_ref[...], pd_ref[...]) * rc_ref[...]).astype(bf16)
    rows = []
    for j in range(8):
        rows.append(jnp.concatenate([z[CW * c:CW * c + CW, CW * j:CW * j + CW] for c in range(CW)], axis=1))
    y = mm(jnp.concatenate(rows, axis=0), perm[...]).astype(bf16)
    oc1_ref[...] = y
    oc2_ref[...] = y.T


def outer(pd, recip, w):
    sd = jax.ShapeDtypeStruct
    return pl.pallas_call(
        outer_kernel,
        grid=(8,),
        in_specs=[pl.BlockSpec((256, 128), lambda k: (k, 0)), pl.BlockSpec((1, 256), lambda k: (0, k)), pl.BlockSpec((1024, 128), lambda k: (0, 0))],
        out_specs=[pl.BlockSpec((256, 1024), lambda k: (k, 0)), pl.BlockSpec((1024, 256), lambda k: (0, k))],
        out_shape=[sd((2048, 1024), bf16), sd((1024, 2048), bf16)],
        scratch_shapes=[pltpu.VMEM((1024, 1024), bf16)],
        compiler_params=PARAMS,
        name="outer_cotangent",
        cost_estimate=pl.CostEstimate(flops=5_000_000_000, bytes_accessed=10_000_000, transcendentals=0),
    )(pd, recip, w)


def on_device(msa, present, pair, upstream, wq, wk, wv, wg, we, wl, wr, wo):
    d = lax.axis_index("dep")
    D = lax.axis_size("dep")
    R = lax.axis_size("res")

    def to_columns(a):
        a = a.transpose(1, 0, 2).reshape(D, 4, 64, F)
        return lax.all_to_all(a, "dep", 0, 0, tiled=True)

    def to_rows(a):
        a = lax.all_to_all(a, "dep", 0, 0, tiled=True)
        return a.reshape(4 * D, 64, F).transpose(1, 0, 2)

    x = to_columns(msa)
    live_b = present.T.astype(bf16)
    live_i = lax.all_gather(live_b, "dep", axis=1, tiled=True)
    live_own = lax.dynamic_slice_in_dim(live_i, 4 * d, 4, 0)
    live_j = lax.all_gather(live_own, "res", axis=0, tiled=True)
    counts = mmt(live_j, live_i)
    recip = 1.0 / (0.001 + counts)
    up = to_columns(upstream)
    pd = pair.reshape(32, 2, D, 4, CZ).transpose(2, 1, 3, 0, 4)
    pd = lax.all_to_all(pd, "dep", 0, 0, tiled=True)
    oc1, oc2 = outer(pd.reshape(-1, CZ), recip.reshape(1, -1), wo)
    live4 = live_own.astype(f32)
    livet = jnp.pad(live4, ((0, 4), (0, 0)))
    p, o, g, at, lt, rt = fwd(x, livet, wq, wk, wv, wg, we, wl, wr)
    lall = lax.all_gather(lt.reshape(4 * CW, N), "dep", axis=0, tiled=True)
    rall = lax.all_gather(rt.reshape(4 * CW, N), "res", axis=0, tiled=True)
    lp = mm(oc2, rall).astype(bf16).reshape(D, 4 * CW, N)
    rp = mm(oc1, lall).astype(bf16).reshape(R, 4 * CW, N)
    lp = lax.all_to_all(lp, "dep", 0, 0, tiled=True).astype(f32).sum(0).reshape(4, CW, N)
    rp = lax.all_to_all(rp, "res", 0, 0, tiled=True).astype(f32).sum(0).reshape(4, CW, N)
    lg = (lp * live4[:, None, :]).astype(bf16)
    rg = (rp * live4[:, None, :]).astype(bf16)
    dt, inter = mid(at, up, lg, rg, wl, wr)
    grad = bwd(x, dt, p, o, g, wq, wk, wv, wg, we)
    return to_rows(grad), to_rows(inter)


def solution(mesh):
    rows = P("dep", "res", None)
    in_specs = (rows, P("dep", "res"), P("res", "dep", None), rows) + (P(),) * 8
    return jax.shard_map(on_device, mesh=mesh, in_specs=in_specs, out_specs=(rows, rows), check_vma=False)
```

```python
import jax
import jax.numpy as jnp
from jax import lax
from jax.experimental import pallas as pl
from jax.experimental.pallas import tpu as pltpu
from jax.sharding import PartitionSpec as P

F = 256
H = 8
DH = 32
N = 512
CW = 32
CZ = 128
EPS = 1e-05
BIG = 1e9
f32 = jnp.float32
bf16 = jnp.bfloat16
SCALE = DH ** (-0.5)
NT = (((1,), (1,)), ((), ()))


def mm(a, b):
    return jnp.dot(a, b, preferred_element_type=f32)


def mmt(a, b):
    return lax.dot_general(a, b, NT, preferred_element_type=f32)


def norm(v, axis):
    c = v - jnp.mean(v, axis, keepdims=True)
    inv = lax.rsqrt(jnp.mean(c * c, axis, keepdims=True) + EPS)
    return c * inv, inv


def spread(rows, h, extra):
    top = (h % 4) * DH
    parts = []
    if top:
        parts.append(jnp.zeros((top, N), bf16))
    parts.append(rows)
    if top < 96:
        parts.append(jnp.zeros((96 - top, N), bf16))
    parts.append(extra)
    return jnp.concatenate(parts, axis=0)


def fwd_kernel(x_ref, live_ref, wq, wk, wv, wg, we, wl, wr,
               p_ref, o_ref, g_ref, a_ref, l_ref, r_ref,
               wt, wlt, bias_s):
    k = pl.program_id(0)

    @pl.when(k == 0)
    def _():
        for n, w in enumerate((wq, wv, wg, we)):
            wt[n] = w[...].T
        wlt[0] = wl[...].T
        wlt[1] = wr[...].T
        b = (live_ref[...] - 1.0) * BIG
        b = jnp.concatenate([b, jnp.zeros((120, N), f32)], axis=0)
        bias_s[...] = b.T.astype(bf16)

    xin = x_ref[...].reshape(N, F)
    xhat, _ = norm(xin.astype(f32), 1)
    xb = xhat.astype(bf16)
    xbt = xb.T
    qt = (mm(wt[0], xbt) * SCALE).astype(bf16)
    vt = mm(wt[1], xbt).astype(bf16)
    kk = mm(xb, wk[...]).astype(bf16)
    gt = jax.nn.sigmoid(mm(wt[2], xbt))
    g_ref[0] = gt
    extra = (lax.broadcasted_iota(jnp.int32, (128, N), 0) == k).astype(f32).astype(bf16)
    bias = bias_s[...]
    for h in range(H):
        grp = h // 4
        lhs = jnp.concatenate([kk[:, 128 * grp:128 * grp + 128], bias], axis=1)
        st = mm(lhs, spread(qt[DH * h:DH * h + DH], h, extra))
        m = jnp.max(st, 0, keepdims=True)
        e = jnp.exp(st - m)
        s = jnp.sum(e, 0, keepdims=True)
        p = (e * (1.0 / s)).astype(bf16)
        p_ref[0, h] = p
        o_ref[0, pl.ds(DH * h, DH), :] = mm(vt[DH * h:DH * h + DH], p)
    gated = (gt * o_ref[0]).astype(bf16)
    up = mm(wt[3], gated)
    after = (xin.T.astype(f32) + up).astype(bf16)
    a_ref[0] = after
    yhat, _ = norm(after.astype(f32), 0)
    yb = yhat.astype(bf16)
    live = live_ref[pl.ds(k, 1), :]
    l_ref[0] = (mm(wlt[0], yb) * live).astype(bf16)
    r_ref[0] = (mm(wlt[1], yb) * live).astype(bf16)


def mid_kernel(a_ref, up_ref, lg_ref, rg_ref, wl, wr, it_ref, i_ref):
    yhat, inv = norm(a_ref[0].astype(f32), 0)
    dy = mm(wl[...], lg_ref[0]) + mm(wr[...], rg_ref[0])
    m1 = jnp.mean(dy, 0, keepdims=True)
    m2 = jnp.mean(dy * yhat, 0, keepdims=True)
    upt = up_ref[...].reshape(N, F).T.astype(f32)
    out = (inv * (dy - m1 - yhat * m2) + upt).astype(bf16)
    it_ref[0] = out
    i_ref[...] = out.T.reshape(i_ref.shape)


def bwd_kernel(x_ref, d_ref, p_ref, o_ref, g_ref, wq, wk, wv, wg, we,
               out_ref, wkt, acc_k, acc_v, acc_q):
    @pl.when(pl.program_id(0) == 0)
    def _():
        wkt[...] = wk[...].T

    xin = x_ref[...].reshape(N, F)
    xhat, _ = norm(xin.astype(f32), 1)
    xb = xhat.astype(bf16)
    xbt = xb.T
    q = (mm(xb, wq[...]) * SCALE).astype(bf16)
    v = mm(xb, wv[...]).astype(bf16)
    kt = mm(wkt[...], xbt).astype(bf16)
    gt = g_ref[0]
    ot = o_ref[0]
    dt = d_ref[0]
    dg = mm(we[...], dt).astype(bf16).astype(f32)
    dot_ = (dg * gt).astype(bf16)
    dpre = (dg * ot * gt * (1.0 - gt)).astype(bf16)
    do = dot_.T
    prod = dot_.astype(f32) * ot
    row = lax.broadcasted_iota(jnp.int32, (128, N), 0)
    col = lax.broadcasted_iota(jnp.int32, (N, 128), 1)
    ones = (col < 2).astype(f32).astype(bf16)
    lane = lax.broadcasted_iota(jnp.int32, (N, F), 1) // DH
    dk = jnp.zeros((N, F), f32)
    dv = jnp.zeros((N, F), f32)
    for h in range(H):
        grp = h // 4
        sl = slice(DH * h, DH * h + DH)
        dd = -jnp.sum(prod[sl], 0, keepdims=True)
        hi = dd.astype(bf16).astype(f32)
        lo = dd - hi
        extra = jnp.where(row == 0, hi, jnp.where(row == 1, lo, 0.0)).astype(bf16)
        lhs = jnp.concatenate([v[:, 128 * grp:128 * grp + 128], ones], axis=1)
        dp = mm(lhs, spread(dot_[sl], h, extra))
        p = p_ref[0, h]
        ds = (p.astype(f32) * dp).astype(bf16)
        mask = lane == h
        zero = jnp.zeros((), bf16)
        dv = dv + mm(p, jnp.where(mask, do, zero))
        dk = dk + mm(ds, jnp.where(mask, q, zero))
        acc_q[sl, :] = mm(kt[sl], ds)
    dq = (acc_q[...].astype(bf16).astype(f32) * SCALE).astype(bf16)
    dx = (mm(wq[...], dq) + mm(wg[...], dpre)
          + mmt(wk[...], dk.astype(bf16)) + mmt(wv[...], dv.astype(bf16)))
    dx = dx.astype(bf16).astype(f32)
    xt = xin.T.astype(f32)
    xh, inv = norm(xt, 0)
    m1 = jnp.mean(dx, 0, keepdims=True)
    m2 = jnp.mean(dx * xh, 0, keepdims=True)
    dln = (inv * (dx - m1 - xh * m2)).astype(bf16)
    out = (dt.astype(f32) + dln.astype(f32)).astype(bf16)
    out_ref[...] = out.T.reshape(out_ref.shape)


def whole(shape):
    return pl.BlockSpec(shape, lambda k: (0,) * len(shape))


def percol(shape):
    return pl.BlockSpec((1, *shape), lambda k: (k,) + (0,) * len(shape))


COLS = pl.BlockSpec((8, 1, 64, F), lambda k: (0, k, 0, 0))
PARAMS = pltpu.CompilerParams(vmem_limit_bytes=60 * 1024 * 1024, dimension_semantics=("arbitrary",))


def fwd(x, livet, wq, wk, wv, wg, we, wl, wr):
    C = x.shape[1]
    sd = jax.ShapeDtypeStruct
    return pl.pallas_call(
        fwd_kernel,
        grid=(C,),
        in_specs=[COLS, whole((8, N))] + [whole((F, F))] * 5 + [whole((F, CW))] * 2,
        out_specs=[percol((H, N, N)), percol((F, N)), percol((F, N)), percol((F, N)), percol((CW, N)), percol((CW, N))],
        out_shape=[sd((C, H, N, N), bf16), sd((C, F, N), f32), sd((C, F, N), f32), sd((C, F, N), bf16), sd((C, CW, N), bf16), sd((C, CW, N), bf16)],
        scratch_shapes=[pltpu.VMEM((4, F, F), bf16), pltpu.VMEM((2, CW, F), bf16), pltpu.VMEM((N, 128), bf16)],
        compiler_params=PARAMS,
        name="attention_forward",
        cost_estimate=pl.CostEstimate(flops=20_000_000_000, bytes_accessed=30_000_000, transcendentals=8_000_000),
    )(x, livet, wq, wk, wv, wg, we, wl, wr)


def mid(at, up, lg, rg, wl, wr):
    C = at.shape[0]
    sd = jax.ShapeDtypeStruct
    return pl.pallas_call(
        mid_kernel,
        grid=(C,),
        in_specs=[percol((F, N)), COLS, percol((CW, N)), percol((CW, N)), whole((F, CW)), whole((F, CW))],
        out_specs=[percol((F, N)), COLS],
        out_shape=[sd((C, F, N), bf16), sd((8, C, 64, F), bf16)],
        compiler_params=PARAMS,
        name="middle",
        cost_estimate=pl.CostEstimate(flops=500_000_000, bytes_accessed=5_000_000, transcendentals=0),
    )(at, up, lg, rg, wl, wr)


def bwd(x, dt, p, o, g, wq, wk, wv, wg, we):
    C = x.shape[1]
    sd = jax.ShapeDtypeStruct
    return pl.pallas_call(
        bwd_kernel,
        grid=(C,),
        in_specs=[COLS, percol((F, N)), percol((H, N, N)), percol((F, N)), percol((F, N))] + [whole((F, F))] * 5,
        out_specs=COLS,
        out_shape=sd((8, C, 64, F), bf16),
        scratch_shapes=[pltpu.VMEM((F, F), bf16), pltpu.VMEM((N, F), f32), pltpu.VMEM((N, F), f32), pltpu.VMEM((F, N), f32)],
        compiler_params=PARAMS,
        name="attention_backward",
        cost_estimate=pl.CostEstimate(flops=40_000_000_000, bytes_accessed=30_000_000, transcendentals=0),
    )(x, dt, p, o, g, wq, wk, wv, wg, we)


MESH = pl.DeviceIdType.MESH


def remote(src, dst, send, recv, dep, res):
    return pltpu.make_async_remote_copy(src_ref=src, dst_ref=dst, send_sem=send, recv_sem=recv,
                                        device_id={"dep": dep, "res": res}, device_id_type=MESH)


def greet(peers):
    bar = pltpu.get_barrier_semaphore()
    for dep, res in peers:
        pl.semaphore_signal(bar, inc=1, device_id={"dep": dep, "res": res}, device_id_type=MESH)
    pl.semaphore_wait(bar, len(peers))


def opm_kernel(lt, rt, pd, rc, wo, live, lo, ro,
               perm, oc1, oc2, lbuf, rbuf, lsend, lrecv, psend, precv, rsend, rrecv, lacc, racc,
               ls, lr, rs, rr, fs, fr, ps, pr, s2, r2, s3, r3):
    d = lax.axis_index("dep")
    r = lax.axis_index("res")
    core = lax.rem(r, 2)
    chip = r // 2
    partner = 2 * chip + 1 - core

    def dep_at(k):
        return lax.rem(d + k, 8)

    def chip_at(k):
        return lax.rem(chip + k, 8)

    greet([(dep_at(k), r) for k in range(1, 8)]
          + [(d, 2 * chip_at(k) + core) for k in range(1, 8)] + [(d, partner)])

    gl = [remote(lt, lbuf.at[d], ls.at[k], lr.at[k], dep_at(k), r) for k in range(1, 8)]
    gr = [remote(rt, rbuf.at[r], rs.at[k], rr.at[k], d, 2 * chip_at(k) + core) for k in range(1, 8)]
    first = remote(rt, rbuf.at[r], fs.at[0], fr.at[0], d, partner)
    for a, b in zip(gl, gr):
        b.start()
        a.start()
    first.start()
    lbuf[d] = lt[...]
    rbuf[r] = rt[...]

    a = lax.broadcasted_iota(jnp.int32, (1024, 1024), 0)
    b = lax.broadcasted_iota(jnp.int32, (1024, 1024), 1)
    hit = ((a // CW) == (b % CW)) & ((a % CW) == (b // CW))
    perm[...] = hit.astype(f32).astype(bf16)

    def forward(k):
        slot = 2 * lax.rem(chip + 8 - k, 8) + core
        return remote(rbuf.at[slot], rbuf.at[slot], fs.at[k], fr.at[k], d, partner)

    def outer_step(n, carry):
        at = pl.multiple_of(256 * n, 256)
        z = (mmt(wo[...], pd[pl.ds(at, 256), :]) * rc[pl.ds(n, 1), :]).astype(bf16)
        rows = []
        for j in range(8):
            rows.append(jnp.concatenate([z[CW * c:CW * c + CW, CW * j:CW * j + CW] for c in range(CW)], axis=1))
        y = mm(jnp.concatenate(rows, axis=0), perm[...]).astype(bf16)
        oc1[pl.ds(at, 256), :] = y
        oc2[:, pl.ds(at, 256)] = y.T

        @pl.when(n > 0)
        def _():
            remote(rt, rbuf.at[r], rs.at[n], rr.at[n], d, partner).wait_recv()
            forward(n).start()
        return carry

    lax.fori_loop(0, 8, outer_step, 0)
    for c in gl:
        c.wait_recv()
    lall = lbuf[...].reshape(1024, N)
    part = []
    for k in [1, 2, 3, 4, 5, 6, 7, 0]:
        q = chip_at(k)
        at = pl.multiple_of(256 * q + 128 * (1 - core), 128)
        psend[k] = mm(oc1[pl.ds(at, 128), :], lall).astype(bf16)
        c = remote(psend.at[k], precv.at[k], ps.at[k], pr.at[k], d, partner)
        c.start()
        part.append(c)
    second = []
    for k in [1, 2, 3, 4, 5, 6, 7, 0]:
        q = chip_at(k)
        at = pl.multiple_of(256 * q + 128 * core, 128)
        own = mm(oc1[pl.ds(at, 128), :], lall)
        remote(psend.at[k], precv.at[k], ps.at[k], pr.at[k], d, partner).wait_recv()
        own = own + precv[k].astype(f32)
        if k:
            rsend[k] = own.astype(bf16)
            c = remote(rsend.at[k], rrecv.at[k], s2.at[k], r2.at[k], d, 2 * q + core)
            c.start()
            second.append(c)
        else:
            racc[...] = own
    first.wait_recv()
    for k in range(1, 8):
        forward(k).wait_recv()
    rall = rbuf[...].reshape(2048, N)
    third = []
    for k in [1, 2, 3, 4, 5, 6, 7, 0]:
        at = pl.multiple_of(128 * dep_at(k), 128)
        own = mm(oc2[pl.ds(at, 128), :], rall)
        if k:
            lsend[k] = own.astype(bf16)
            c = remote(lsend.at[k], lrecv.at[k], s3.at[k], r3.at[k], dep_at(k), r)
            c.start()
            third.append(c)
        else:
            lacc[...] = own
    for c in second:
        c.wait_recv()
    racc[...] += jnp.sum(rrecv[1:8].astype(f32), 0)
    for n in range(4):
        ro[n] = (racc[CW * n:CW * n + CW, :] * live[n:n + 1, :]).astype(bf16)
    for c in third:
        c.wait_recv()
    lacc[...] += jnp.sum(lrecv[1:8].astype(f32), 0)
    for n in range(4):
        lo[n] = (lacc[CW * n:CW * n + CW, :] * live[n:n + 1, :]).astype(bf16)
    for c in gl + gr + [first] + part + second + third:
        c.wait_send()
    for k in range(1, 8):
        forward(k).wait_send()


def opm(lt, rt, pd, rc, wo, live):
    sd = jax.ShapeDtypeStruct
    vm = pl.BlockSpec(memory_space=pltpu.VMEM)
    chunk = (128, N)
    V = pltpu.VMEM
    dma = pltpu.SemaphoreType.DMA((8,))
    return pl.pallas_call(
        opm_kernel,
        in_specs=[vm] * 6,
        out_specs=[vm] * 2,
        out_shape=[sd((4, CW, N), bf16)] * 2,
        scratch_shapes=[V((1024, 1024), bf16), V((2048, 1024), bf16), V((1024, 2048), bf16),
                        V((8, *chunk), bf16), V((16, *chunk), bf16)] + [V((8, *chunk), bf16)] * 6
        + [V(chunk, f32)] * 2 + [dma] * 12,
        compiler_params=pltpu.CompilerParams(vmem_limit_bytes=60 * 1024 * 1024, collective_id=1, has_side_effects=True),
        name="outer_product",
        cost_estimate=pl.CostEstimate(flops=10_000_000_000, bytes_accessed=10_000_000, transcendentals=0),
    )(lt, rt, pd, rc, wo, live)


def on_device(msa, present, pair, upstream, wq, wk, wv, wg, we, wl, wr, wo):
    d = lax.axis_index("dep")
    D = lax.axis_size("dep")

    def to_columns(a):
        a = a.transpose(1, 0, 2).reshape(D, 4, 64, F)
        return lax.all_to_all(a, "dep", 0, 0, tiled=True)

    def to_rows(a):
        a = lax.all_to_all(a, "dep", 0, 0, tiled=True)
        return a.reshape(4 * D, 64, F).transpose(1, 0, 2)

    x = to_columns(msa)
    live_b = present.T.astype(bf16)
    live_i = lax.all_gather(live_b, "dep", axis=1, tiled=True)
    live_own = lax.dynamic_slice_in_dim(live_i, 4 * d, 4, 0)
    live_j = lax.all_gather(live_own, "res", axis=0, tiled=True)
    counts = mmt(live_j, live_i)
    recip = 1.0 / (0.001 + counts)
    up = to_columns(upstream)
    pd = pair.reshape(32, 2, D, 4, CZ).transpose(2, 1, 3, 0, 4)
    pd = lax.all_to_all(pd, "dep", 0, 0, tiled=True)
    live4 = live_own.astype(f32)
    livet = jnp.pad(live4, ((0, 4), (0, 0)))
    p, o, g, at, lt, rt = fwd(x, livet, wq, wk, wv, wg, we, wl, wr)
    lg, rg = opm(lt.reshape(4 * CW, N), rt.reshape(4 * CW, N), pd.reshape(-1, CZ), recip.reshape(8, 256), wo, livet)
    dt, inter = mid(at, up, lg, rg, wl, wr)
    grad = bwd(x, dt, p, o, g, wq, wk, wv, wg, we)
    return to_rows(grad), to_rows(inter)


def solution(mesh):
    rows = P("dep", "res", None)
    in_specs = (rows, P("dep", "res"), P("res", "dep", None), rows) + (P(),) * 8
    return jax.shard_map(on_device, mesh=mesh, in_specs=in_specs, out_specs=(rows, rows), check_vma=False)
```

```python
import jax
import jax.numpy as jnp
from jax import lax
from jax.experimental import pallas as pl
from jax.experimental.pallas import tpu as pltpu
from jax.sharding import PartitionSpec as P

F = 256
H = 8
DH = 32
N = 512
CW = 32
CZ = 128
EPS = 1e-05
BIG = 1e9
f32 = jnp.float32
bf16 = jnp.bfloat16
SCALE = DH ** (-0.5)
NT = (((1,), (1,)), ((), ()))


def mm(a, b):
    return jnp.dot(a, b, preferred_element_type=f32)


def mmt(a, b):
    return lax.dot_general(a, b, NT, preferred_element_type=f32)


def norm(v, axis):
    c = v - jnp.mean(v, axis, keepdims=True)
    inv = lax.rsqrt(jnp.mean(c * c, axis, keepdims=True) + EPS)
    return c * inv, inv


def spread(rows, h, extra):
    top = (h % 4) * DH
    parts = []
    if top:
        parts.append(jnp.zeros((top, N), bf16))
    parts.append(rows)
    if top < 96:
        parts.append(jnp.zeros((96 - top, N), bf16))
    parts.append(extra)
    return jnp.concatenate(parts, axis=0)


MESH = pl.DeviceIdType.MESH


def remote(src, dst, send, recv, dep, res):
    return pltpu.make_async_remote_copy(src_ref=src, dst_ref=dst, send_sem=send, recv_sem=recv,
                                        device_id={"dep": dep, "res": res}, device_id_type=MESH)


def greet(peers):
    bar = pltpu.get_barrier_semaphore()
    for dep, res in peers:
        pl.semaphore_signal(bar, inc=1, device_id={"dep": dep, "res": res}, device_id_type=MESH)
    pl.semaphore_wait(bar, len(peers))


def fwd_kernel(hx, ux, px, live_in, wq, wk, wv, wg, we, wl, wr,
               x_ref, p_ref, o_ref, g_ref, a_ref, l_ref, r_ref, up_out, pd_out, rc_ref, live_out,
               wt, wlt, bias_s, xbuf, lbuf, livet, jbuf, mine, ustage, pstage,
               xs, xr, us, ur, ps, pr, ls, lr, js, jr, own):
    k = pl.program_id(0)
    d = lax.axis_index("dep")
    r = lax.axis_index("res")

    def dep_at(n):
        return lax.rem(d + n, 8)

    def res_at(n):
        return lax.rem(r + n, 16)

    def x_copy(c, n):
        return remote(hx.at[dep_at(n), c], xbuf.at[c, d], xs.at[c, n], xr.at[c, n], dep_at(n), r)

    def up_copy(n):
        return remote(ux.at[dep_at(n)], up_out.at[d], us.at[n], ur.at[n], dep_at(n), r)

    def pd_copy(n):
        return remote(px.at[dep_at(n)], pd_out.at[d], ps.at[n], pr.at[n], dep_at(n), r)

    def live_copy(n):
        return remote(live_in, lbuf.at[d], ls.at[n], lr.at[n], dep_at(n), r)

    def row_copy(n):
        return remote(mine, jbuf.at[r], js.at[n], jr.at[n], d, res_at(n))

    def own_x(c):
        return pltpu.make_async_copy(hx.at[d, c], xbuf.at[c, d], own.at[c])

    own_up = pltpu.make_async_copy(ux.at[d], ustage, own.at[4])
    own_pd = pltpu.make_async_copy(px.at[d], pstage, own.at[5])
    own_up2 = pltpu.make_async_copy(ustage, up_out.at[d], own.at[6])
    own_pd2 = pltpu.make_async_copy(pstage, pd_out.at[d], own.at[7])

    @pl.when(k == 0)
    def _():
        for c in range(4):
            own_x(c).start()
        own_up.start()
        own_pd.start()
        greet([(dep_at(n), r) for n in range(1, 8)] + [(d, res_at(n)) for n in range(1, 16)])
        for n in range(1, 8):
            live_copy(n).start()
        for c in range(4):
            for n in range(1, 8):
                x_copy(c, n).start()
        for n in range(1, 8):
            pd_copy(n).start()
        for n in range(1, 8):
            up_copy(n).start()
        lbuf[d] = live_in[...]
        for n, w in enumerate((wq, wv, wg, we)):
            wt[n] = w[...].T
        wlt[0] = wl[...].T
        wlt[1] = wr[...].T
        for n in range(1, 8):
            live_copy(n).wait_recv()
        live = lbuf[...].reshape(N, 128).astype(f32)
        bias_s[...] = ((live - 1.0) * BIG).astype(bf16)
        livet[...] = live.T
        rows = [livet[pl.ds(4 * d + n, 1), :] for n in range(4)]
        held = jnp.concatenate(rows + [jnp.zeros((4, N), f32)], axis=0)
        mine[...] = held
        live_out[...] = held
        jbuf[r] = held
        for n in range(1, 16):
            row_copy(n).start()

    @pl.when(k == 1)
    def _():
        own_up.wait()
        own_pd.wait()
        own_up2.start()
        own_pd2.start()

    @pl.when(k == 3)
    def _():
        for n in range(1, 16):
            row_copy(n).wait_recv()
        counts = mm(jbuf[...].reshape(128, N).astype(bf16), lbuf[...].reshape(N, 128))
        rec = 1.0 / (0.001 + counts)
        for n in range(8):
            pieces = []
            for j in range(8):
                at = 16 * n + 8 * (j // 4) + j % 4
                pieces.append(rec[at:at + 1, :CW])
            rc_ref[n:n + 1, :] = jnp.concatenate(pieces, axis=1)

    own_x(k).wait()
    for n in range(1, 8):
        x_copy(k, n).wait_recv()
    xin = xbuf[k].reshape(N, F)
    x_ref[...] = xin.reshape(x_ref.shape)
    xhat, _ = norm(xin.astype(f32), 1)
    xb = xhat.astype(bf16)
    xbt = xb.T
    qt = (mm(wt[0], xbt) * SCALE).astype(bf16)
    vt = mm(wt[1], xbt).astype(bf16)
    kk = mm(xb, wk[...]).astype(bf16)
    gt = jax.nn.sigmoid(mm(wt[2], xbt))
    g_ref[0] = gt
    extra = (lax.broadcasted_iota(jnp.int32, (128, N), 0) == 4 * d + k).astype(f32).astype(bf16)
    bias = bias_s[...]
    for h in range(H):
        grp = h // 4
        lhs = jnp.concatenate([kk[:, 128 * grp:128 * grp + 128], bias], axis=1)
        st = mm(lhs, spread(qt[DH * h:DH * h + DH], h, extra))
        m = jnp.max(st, 0, keepdims=True)
        e = jnp.exp(st - m)
        s = jnp.sum(e, 0, keepdims=True)
        p = (e * (1.0 / s)).astype(bf16)
        p_ref[0, h] = p
        o_ref[0, pl.ds(DH * h, DH), :] = mm(vt[DH * h:DH * h + DH], p)
    gated = (gt * o_ref[0]).astype(bf16)
    up = mm(wt[3], gated)
    after = (xin.T.astype(f32) + up).astype(bf16)
    a_ref[0] = after
    yhat, _ = norm(after.astype(f32), 0)
    yb = yhat.astype(bf16)
    live = livet[pl.ds(4 * d + k, 1), :]
    l_ref[0] = (mm(wlt[0], yb) * live).astype(bf16)
    r_ref[0] = (mm(wlt[1], yb) * live).astype(bf16)

    @pl.when(k == 3)
    def _():
        for n in range(1, 8):
            pd_copy(n).wait_recv()
            up_copy(n).wait_recv()
        own_up2.wait()
        own_pd2.wait()
        for n in range(1, 8):
            live_copy(n).wait_send()
            pd_copy(n).wait_send()
            up_copy(n).wait_send()
            for c in range(4):
                x_copy(c, n).wait_send()
        for n in range(1, 16):
            row_copy(n).wait_send()


def bwd_kernel(x_ref, up_ref, at_ref, lg_ref, rg_ref, p_ref, o_ref, g_ref, wq, wk, wv, wg, we, wl, wr,
               out_g, out_i, wkt, acc_q, sbuf, ss, rs, own):
    k = pl.program_id(0)
    d = lax.axis_index("dep")
    r = lax.axis_index("res")
    outs = (out_g, out_i)

    def dep_at(n):
        return lax.rem(d + n, 8)

    def send(which, c, n):
        return remote(sbuf.at[which, c, dep_at(n)], outs[which].at[d, c],
                      ss.at[which, c, n], rs.at[which, c, n], dep_at(n), r)

    def keep(which, c):
        return pltpu.make_async_copy(sbuf.at[which, c, d], outs[which].at[d, c], own.at[which, c])

    def ship(which, value):
        sbuf[which, k] = value.T.reshape(8, 64, F)
        for n in range(1, 8):
            send(which, k, n).start()
        keep(which, k).start()

    @pl.when(k == 0)
    def _():
        wkt[...] = wk[...].T
        greet([(dep_at(n), r) for n in range(1, 8)])

    yhat, yinv = norm(at_ref[0].astype(f32), 0)
    dy = mm(wl[...], lg_ref[0]) + mm(wr[...], rg_ref[0])
    m1 = jnp.mean(dy, 0, keepdims=True)
    m2 = jnp.mean(dy * yhat, 0, keepdims=True)
    upt = up_ref[...].reshape(N, F).T.astype(f32)
    dt = (yinv * (dy - m1 - yhat * m2) + upt).astype(bf16)
    ship(1, dt)

    xin = x_ref[...].reshape(N, F)
    xhat, _ = norm(xin.astype(f32), 1)
    xb = xhat.astype(bf16)
    xbt = xb.T
    q = (mm(xb, wq[...]) * SCALE).astype(bf16)
    v = mm(xb, wv[...]).astype(bf16)
    kt = mm(wkt[...], xbt).astype(bf16)
    gt = g_ref[0]
    ot = o_ref[0]
    dg = mm(we[...], dt).astype(bf16).astype(f32)
    dot_ = (dg * gt).astype(bf16)
    dpre = (dg * ot * gt * (1.0 - gt)).astype(bf16)
    do = dot_.T
    prod = dot_.astype(f32) * ot
    row = lax.broadcasted_iota(jnp.int32, (128, N), 0)
    col = lax.broadcasted_iota(jnp.int32, (N, 128), 1)
    ones = (col < 2).astype(f32).astype(bf16)
    lane = lax.broadcasted_iota(jnp.int32, (N, F), 1) // DH
    dk = jnp.zeros((N, F), f32)
    dv = jnp.zeros((N, F), f32)
    for h in range(H):
        grp = h // 4
        sl = slice(DH * h, DH * h + DH)
        dd = -jnp.sum(prod[sl], 0, keepdims=True)
        hi = dd.astype(bf16).astype(f32)
        lo = dd - hi
        extra = jnp.where(row == 0, hi, jnp.where(row == 1, lo, 0.0)).astype(bf16)
        lhs = jnp.concatenate([v[:, 128 * grp:128 * grp + 128], ones], axis=1)
        dp = mm(lhs, spread(dot_[sl], h, extra))
        p = p_ref[0, h]
        ds = (p.astype(f32) * dp).astype(bf16)
        mask = lane == h
        zero = jnp.zeros((), bf16)
        dv = dv + mm(p, jnp.where(mask, do, zero))
        dk = dk + mm(ds, jnp.where(mask, q, zero))
        acc_q[sl, :] = mm(kt[sl], ds)
    dq = (acc_q[...].astype(bf16).astype(f32) * SCALE).astype(bf16)
    dx = (mm(wq[...], dq) + mm(wg[...], dpre)
          + mmt(wk[...], dk.astype(bf16)) + mmt(wv[...], dv.astype(bf16)))
    dx = dx.astype(bf16).astype(f32)
    xt = xin.T.astype(f32)
    xh, inv = norm(xt, 0)
    m1 = jnp.mean(dx, 0, keepdims=True)
    m2 = jnp.mean(dx * xh, 0, keepdims=True)
    dln = (inv * (dx - m1 - xh * m2)).astype(bf16)
    out = (dt.astype(f32) + dln.astype(f32)).astype(bf16)
    ship(0, out)

    @pl.when(k == 3)
    def _():
        for which in range(2):
            for c in range(4):
                keep(which, c).wait()
                for n in range(1, 8):
                    send(which, c, n).wait_recv()
                    send(which, c, n).wait_send()


def whole(shape):
    return pl.BlockSpec(shape, lambda k: (0,) * len(shape))


def percol(shape):
    return pl.BlockSpec((1, *shape), lambda k: (k,) + (0,) * len(shape))


COLS = pl.BlockSpec((8, 1, 64, F), lambda k: (0, k, 0, 0))
ANY = pl.BlockSpec(memory_space=pl.ANY)


def fwd(hx, ux, px, live, wq, wk, wv, wg, we, wl, wr):
    sd = jax.ShapeDtypeStruct
    V = pltpu.VMEM
    dma = pltpu.SemaphoreType.DMA
    return pl.pallas_call(
        fwd_kernel,
        grid=(4,),
        in_specs=[ANY] * 3 + [whole((64, 128))] + [whole((F, F))] * 5 + [whole((F, CW))] * 2,
        out_specs=[COLS, percol((H, N, N)), percol((F, N)), percol((F, N)), percol((F, N)), percol((CW, N)),
                   percol((CW, N)), ANY, ANY, whole((8, 256)), whole((8, N))],
        out_shape=[sd((8, 4, 64, F), bf16), sd((4, H, N, N), bf16), sd((4, F, N), f32), sd((4, F, N), f32),
                   sd((4, F, N), bf16), sd((4, CW, N), bf16), sd((4, CW, N), bf16),
                   sd(ux.shape, bf16), sd(px.shape, bf16), sd((8, 256), f32), sd((8, N), f32)],
        scratch_shapes=[V((4, F, F), bf16), V((2, CW, F), bf16), V((N, 128), bf16), V((4, 8, 64, F), bf16),
                        V((8, 64, 128), bf16), V((128, N), f32), V((16, 8, N), f32), V((8, N), f32), V(ux.shape[1:], bf16),
                        V(px.shape[1:], bf16), dma((4, 8)), dma((4, 8))] + [dma((8,))] * 6 + [dma((16,))] * 2 + [dma((8,))],
        compiler_params=pltpu.CompilerParams(vmem_limit_bytes=60 * 1024 * 1024, collective_id=2, has_side_effects=True,
                                             dimension_semantics=("arbitrary",)),
        name="attention_forward",
    )(hx, ux, px, live, wq, wk, wv, wg, we, wl, wr)


def bwd(x, up, at, lg, rg, p, o, g, wq, wk, wv, wg, we, wl, wr):
    sd = jax.ShapeDtypeStruct
    V = pltpu.VMEM
    dma = pltpu.SemaphoreType.DMA
    return pl.pallas_call(
        bwd_kernel,
        grid=(4,),
        in_specs=[COLS, COLS, percol((F, N)), percol((CW, N)), percol((CW, N)), percol((H, N, N)), percol((F, N)),
                  percol((F, N))] + [whole((F, F))] * 5 + [whole((F, CW))] * 2,
        out_specs=[ANY, ANY],
        out_shape=[sd((8, 4, 64, F), bf16)] * 2,
        scratch_shapes=[V((F, F), bf16), V((F, N), f32), V((2, 4, 8, 64, F), bf16),
                        dma((2, 4, 8)), dma((2, 4, 8)), dma((2, 4))],
        compiler_params=pltpu.CompilerParams(vmem_limit_bytes=60 * 1024 * 1024, collective_id=3, has_side_effects=True,
                                             dimension_semantics=("arbitrary",)),
        name="attention_backward",
    )(x, up, at, lg, rg, p, o, g, wq, wk, wv, wg, we, wl, wr)


def opm_kernel(lt, rt, pd, rc, wo, live, lo, ro,
               perm, oc1, oc2, lbuf, rbuf, lsend, lrecv, psend, precv, rsend, rrecv, lacc, racc,
               ls, lr, rs, rr, fs, fr, ps, pr, s2, r2, s3, r3):
    d = lax.axis_index("dep")
    r = lax.axis_index("res")
    core = lax.rem(r, 2)
    chip = r // 2
    partner = 2 * chip + 1 - core

    def dep_at(k):
        return lax.rem(d + k, 8)

    def chip_at(k):
        return lax.rem(chip + k, 8)

    greet([(dep_at(k), r) for k in range(1, 8)]
          + [(d, 2 * chip_at(k) + core) for k in range(1, 8)] + [(d, partner)])

    gl = [remote(lt, lbuf.at[d], ls.at[k], lr.at[k], dep_at(k), r) for k in range(1, 8)]
    gr = [remote(rt, rbuf.at[r], rs.at[k], rr.at[k], d, 2 * chip_at(k) + core) for k in range(1, 8)]
    first = remote(rt, rbuf.at[r], fs.at[0], fr.at[0], d, partner)
    for a, b in zip(gl, gr):
        b.start()
        a.start()
    first.start()
    lbuf[d] = lt[...]
    rbuf[r] = rt[...]

    a = lax.broadcasted_iota(jnp.int32, (1024, 1024), 0)
    b = lax.broadcasted_iota(jnp.int32, (1024, 1024), 1)
    hit = ((a // CW) == (b % CW)) & ((a % CW) == (b // CW))
    perm[...] = hit.astype(f32).astype(bf16)

    def forward(k):
        slot = 2 * lax.rem(chip + 8 - k, 8) + core
        return remote(rbuf.at[slot], rbuf.at[slot], fs.at[k], fr.at[k], d, partner)

    def outer_step(n, carry):
        at = pl.multiple_of(256 * n, 256)
        z = (mmt(wo[...], pd[pl.ds(at, 256), :]) * rc[pl.ds(n, 1), :]).astype(bf16)
        rows = []
        for j in range(8):
            rows.append(jnp.concatenate([z[CW * c:CW * c + CW, CW * j:CW * j + CW] for c in range(CW)], axis=1))
        y = mm(jnp.concatenate(rows, axis=0), perm[...]).astype(bf16)
        oc1[pl.ds(at, 256), :] = y
        oc2[:, pl.ds(at, 256)] = y.T

        @pl.when(n > 0)
        def _():
            remote(rt, rbuf.at[r], rs.at[n], rr.at[n], d, partner).wait_recv()
            forward(n).start()
        return carry

    lax.fori_loop(0, 8, outer_step, 0)
    for c in gl:
        c.wait_recv()
    lall = lbuf[...].reshape(1024, N)
    part = []
    for k in [1, 2, 3, 4, 5, 6, 7, 0]:
        q = chip_at(k)
        at = pl.multiple_of(256 * q + 128 * (1 - core), 128)
        psend[k] = mm(oc1[pl.ds(at, 128), :], lall).astype(bf16)
        c = remote(psend.at[k], precv.at[k], ps.at[k], pr.at[k], d, partner)
        c.start()
        part.append(c)
    second = []
    for k in [1, 2, 3, 4, 5, 6, 7, 0]:
        q = chip_at(k)
        at = pl.multiple_of(256 * q + 128 * core, 128)
        own = mm(oc1[pl.ds(at, 128), :], lall)
        remote(psend.at[k], precv.at[k], ps.at[k], pr.at[k], d, partner).wait_recv()
        own = own + precv[k].astype(f32)
        if k:
            rsend[k] = own.astype(bf16)
            c = remote(rsend.at[k], rrecv.at[k], s2.at[k], r2.at[k], d, 2 * q + core)
            c.start()
            second.append(c)
        else:
            racc[...] = own
    first.wait_recv()
    for k in range(1, 8):
        forward(k).wait_recv()
    rall = rbuf[...].reshape(2048, N)
    third = []
    for k in [1, 2, 3, 4, 5, 6, 7, 0]:
        at = pl.multiple_of(128 * dep_at(k), 128)
        own = mm(oc2[pl.ds(at, 128), :], rall)
        if k:
            lsend[k] = own.astype(bf16)
            c = remote(lsend.at[k], lrecv.at[k], s3.at[k], r3.at[k], dep_at(k), r)
            c.start()
            third.append(c)
        else:
            lacc[...] = own
    for c in second:
        c.wait_recv()
    racc[...] += jnp.sum(rrecv[1:8].astype(f32), 0)
    for n in range(4):
        ro[n] = (racc[CW * n:CW * n + CW, :] * live[n:n + 1, :]).astype(bf16)
    for c in third:
        c.wait_recv()
    lacc[...] += jnp.sum(lrecv[1:8].astype(f32), 0)
    for n in range(4):
        lo[n] = (lacc[CW * n:CW * n + CW, :] * live[n:n + 1, :]).astype(bf16)
    for c in gl + gr + [first] + part + second + third:
        c.wait_send()
    for k in range(1, 8):
        forward(k).wait_send()


def opm(lt, rt, pd, rc, wo, live):
    sd = jax.ShapeDtypeStruct
    vm = pl.BlockSpec(memory_space=pltpu.VMEM)
    chunk = (128, N)
    V = pltpu.VMEM
    dma = pltpu.SemaphoreType.DMA((8,))
    return pl.pallas_call(
        opm_kernel,
        in_specs=[vm] * 6,
        out_specs=[vm] * 2,
        out_shape=[sd((4, CW, N), bf16)] * 2,
        scratch_shapes=[V((1024, 1024), bf16), V((2048, 1024), bf16), V((1024, 2048), bf16),
                        V((8, *chunk), bf16), V((16, *chunk), bf16)] + [V((8, *chunk), bf16)] * 6
        + [V(chunk, f32)] * 2 + [dma] * 12,
        compiler_params=pltpu.CompilerParams(vmem_limit_bytes=60 * 1024 * 1024, collective_id=1, has_side_effects=True),
        name="outer_product",
        cost_estimate=pl.CostEstimate(flops=10_000_000_000, bytes_accessed=10_000_000, transcendentals=0),
    )(lt, rt, pd, rc, wo, live)


def on_device(msa, present, pair, upstream, wq, wk, wv, wg, we, wl, wr, wo):
    def by_column(a):
        return a.transpose(1, 0, 2).reshape(8, 4, 64, F)

    def by_row(a):
        return a.reshape(32, 64, F).transpose(1, 0, 2)

    live = jnp.pad(present.astype(bf16), ((0, 0), (0, 96)))
    pd = pair.reshape(32, 2, 8, 4, CZ).transpose(2, 1, 3, 0, 4)
    x, p, o, g, at, lt, rt, up, pd, recip, livet = fwd(
        by_column(msa), by_column(upstream), pd, live, wq, wk, wv, wg, we, wl, wr)
    lg, rg = opm(lt.reshape(4 * CW, N), rt.reshape(4 * CW, N), pd.reshape(-1, CZ), recip, wo, livet)
    grad, inter = bwd(x, up, at, lg, rg, p, o, g, wq, wk, wv, wg, we, wl, wr)
    return by_row(grad), by_row(inter)


def solution(mesh):
    rows = P("dep", "res", None)
    in_specs = (rows, P("dep", "res"), P("res", "dep", None), rows) + (P(),) * 8
    return jax.shard_map(on_device, mesh=mesh, in_specs=in_specs, out_specs=(rows, rows), check_vma=False)
```

```python
import jax
import jax.numpy as jnp
from jax import lax
from jax.experimental import pallas as pl
from jax.experimental.pallas import tpu as pltpu
from jax.sharding import PartitionSpec as P

F = 256
H = 8
DH = 32
N = 512
CW = 32
CZ = 128
EPS = 1e-05
BIG = 1e9
f32 = jnp.float32
bf16 = jnp.bfloat16
SCALE = DH ** (-0.5)
NT = (((1,), (1,)), ((), ()))


def mm(a, b):
    return jnp.dot(a, b, preferred_element_type=f32)


def mmt(a, b):
    return lax.dot_general(a, b, NT, preferred_element_type=f32)


def norm(v, axis):
    c = v - jnp.mean(v, axis, keepdims=True)
    inv = lax.rsqrt(jnp.mean(c * c, axis, keepdims=True) + EPS)
    return c * inv, inv


def spread(rows, h, extra):
    top = (h % 4) * DH
    parts = []
    if top:
        parts.append(jnp.zeros((top, N), bf16))
    parts.append(rows)
    if top < 96:
        parts.append(jnp.zeros((96 - top, N), bf16))
    parts.append(extra)
    return jnp.concatenate(parts, axis=0)


MESH = pl.DeviceIdType.MESH


def remote(src, dst, send, recv, dep, res):
    return pltpu.make_async_remote_copy(src_ref=src, dst_ref=dst, send_sem=send, recv_sem=recv,
                                        device_id={"dep": dep, "res": res}, device_id_type=MESH)


def greet(peers):
    bar = pltpu.get_barrier_semaphore()
    for dep, res in peers:
        pl.semaphore_signal(bar, inc=1, device_id={"dep": dep, "res": res}, device_id_type=MESH)
    pl.semaphore_wait(bar, len(peers))


def fwd_kernel(hx, ux, px, live_in, wq, wk, wv, wg, we, wl, wr,
               x_ref, p_ref, o_ref, g_ref, a_ref, l_ref, r_ref, up_out, pd_out, rc_ref, live_out,
               wt, bias_s, xbuf, lbuf, livet, jbuf, mine, ustage, pstage,
               xs, xr, us, ur, ps, pr, ls, lr, js, jr, own):
    k = pl.program_id(0)
    d = lax.axis_index("dep")
    r = lax.axis_index("res")

    def dep_at(n):
        return lax.rem(d + n, 8)

    def res_at(n):
        return lax.rem(r + n, 16)

    def x_copy(c, n):
        return remote(hx.at[dep_at(n), c], xbuf.at[c, d], xs.at[c, n], xr.at[c, n], dep_at(n), r)

    def up_copy(c, n):
        return remote(ux.at[dep_at(n), c], up_out.at[d, c], us.at[c, n], ur.at[c, n], dep_at(n), r)

    def pd_copy(n):
        return remote(px.at[dep_at(n)], pd_out.at[d], ps.at[n], pr.at[n], dep_at(n), r)

    def live_copy(n):
        return remote(live_in, lbuf.at[d], ls.at[n], lr.at[n], dep_at(n), r)

    def row_copy(n):
        return remote(mine, jbuf.at[r], js.at[n], jr.at[n], d, res_at(n))

    def own_x(c):
        return pltpu.make_async_copy(hx.at[d, c], xbuf.at[c, d], own.at[c])

    own_up = pltpu.make_async_copy(ux.at[d], ustage, own.at[4])
    own_pd = pltpu.make_async_copy(px.at[d], pstage, own.at[5])
    own_up2 = pltpu.make_async_copy(ustage, up_out.at[d], own.at[6])
    own_pd2 = pltpu.make_async_copy(pstage, pd_out.at[d], own.at[7])

    @pl.when(k == 0)
    def _():
        for c in range(4):
            own_x(c).start()
        own_up.start()
        own_pd.start()
        greet([(dep_at(n), r) for n in range(1, 8)] + [(d, res_at(n)) for n in range(1, 16)])
        for n in range(1, 8):
            live_copy(n).start()
        for n in range(1, 8):
            x_copy(0, n).start()
        lbuf[d] = live_in[...]
        for n, w in enumerate((wq, wv, wg, we)):
            wt[n] = w[...].T
        for n in range(1, 8):
            live_copy(n).wait_recv()
        live = lbuf[...].reshape(N, 128).astype(f32)
        bias_s[...] = ((live - 1.0) * BIG).astype(bf16)
        livet[...] = live.T
        rows = [livet[pl.ds(4 * d + n, 1), :] for n in range(4)]
        held = jnp.concatenate(rows + [jnp.zeros((4, N), f32)], axis=0)
        mine[...] = held
        live_out[...] = held
        jbuf[r] = held
        for n in range(1, 16):
            row_copy(n).start()
        for n in range(1, 8):
            x_copy(0, n).wait_send()
        for n in range(1, 8):
            x_copy(1, n).start()

    @pl.when(k == 1)
    def _():
        for n in range(1, 8):
            x_copy(3, n).start()
        own_up.wait()
        own_pd.wait()
        own_up2.start()
        own_pd2.start()

    @pl.when(k == 2)
    def _():
        for n in range(1, 8):
            up_copy(0, n).start()

    @pl.when(k == 3)
    def _():
        for c in (2, 3):
            for n in range(1, 8):
                up_copy(c, n).start()
        for n in range(1, 16):
            row_copy(n).wait_recv()
        counts = mm(jbuf[...].reshape(128, N).astype(bf16), lbuf[...].reshape(N, 128))
        rec = 1.0 / (0.001 + counts)
        for n in range(8):
            pieces = []
            for j in range(8):
                at = 16 * n + 8 * (j // 4) + j % 4
                pieces.append(rec[at:at + 1, :CW])
            rc_ref[n:n + 1, :] = jnp.concatenate(pieces, axis=1)

    own_x(k).wait()
    for n in range(1, 8):
        x_copy(k, n).wait_recv()
    xin = xbuf[k].reshape(N, F)
    x_ref[...] = xin.reshape(x_ref.shape)
    xhat, _ = norm(xin.astype(f32), 1)
    xb = xhat.astype(bf16)
    xbt = xb.T
    qt = (mm(wt[0], xbt) * SCALE).astype(bf16)
    vt = mm(wt[1], xbt).astype(bf16)
    kk = mm(xb, wk[...]).astype(bf16)
    gt = jax.nn.sigmoid(mm(wt[2], xbt))
    g_ref[0] = gt
    extra = (lax.broadcasted_iota(jnp.int32, (128, N), 0) == 4 * d + k).astype(f32).astype(bf16)
    bias = bias_s[...]
    for h in range(H):
        if h == 4:
            @pl.when(k == 0)
            def _():
                for n in range(1, 8):
                    x_copy(2, n).start()

            @pl.when(k == 1)
            def _():
                for n in range(1, 8):
                    pd_copy(n).start()

            @pl.when(k == 2)
            def _():
                for n in range(1, 8):
                    up_copy(1, n).start()
        grp = h // 4
        lhs = jnp.concatenate([kk[:, 128 * grp:128 * grp + 128], bias], axis=1)
        st = mm(lhs, spread(qt[DH * h:DH * h + DH], h, extra))
        m = jnp.max(st, 0, keepdims=True)
        e = jnp.exp(st - m)
        s = jnp.sum(e, 0, keepdims=True)
        p = (e * (1.0 / s)).astype(bf16)
        p_ref[0, h] = p
        o_ref[0, pl.ds(DH * h, DH), :] = mm(vt[DH * h:DH * h + DH], p)
    gated = (gt * o_ref[0]).astype(bf16)
    up = mm(wt[3], gated)
    after = (xin.T.astype(f32) + up).astype(bf16)
    a_ref[0] = after
    yhat, _ = norm(after.astype(f32), 0)
    yb = yhat.astype(bf16)
    live = livet[pl.ds(4 * d + k, 1), :]
    l_ref[0] = (mm(wl[...], yb) * live).astype(bf16)
    r_ref[0] = (mm(wr[...], yb) * live).astype(bf16)

    @pl.when(k == 3)
    def _():
        for n in range(1, 8):
            pd_copy(n).wait_recv()
            for c in range(4):
                up_copy(c, n).wait_recv()
        own_up2.wait()
        own_pd2.wait()
        for n in range(1, 8):
            live_copy(n).wait_send()
            pd_copy(n).wait_send()
            for c in range(4):
                up_copy(c, n).wait_send()
                if c:
                    x_copy(c, n).wait_send()
        for n in range(1, 16):
            row_copy(n).wait_send()


def bwd_kernel(x_ref, up_ref, at_ref, lg_ref, rg_ref, p_ref, o_ref, g_ref, wq, wk, wv, wg, we, wl, wr,
               out_g, out_i, wkt, acc_q, dt_s, sbuf, ss, rs, own):
    k = pl.program_id(0)
    d = lax.axis_index("dep")
    r = lax.axis_index("res")
    outs = (out_g, out_i)

    def dep_at(n):
        return lax.rem(d + n, 8)

    def send(which, c, n):
        return remote(sbuf.at[which, c, dep_at(n)], outs[which].at[d, c],
                      ss.at[which, c, n], rs.at[which, c, n], dep_at(n), r)

    def keep(which, c):
        return pltpu.make_async_copy(sbuf.at[which, c, d], outs[which].at[d, c], own.at[which, c])

    def ship(which, c, value):
        sbuf[which, c] = value.T.reshape(8, 64, F)
        for n in range(1, 8):
            send(which, c, n).start()
        keep(which, c).start()

    @pl.when(k == 0)
    def _():
        wkt[...] = wk[...].T
        wlt, wrt = wl[...].T, wr[...].T
        greet([(dep_at(n), r) for n in range(1, 8)])
        for c in range(4):
            yhat, yinv = norm(at_ref[c].astype(f32), 0)
            dy = mm(wlt, lg_ref[c]) + mm(wrt, rg_ref[c])
            m1 = jnp.mean(dy, 0, keepdims=True)
            m2 = jnp.mean(dy * yhat, 0, keepdims=True)
            upt = up_ref[:, c].reshape(N, F).T.astype(f32)
            dt_s[c] = (yinv * (dy - m1 - yhat * m2) + upt).astype(bf16)
            ship(1, c, dt_s[c])

    xin = x_ref[...].reshape(N, F)
    xhat, _ = norm(xin.astype(f32), 1)
    xb = xhat.astype(bf16)
    xbt = xb.T
    q = (mm(xb, wq[...]) * SCALE).astype(bf16)
    v = mm(xb, wv[...]).astype(bf16)
    kt = mm(wkt[...], xbt).astype(bf16)
    gt = g_ref[0]
    ot = o_ref[0]
    dt = dt_s[k]
    dg = mm(we[...], dt).astype(bf16).astype(f32)
    dot_ = (dg * gt).astype(bf16)
    dpre = (dg * ot * gt * (1.0 - gt)).astype(bf16)
    do = dot_.T
    prod = dot_.astype(f32) * ot
    row = lax.broadcasted_iota(jnp.int32, (128, N), 0)
    col = lax.broadcasted_iota(jnp.int32, (N, 128), 1)
    ones = (col < 2).astype(f32).astype(bf16)
    lane = lax.broadcasted_iota(jnp.int32, (N, F), 1) // DH
    dk = jnp.zeros((N, F), f32)
    dv = jnp.zeros((N, F), f32)
    for h in range(H):
        grp = h // 4
        sl = slice(DH * h, DH * h + DH)
        dd = -jnp.sum(prod[sl], 0, keepdims=True)
        hi = dd.astype(bf16).astype(f32)
        lo = dd - hi
        extra = jnp.where(row == 0, hi, jnp.where(row == 1, lo, 0.0)).astype(bf16)
        lhs = jnp.concatenate([v[:, 128 * grp:128 * grp + 128], ones], axis=1)
        dp = mm(lhs, spread(dot_[sl], h, extra))
        p = p_ref[0, h]
        ds = (p.astype(f32) * dp).astype(bf16)
        mask = lane == h
        zero = jnp.zeros((), bf16)
        dv = dv + mm(p, jnp.where(mask, do, zero))
        dk = dk + mm(ds, jnp.where(mask, q, zero))
        acc_q[sl, :] = mm(kt[sl], ds)
    dq = (acc_q[...].astype(bf16).astype(f32) * SCALE).astype(bf16)
    dx = (mm(wq[...], dq) + mm(wg[...], dpre)
          + mmt(wk[...], dk.astype(bf16)) + mmt(wv[...], dv.astype(bf16)))
    dx = dx.astype(bf16).astype(f32)
    xt = xin.T.astype(f32)
    xh, inv = norm(xt, 0)
    m1 = jnp.mean(dx, 0, keepdims=True)
    m2 = jnp.mean(dx * xh, 0, keepdims=True)
    dln = (inv * (dx - m1 - xh * m2)).astype(bf16)
    out = (dt.astype(f32) + dln.astype(f32)).astype(bf16)
    ship(0, k, out)

    @pl.when(k == 3)
    def _():
        for which in range(2):
            for c in range(4):
                keep(which, c).wait()
                for n in range(1, 8):
                    send(which, c, n).wait_recv()
                    send(which, c, n).wait_send()


def whole(shape):
    return pl.BlockSpec(shape, lambda k: (0,) * len(shape))


def percol(shape):
    return pl.BlockSpec((1, *shape), lambda k: (k,) + (0,) * len(shape))


COLS = pl.BlockSpec((8, 1, 64, F), lambda k: (0, k, 0, 0))
ANY = pl.BlockSpec(memory_space=pl.ANY)


def fwd(hx, ux, px, live, wq, wk, wv, wg, we, wl, wr):
    sd = jax.ShapeDtypeStruct
    V = pltpu.VMEM
    dma = pltpu.SemaphoreType.DMA
    return pl.pallas_call(
        fwd_kernel,
        grid=(4,),
        in_specs=[ANY] * 3 + [whole((64, 128))] + [whole((F, F))] * 5 + [whole((CW, F))] * 2,
        out_specs=[COLS, percol((H, N, N)), percol((F, N)), percol((F, N)), percol((F, N)), percol((CW, N)),
                   percol((CW, N)), ANY, ANY, whole((8, 256)), whole((8, N))],
        out_shape=[sd((8, 4, 64, F), bf16), sd((4, H, N, N), bf16), sd((4, F, N), f32), sd((4, F, N), f32),
                   sd((4, F, N), bf16), sd((4, CW, N), bf16), sd((4, CW, N), bf16),
                   sd(ux.shape, bf16), sd(px.shape, bf16), sd((8, 256), f32), sd((8, N), f32)],
        scratch_shapes=[V((4, F, F), bf16), V((N, 128), bf16), V((4, 8, 64, F), bf16),
                        V((8, 64, 128), bf16), V((128, N), f32), V((16, 8, N), f32), V((8, N), f32), V(ux.shape[1:], bf16),
                        V(px.shape[1:], bf16), dma((4, 8)), dma((4, 8)), dma((4, 8)), dma((4, 8))] + [dma((8,))] * 4 + [dma((16,))] * 2 + [dma((8,))],
        compiler_params=pltpu.CompilerParams(vmem_limit_bytes=60 * 1024 * 1024, collective_id=2, has_side_effects=True,
                                             dimension_semantics=("arbitrary",)),
        name="attention_forward",
    )(hx, ux, px, live, wq, wk, wv, wg, we, wl, wr)


def bwd(x, up, at, lg, rg, p, o, g, wq, wk, wv, wg, we, wl, wr):
    sd = jax.ShapeDtypeStruct
    V = pltpu.VMEM
    dma = pltpu.SemaphoreType.DMA
    return pl.pallas_call(
        bwd_kernel,
        grid=(4,),
        in_specs=[COLS, whole((8, 4, 64, F)), whole((4, F, N)), whole((4, CW, N)), whole((4, CW, N)), percol((H, N, N)), percol((F, N)),
                  percol((F, N))] + [whole((F, F))] * 5 + [whole((CW, F))] * 2,
        out_specs=[ANY, ANY],
        out_shape=[sd((8, 4, 64, F), bf16)] * 2,
        scratch_shapes=[V((F, F), bf16), V((F, N), f32), V((4, F, N), bf16), V((2, 4, 8, 64, F), bf16),
                        dma((2, 4, 8)), dma((2, 4, 8)), dma((2, 4))],
        compiler_params=pltpu.CompilerParams(vmem_limit_bytes=60 * 1024 * 1024, collective_id=3, has_side_effects=True,
                                             dimension_semantics=("arbitrary",)),
        name="attention_backward",
    )(x, up, at, lg, rg, p, o, g, wq, wk, wv, wg, we, wl, wr)


def opm_kernel(lt, rt, pd, rc, wo, live, lo, ro,
               perm, oc1, oc2, lbuf, rbuf, lsend, lrecv, psend, precv, rsend, rrecv, lacc, racc,
               ls, lr, rs, rr, fs, fr, ps, pr, s2, r2, s3, r3):
    d = lax.axis_index("dep")
    r = lax.axis_index("res")
    core = lax.rem(r, 2)
    chip = r // 2
    partner = 2 * chip + 1 - core

    def dep_at(k):
        return lax.rem(d + k, 8)

    def chip_at(k):
        return lax.rem(chip + k, 8)

    greet([(dep_at(k), r) for k in range(1, 8)]
          + [(d, 2 * chip_at(k) + core) for k in range(1, 8)] + [(d, partner)])

    gl = [remote(lt, lbuf.at[d], ls.at[k], lr.at[k], dep_at(k), r) for k in range(1, 8)]
    gr = [remote(rt, rbuf.at[r], rs.at[k], rr.at[k], d, 2 * chip_at(k) + core) for k in range(1, 8)]
    first = remote(rt, rbuf.at[r], fs.at[0], fr.at[0], d, partner)
    for a, b in zip(gl, gr):
        b.start()
        a.start()
    first.start()
    lbuf[d] = lt[...]
    rbuf[r] = rt[...]

    a = lax.broadcasted_iota(jnp.int32, (1024, 1024), 0)
    b = lax.broadcasted_iota(jnp.int32, (1024, 1024), 1)
    hit = ((a // CW) == (b % CW)) & ((a % CW) == (b // CW))
    perm[...] = hit.astype(f32).astype(bf16)

    def forward(k):
        slot = 2 * lax.rem(chip + 8 - k, 8) + core
        return remote(rbuf.at[slot], rbuf.at[slot], fs.at[k], fr.at[k], d, partner)

    def outer_step(n, carry):
        at = pl.multiple_of(256 * n, 256)
        z = (mmt(wo[...], pd[pl.ds(at, 256), :]) * rc[pl.ds(n, 1), :]).astype(bf16)
        rows = []
        for j in range(8):
            rows.append(jnp.concatenate([z[CW * c:CW * c + CW, CW * j:CW * j + CW] for c in range(CW)], axis=1))
        y = mm(jnp.concatenate(rows, axis=0), perm[...]).astype(bf16)
        oc1[pl.ds(at, 256), :] = y
        oc2[:, pl.ds(at, 256)] = y.T

        @pl.when(n > 0)
        def _():
            remote(rt, rbuf.at[r], rs.at[n], rr.at[n], d, partner).wait_recv()
            forward(n).start()
        return carry

    lax.fori_loop(0, 8, outer_step, 0)
    for c in gl:
        c.wait_recv()
    lall = lbuf[...].reshape(1024, N)
    part = []
    for k in [1, 2, 3, 4, 5, 6, 7, 0]:
        q = chip_at(k)
        at = pl.multiple_of(256 * q + 128 * (1 - core), 128)
        psend[k] = mm(oc1[pl.ds(at, 128), :], lall).astype(bf16)
        c = remote(psend.at[k], precv.at[k], ps.at[k], pr.at[k], d, partner)
        c.start()
        part.append(c)
    second = []
    for k in [1, 2, 3, 4, 5, 6, 7, 0]:
        q = chip_at(k)
        at = pl.multiple_of(256 * q + 128 * core, 128)
        own = mm(oc1[pl.ds(at, 128), :], lall)
        remote(psend.at[k], precv.at[k], ps.at[k], pr.at[k], d, partner).wait_recv()
        own = own + precv[k].astype(f32)
        if k:
            rsend[k] = own.astype(bf16)
            c = remote(rsend.at[k], rrecv.at[k], s2.at[k], r2.at[k], d, 2 * q + core)
            c.start()
            second.append(c)
        else:
            racc[...] = own
    first.wait_recv()
    for k in range(1, 8):
        forward(k).wait_recv()
    rall = rbuf[...].reshape(2048, N)
    third = []
    for k in [1, 2, 3, 4, 5, 6, 7, 0]:
        at = pl.multiple_of(128 * dep_at(k), 128)
        own = mm(oc2[pl.ds(at, 128), :], rall)
        if k:
            lsend[k] = own.astype(bf16)
            c = remote(lsend.at[k], lrecv.at[k], s3.at[k], r3.at[k], dep_at(k), r)
            c.start()
            third.append(c)
        else:
            lacc[...] = own
    for c in second:
        c.wait_recv()
    racc[...] += jnp.sum(rrecv[1:8].astype(f32), 0)
    for n in range(4):
        ro[n] = (racc[CW * n:CW * n + CW, :] * live[n:n + 1, :]).astype(bf16)
    for c in third:
        c.wait_recv()
    lacc[...] += jnp.sum(lrecv[1:8].astype(f32), 0)
    for n in range(4):
        lo[n] = (lacc[CW * n:CW * n + CW, :] * live[n:n + 1, :]).astype(bf16)
    for c in gl + gr + [first] + part + second + third:
        c.wait_send()
    for k in range(1, 8):
        forward(k).wait_send()


def opm(lt, rt, pd, rc, wo, live):
    sd = jax.ShapeDtypeStruct
    vm = pl.BlockSpec(memory_space=pltpu.VMEM)
    chunk = (128, N)
    V = pltpu.VMEM
    dma = pltpu.SemaphoreType.DMA((8,))
    return pl.pallas_call(
        opm_kernel,
        in_specs=[vm] * 6,
        out_specs=[vm] * 2,
        out_shape=[sd((4, CW, N), bf16)] * 2,
        scratch_shapes=[V((1024, 1024), bf16), V((2048, 1024), bf16), V((1024, 2048), bf16),
                        V((8, *chunk), bf16), V((16, *chunk), bf16)] + [V((8, *chunk), bf16)] * 6
        + [V(chunk, f32)] * 2 + [dma] * 12,
        compiler_params=pltpu.CompilerParams(vmem_limit_bytes=60 * 1024 * 1024, collective_id=1, has_side_effects=True),
        name="outer_product",
        cost_estimate=pl.CostEstimate(flops=10_000_000_000, bytes_accessed=10_000_000, transcendentals=0),
    )(lt, rt, pd, rc, wo, live)


def on_device(msa, present, pair, upstream, wq, wk, wv, wg, we, wl, wr, wo):
    def by_column(a):
        return a.transpose(1, 0, 2).reshape(8, 4, 64, F)

    def by_row(a):
        return a.reshape(32, 64, F).transpose(1, 0, 2)

    live = jnp.pad(present.astype(bf16), ((0, 0), (0, 96)))
    pd = pair.reshape(32, 2, 8, 4, CZ).transpose(2, 1, 3, 0, 4)
    x, p, o, g, at, lt, rt, up, pd, recip, livet = fwd(
        by_column(msa), by_column(upstream), pd, live, wq, wk, wv, wg, we, wl.T, wr.T)
    lg, rg = opm(lt.reshape(4 * CW, N), rt.reshape(4 * CW, N), pd.reshape(-1, CZ), recip, wo, livet)
    grad, inter = bwd(x, up, at, lg, rg, p, o, g, wq, wk, wv, wg, we, wl.T, wr.T)
    return by_row(grad), by_row(inter)


def solution(mesh):
    rows = P("dep", "res", None)
    in_specs = (rows, P("dep", "res"), P("res", "dep", None), rows) + (P(),) * 8
    return jax.shard_map(on_device, mesh=mesh, in_specs=in_specs, out_specs=(rows, rows), check_vma=False)
```

```python
import jax
import jax.numpy as jnp
from jax import lax
from jax.experimental import pallas as pl
from jax.experimental.pallas import tpu as pltpu
from jax.sharding import PartitionSpec as P

F = 256
H = 8
DH = 32
N = 512
CW = 32
CZ = 128
EPS = 1e-05
BIG = 1e9
f32 = jnp.float32
bf16 = jnp.bfloat16
SCALE = DH ** (-0.5)
NT = (((1,), (1,)), ((), ()))


def mm(a, b):
    return jnp.dot(a, b, preferred_element_type=f32)


def mmt(a, b):
    return lax.dot_general(a, b, NT, preferred_element_type=f32)


def norm(v, axis):
    c = v - jnp.mean(v, axis, keepdims=True)
    inv = lax.rsqrt(jnp.mean(c * c, axis, keepdims=True) + EPS)
    return c * inv, inv


def spread(rows, h, extra):
    top = (h % 4) * DH
    parts = []
    if top:
        parts.append(jnp.zeros((top, N), bf16))
    parts.append(rows)
    if top < 96:
        parts.append(jnp.zeros((96 - top, N), bf16))
    parts.append(extra)
    return jnp.concatenate(parts, axis=0)


MESH = pl.DeviceIdType.MESH


def remote(src, dst, send, recv, dep, res):
    return pltpu.make_async_remote_copy(src_ref=src, dst_ref=dst, send_sem=send, recv_sem=recv,
                                        device_id={"dep": dep, "res": res}, device_id_type=MESH)


def greet(peers):
    bar = pltpu.get_barrier_semaphore()
    for dep, res in peers:
        pl.semaphore_signal(bar, inc=1, device_id={"dep": dep, "res": res}, device_id_type=MESH)
    pl.semaphore_wait(bar, len(peers))


def fwd_kernel(hx, ux, px, live_in, wq, wk, wv, wg, we, wl, wr,
               x_ref, p_ref, o_ref, g_ref, a_ref, l_ref, r_ref, up_out, pd_out, rc_ref, live_out,
               wt, bias_s, xbuf, lbuf, livet, jbuf, mine, ustage, pstage,
               xs, xr, us, ur, ps, pr, ls, lr, js, jr, own):
    k = pl.program_id(0)
    d = lax.axis_index("dep")
    r = lax.axis_index("res")

    def dep_at(n):
        return lax.rem(d + n, 8)

    def res_at(n):
        return lax.rem(r + n, 16)

    def x_copy(c, n):
        return remote(hx.at[dep_at(n), c], xbuf.at[c, d], xs.at[c, n], xr.at[c, n], dep_at(n), r)

    def up_copy(c, n):
        return remote(ux.at[dep_at(n), c], up_out.at[d, c], us.at[c, n], ur.at[c, n], dep_at(n), r)

    def pd_copy(n):
        return remote(px.at[dep_at(n)], pd_out.at[d], ps.at[n], pr.at[n], dep_at(n), r)

    def live_copy(n):
        return remote(live_in, lbuf.at[d], ls.at[n], lr.at[n], dep_at(n), r)

    def row_copy(n):
        return remote(mine, jbuf.at[r], js.at[n], jr.at[n], d, res_at(n))

    def own_x(c):
        return pltpu.make_async_copy(hx.at[d, c], xbuf.at[c, d], own.at[c])

    own_up = pltpu.make_async_copy(ux.at[d], ustage, own.at[4])
    own_pd = pltpu.make_async_copy(px.at[d], pstage, own.at[5])
    own_up2 = pltpu.make_async_copy(ustage, up_out.at[d], own.at[6])
    own_pd2 = pltpu.make_async_copy(pstage, pd_out.at[d], own.at[7])

    @pl.when(k == 0)
    def _():
        for c in range(4):
            own_x(c).start()
        own_up.start()
        own_pd.start()
        greet([(dep_at(n), r) for n in range(1, 8)] + [(d, res_at(n)) for n in range(1, 16)])
        for n in range(1, 8):
            live_copy(n).start()
        for n in range(1, 8):
            x_copy(0, n).start()
        lbuf[d] = live_in[...]
        for n, w in enumerate((wq, wv, wg, we)):
            wt[n] = w[...].T
        for n in range(1, 8):
            live_copy(n).wait_recv()
        live = lbuf[...].reshape(N, 128).astype(f32)
        bias_s[...] = ((live - 1.0) * BIG).astype(bf16)
        livet[...] = live.T
        rows = [livet[pl.ds(4 * d + n, 1), :] for n in range(4)]
        held = jnp.concatenate(rows + [jnp.zeros((4, N), f32)], axis=0)
        mine[...] = held
        live_out[...] = held
        jbuf[r] = held
        for n in range(1, 16):
            row_copy(n).start()
        for n in range(1, 8):
            x_copy(0, n).wait_send()
        for n in range(1, 8):
            x_copy(1, n).start()

    @pl.when(k == 1)
    def _():
        for n in range(1, 8):
            x_copy(3, n).start()
        own_up.wait()
        own_pd.wait()
        own_up2.start()
        own_pd2.start()

    @pl.when(k == 2)
    def _():
        for n in range(1, 8):
            up_copy(0, n).start()

    @pl.when(k == 3)
    def _():
        for c in (2, 3):
            for n in range(1, 8):
                up_copy(c, n).start()
        for n in range(1, 16):
            row_copy(n).wait_recv()
        counts = mm(jbuf[...].reshape(128, N).astype(bf16), lbuf[...].reshape(N, 128))
        rec = 1.0 / (0.001 + counts)
        for n in range(8):
            pieces = []
            for j in range(8):
                at = 16 * n + 8 * (j // 4) + j % 4
                pieces.append(rec[at:at + 1, :CW])
            rc_ref[n:n + 1, :] = jnp.concatenate(pieces, axis=1)

    own_x(k).wait()
    for n in range(1, 8):
        x_copy(k, n).wait_recv()
    xin = xbuf[k].reshape(N, F)
    x_ref[...] = xin.reshape(x_ref.shape)
    xhat, _ = norm(xin.astype(f32), 1)
    xb = xhat.astype(bf16)
    xbt = xb.T
    qt = (mm(wt[0], xbt) * SCALE).astype(bf16)
    vt = mm(wt[1], xbt).astype(bf16)
    kk = mm(xb, wk[...]).astype(bf16)
    gt = jax.nn.sigmoid(mm(wt[2], xbt))
    g_ref[0] = gt
    extra = (lax.broadcasted_iota(jnp.int32, (128, N), 0) == 4 * d + k).astype(f32).astype(bf16)
    bias = bias_s[...]
    for h in range(H):
        if h == 4:
            @pl.when(k == 0)
            def _():
                for n in range(1, 8):
                    x_copy(2, n).start()

            @pl.when(k == 1)
            def _():
                for n in range(1, 8):
                    pd_copy(n).start()

            @pl.when(k == 2)
            def _():
                for n in range(1, 8):
                    up_copy(1, n).start()
        grp = h // 4
        lhs = jnp.concatenate([kk[:, 128 * grp:128 * grp + 128], bias], axis=1)
        st = mm(lhs, spread(qt[DH * h:DH * h + DH], h, extra))
        m = jnp.max(st, 0, keepdims=True)
        e = jnp.exp(st - m)
        s = jnp.sum(e, 0, keepdims=True)
        p = (e * (1.0 / s)).astype(bf16)
        p_ref[0, h] = p
        o_ref[0, pl.ds(DH * h, DH), :] = mm(vt[DH * h:DH * h + DH], p)
    gated = (gt * o_ref[0]).astype(bf16)
    up = mm(wt[3], gated)
    after = (xin.T.astype(f32) + up).astype(bf16)
    a_ref[0] = after
    yhat, _ = norm(after.astype(f32), 0)
    yb = yhat.astype(bf16)
    live = livet[pl.ds(4 * d + k, 1), :]
    l_ref[0] = (mm(wl[...], yb) * live).astype(bf16)
    r_ref[0] = (mm(wr[...], yb) * live).astype(bf16)

    @pl.when(k == 3)
    def _():
        for n in range(1, 8):
            pd_copy(n).wait_recv()
            for c in range(4):
                up_copy(c, n).wait_recv()
        own_up2.wait()
        own_pd2.wait()
        for n in range(1, 8):
            live_copy(n).wait_send()
            pd_copy(n).wait_send()
            for c in range(4):
                up_copy(c, n).wait_send()
                if c:
                    x_copy(c, n).wait_send()
        for n in range(1, 16):
            row_copy(n).wait_send()


def bwd_kernel(x_ref, up_ref, at_ref, lg_ref, rg_ref, p_ref, o_ref, g_ref, wq, wk, wv, wg, we, wl, wr,
               out_g, out_i, wkt, acc_q, dt_s, sbuf, ss, rs, own):
    k = pl.program_id(0)
    d = lax.axis_index("dep")
    r = lax.axis_index("res")
    outs = (out_g, out_i)

    def dep_at(n):
        return lax.rem(d + n, 8)

    def send(which, c, n):
        return remote(sbuf.at[which, c, dep_at(n)], outs[which].at[d, c],
                      ss.at[which, c, n], rs.at[which, c, n], dep_at(n), r)

    def keep(which, c):
        return pltpu.make_async_copy(sbuf.at[which, c, d], outs[which].at[d, c], own.at[which, c])

    def ship(which, c, value):
        sbuf[which, c] = value.T.reshape(8, 64, F)
        for n in range(1, 8):
            send(which, c, n).start()
        keep(which, c).start()

    @pl.when(k == 0)
    def _():
        wkt[...] = wk[...].T
        wlt, wrt = wl[...].T, wr[...].T
        greet([(dep_at(n), r) for n in range(1, 8)])
        for c in range(4):
            yhat, yinv = norm(at_ref[c].astype(f32), 0)
            dy = mm(wlt, lg_ref[c]) + mm(wrt, rg_ref[c])
            m1 = jnp.mean(dy, 0, keepdims=True)
            m2 = jnp.mean(dy * yhat, 0, keepdims=True)
            upt = up_ref[:, c].reshape(N, F).T.astype(f32)
            dt_s[c] = (yinv * (dy - m1 - yhat * m2) + upt).astype(bf16)
            ship(1, c, dt_s[c])

    xin = x_ref[...].reshape(N, F)
    xhat, _ = norm(xin.astype(f32), 1)
    xb = xhat.astype(bf16)
    xbt = xb.T
    q = (mm(xb, wq[...]) * SCALE).astype(bf16)
    v = mm(xb, wv[...]).astype(bf16)
    kt = mm(wkt[...], xbt).astype(bf16)
    gt = g_ref[0]
    ot = o_ref[0]
    dt = dt_s[k]
    dg = mm(we[...], dt).astype(bf16).astype(f32)
    dot_ = (dg * gt).astype(bf16)
    dpre = (dg * ot * gt * (1.0 - gt)).astype(bf16)
    do = dot_.T
    prod = dot_.astype(f32) * ot
    row = lax.broadcasted_iota(jnp.int32, (128, N), 0)
    col = lax.broadcasted_iota(jnp.int32, (N, 128), 1)
    ones = (col < 2).astype(f32).astype(bf16)
    lane = lax.broadcasted_iota(jnp.int32, (N, F), 1) // DH
    dk = jnp.zeros((N, F), f32)
    dv = jnp.zeros((N, F), f32)
    for h in range(H):
        grp = h // 4
        sl = slice(DH * h, DH * h + DH)
        dd = -jnp.sum(prod[sl], 0, keepdims=True)
        hi = dd.astype(bf16).astype(f32)
        lo = dd - hi
        extra = jnp.where(row == 0, hi, jnp.where(row == 1, lo, 0.0)).astype(bf16)
        lhs = jnp.concatenate([v[:, 128 * grp:128 * grp + 128], ones], axis=1)
        dp = mm(lhs, spread(dot_[sl], h, extra))
        p = p_ref[0, h]
        ds = (p.astype(f32) * dp).astype(bf16)
        mask = lane == h
        zero = jnp.zeros((), bf16)
        dv = dv + mm(p, jnp.where(mask, do, zero))
        dk = dk + mm(ds, jnp.where(mask, q, zero))
        acc_q[sl, :] = mm(kt[sl], ds)
    dq = (acc_q[...].astype(bf16).astype(f32) * SCALE).astype(bf16)
    dx = (mm(wq[...], dq) + mm(wg[...], dpre)
          + mmt(wk[...], dk.astype(bf16)) + mmt(wv[...], dv.astype(bf16)))
    dx = dx.astype(bf16).astype(f32)
    xt = xin.T.astype(f32)
    xh, inv = norm(xt, 0)
    m1 = jnp.mean(dx, 0, keepdims=True)
    m2 = jnp.mean(dx * xh, 0, keepdims=True)
    dln = (inv * (dx - m1 - xh * m2)).astype(bf16)
    out = (dt.astype(f32) + dln.astype(f32)).astype(bf16)
    ship(0, k, out)

    @pl.when(k == 3)
    def _():
        for which in range(2):
            for c in range(4):
                keep(which, c).wait()
                for n in range(1, 8):
                    send(which, c, n).wait_recv()
                    send(which, c, n).wait_send()


def whole(shape):
    return pl.BlockSpec(shape, lambda k: (0,) * len(shape))


def percol(shape):
    return pl.BlockSpec((1, *shape), lambda k: (k,) + (0,) * len(shape))


COLS = pl.BlockSpec((8, 1, 64, F), lambda k: (0, k, 0, 0))
ANY = pl.BlockSpec(memory_space=pl.ANY)


def fwd(hx, ux, px, live, wq, wk, wv, wg, we, wl, wr):
    sd = jax.ShapeDtypeStruct
    V = pltpu.VMEM
    dma = pltpu.SemaphoreType.DMA
    return pl.pallas_call(
        fwd_kernel,
        grid=(4,),
        in_specs=[ANY] * 3 + [whole((64, 128))] + [whole((F, F))] * 5 + [whole((CW, F))] * 2,
        out_specs=[COLS, percol((H, N, N)), percol((F, N)), percol((F, N)), percol((F, N)), percol((CW, N)),
                   percol((CW, N)), ANY, ANY, whole((8, 256)), whole((8, N))],
        out_shape=[sd((8, 4, 64, F), bf16), sd((4, H, N, N), bf16), sd((4, F, N), f32), sd((4, F, N), f32),
                   sd((4, F, N), bf16), sd((4, CW, N), bf16), sd((4, CW, N), bf16),
                   sd(ux.shape, bf16), sd(px.shape, bf16), sd((8, 256), f32), sd((8, N), f32)],
        scratch_shapes=[V((4, F, F), bf16), V((N, 128), bf16), V((4, 8, 64, F), bf16),
                        V((8, 64, 128), bf16), V((128, N), f32), V((16, 8, N), f32), V((8, N), f32), V(ux.shape[1:], bf16),
                        V(px.shape[1:], bf16), dma((4, 8)), dma((4, 8)), dma((4, 8)), dma((4, 8))] + [dma((8,))] * 4 + [dma((16,))] * 2 + [dma((8,))],
        compiler_params=pltpu.CompilerParams(vmem_limit_bytes=60 * 1024 * 1024, collective_id=2, has_side_effects=True,
                                             dimension_semantics=("arbitrary",)),
        name="attention_forward",
    )(hx, ux, px, live, wq, wk, wv, wg, we, wl, wr)


def bwd(x, up, at, lg, rg, p, o, g, wq, wk, wv, wg, we, wl, wr):
    sd = jax.ShapeDtypeStruct
    V = pltpu.VMEM
    dma = pltpu.SemaphoreType.DMA
    return pl.pallas_call(
        bwd_kernel,
        grid=(4,),
        in_specs=[COLS, whole((8, 4, 64, F)), whole((4, F, N)), whole((4, CW, N)), whole((4, CW, N)), percol((H, N, N)), percol((F, N)),
                  percol((F, N))] + [whole((F, F))] * 5 + [whole((CW, F))] * 2,
        out_specs=[ANY, ANY],
        out_shape=[sd((8, 4, 64, F), bf16)] * 2,
        scratch_shapes=[V((F, F), bf16), V((F, N), f32), V((4, F, N), bf16), V((2, 4, 8, 64, F), bf16),
                        dma((2, 4, 8)), dma((2, 4, 8)), dma((2, 4))],
        compiler_params=pltpu.CompilerParams(vmem_limit_bytes=60 * 1024 * 1024, collective_id=3, has_side_effects=True,
                                             dimension_semantics=("arbitrary",)),
        name="attention_backward",
    )(x, up, at, lg, rg, p, o, g, wq, wk, wv, wg, we, wl, wr)


def opm_kernel(lt, rt, pd, rc, wo, live, lo, ro,
               perm, oc1, oc2, lbuf, rbuf, lsend, lrecv, psend, precv, rsend, rrecv, both, lkeep, lacc,
               ls, lr, rs, rr, fs, fr, ps, pr, s2, r2, s3, r3):
    d = lax.axis_index("dep")
    r = lax.axis_index("res")
    xl, z = d // 4, lax.rem(d, 4)
    y, xh, core = r // 4, lax.rem(r // 2, 2), lax.rem(r, 2)

    def dep_of(flip, step):
        return 4 * lax.rem(xl + flip, 2) + lax.rem(z + step + 4, 4)

    def chip_of(flip, step):
        return 2 * lax.rem(y + step + 4, 4) + lax.rem(xh + flip, 2)

    def res_of(flip, step):
        return 2 * chip_of(flip, step) + core

    partner = 2 * chip_of(0, 0) + 1 - core
    greet([(dep_of(0, n), r) for n in range(1, 4)] + [(dep_of(1, 0), r)]
          + [(d, res_of(0, n)) for n in range(1, 4)] + [(d, res_of(1, 0)), (d, partner)])

    def left_copy(n):
        if n == 0:
            return remote(lt, lbuf.at[d], ls.at[0], lr.at[0], dep_of(1, 0), r)
        if n < 4:
            return remote(lt, lbuf.at[d], ls.at[n], lr.at[n], dep_of(0, n), r)
        slot = dep_of(1, 0)
        return remote(lbuf.at[slot], lbuf.at[slot], ls.at[n], lr.at[n], dep_of(0, n - 3), r)

    def right_copy(n):
        if n == 0:
            return remote(rt, rbuf.at[r], rs.at[0], rr.at[0], d, res_of(1, 0))
        if n < 4:
            return remote(rt, rbuf.at[r], rs.at[n], rr.at[n], d, res_of(0, n))
        slot = res_of(1, 0)
        return remote(rbuf.at[slot], rbuf.at[slot], rs.at[n], rr.at[n], d, res_of(0, n - 3))

    def across(n):
        if n == 7:
            return remote(rt, rbuf.at[r], fs.at[7], fr.at[7], d, partner)
        slot = res_of(1, 0) if n == 0 else res_of(0, -n) if n < 4 else res_of(1, 3 - n)
        return remote(rbuf.at[slot], rbuf.at[slot], fs.at[n], fr.at[n], d, partner)

    for n in range(4):
        left_copy(n).start()
        right_copy(n).start()
    across(7).start()
    lbuf[d] = lt[...]
    rbuf[r] = rt[...]

    a = lax.broadcasted_iota(jnp.int32, (1024, 1024), 0)
    b = lax.broadcasted_iota(jnp.int32, (1024, 1024), 1)
    hit = ((a // CW) == (b % CW)) & ((a % CW) == (b // CW))
    perm[...] = hit.astype(f32).astype(bf16)

    def outer_step(n, carry):
        at = pl.multiple_of(256 * n, 256)
        zz = (mmt(wo[...], pd[pl.ds(at, 256), :]) * rc[pl.ds(n, 1), :]).astype(bf16)
        rows = []
        for j in range(8):
            rows.append(jnp.concatenate([zz[CW * c:CW * c + CW, CW * j:CW * j + CW] for c in range(CW)], axis=1))
        yy = mm(jnp.concatenate(rows, axis=0), perm[...]).astype(bf16)
        oc1[pl.ds(at, 256), :] = yy
        oc2[:, pl.ds(at, 256)] = yy.T

        @pl.when(n == 1)
        def _():
            left_copy(0).wait_recv()
            for i in range(4, 7):
                left_copy(i).start()

        @pl.when(n == 2)
        def _():
            right_copy(0).wait_recv()
            for i in range(4, 7):
                right_copy(i).start()
            across(0).start()

        @pl.when(n == 5)
        def _():
            for i in range(1, 4):
                right_copy(i).wait_recv()
                across(i).start()
        return carry

    lax.fori_loop(0, 8, outer_step, 0)
    for n in range(1, 7):
        left_copy(n).wait_recv()
    for n in range(4, 7):
        right_copy(n).wait_recv()
        across(n).start()

    order = [(1, 1), (1, 2), (1, 3), (1, 0), (0, 1), (0, 2), (0, 3), (0, 0)]

    def pass_over(i):
        return remote(psend.at[i], precv.at[i], ps.at[i], pr.at[i], d, partner)

    def right_part(i):
        target = res_of(1, 0) if i == 3 else res_of(0, order[i][1])
        return remote(rsend.at[i], rrecv.at[i], s2.at[i], r2.at[i], d, target)

    def left_part(i):
        target = dep_of(1, 0) if i == 3 else dep_of(0, order[i][1])
        return remote(lsend.at[i], lrecv.at[i], s3.at[i], r3.at[i], target, r)

    mine = pl.ds(pl.multiple_of(128 * core, 128), 128)
    theirs = pl.ds(pl.multiple_of(128 * (1 - core), 128), 128)
    lall = lbuf[...].reshape(1024, N)
    for i, (flip, step) in enumerate(order):
        at = pl.multiple_of(256 * chip_of(flip, step), 256)
        both[i] = mm(oc1[pl.ds(at, 256), :], lall)
        psend[i] = both[i, theirs, :].astype(bf16)
        pass_over(i).start()
    for i in range(8):
        pass_over(i).wait_recv()
        own = both[i, mine, :] + precv[i].astype(f32)
        if i in (3, 7):
            both[i, mine, :] = own
        else:
            rsend[i] = own.astype(bf16)
            right_part(i).start()
    for n in range(8):
        across(n).wait_recv()
    rall = rbuf[...].reshape(2048, N)
    for i, (flip, step) in enumerate(order):
        at = pl.multiple_of(128 * dep_of(flip, step), 128)
        own = mm(oc2[pl.ds(at, 128), :], rall)
        if i == 3:
            lkeep[...] = own
        elif i == 7:
            lacc[...] = own
        else:
            lsend[i] = own.astype(bf16)
            left_part(i).start()
    for i in range(3):
        right_part(i).wait_recv()
    rsend[3] = (both[3, mine, :] + jnp.sum(rrecv[0:3].astype(f32), 0)).astype(bf16)
    right_part(3).start()
    for i in range(3):
        left_part(i).wait_recv()
    lsend[3] = (lkeep[...] + jnp.sum(lrecv[0:3].astype(f32), 0)).astype(bf16)
    left_part(3).start()
    for i in range(3, 7):
        right_part(i).wait_recv()
    racc = both[7, mine, :] + jnp.sum(rrecv[3:7].astype(f32), 0)
    for n in range(4):
        ro[n] = (racc[CW * n:CW * n + CW, :] * live[n:n + 1, :]).astype(bf16)
    for i in range(3, 7):
        left_part(i).wait_recv()
    lsum = lacc[...] + jnp.sum(lrecv[3:7].astype(f32), 0)
    for n in range(4):
        lo[n] = (lsum[CW * n:CW * n + CW, :] * live[n:n + 1, :]).astype(bf16)
    for n in range(7):
        left_copy(n).wait_send()
        right_copy(n).wait_send()
        right_part(n).wait_send()
        left_part(n).wait_send()
    for n in range(8):
        across(n).wait_send()
        pass_over(n).wait_send()


def opm(lt, rt, pd, rc, wo, live):
    sd = jax.ShapeDtypeStruct
    vm = pl.BlockSpec(memory_space=pltpu.VMEM)
    chunk = (128, N)
    V = pltpu.VMEM
    dma = pltpu.SemaphoreType.DMA((8,))
    return pl.pallas_call(
        opm_kernel,
        in_specs=[vm] * 6,
        out_specs=[vm] * 2,
        out_shape=[sd((4, CW, N), bf16)] * 2,
        scratch_shapes=[V((1024, 1024), bf16), V((2048, 1024), bf16), V((1024, 2048), bf16),
                        V((8, *chunk), bf16), V((16, *chunk), bf16)] + [V((8, *chunk), bf16)] * 6
        + [V((8, 256, N), f32)] + [V(chunk, f32)] * 2 + [dma] * 12,
        compiler_params=pltpu.CompilerParams(vmem_limit_bytes=60 * 1024 * 1024, collective_id=1, has_side_effects=True),
        name="outer_product",
    )(lt, rt, pd, rc, wo, live)


def on_device(msa, present, pair, upstream, wq, wk, wv, wg, we, wl, wr, wo):
    def by_column(a):
        return a.transpose(1, 0, 2).reshape(8, 4, 64, F)

    def by_row(a):
        return a.reshape(32, 64, F).transpose(1, 0, 2)

    live = jnp.pad(present.astype(bf16), ((0, 0), (0, 96)))
    pd = pair.reshape(32, 2, 8, 4, CZ).transpose(2, 1, 3, 0, 4)
    x, p, o, g, at, lt, rt, up, pd, recip, livet = fwd(
        by_column(msa), by_column(upstream), pd, live, wq, wk, wv, wg, we, wl.T, wr.T)
    lg, rg = opm(lt.reshape(4 * CW, N), rt.reshape(4 * CW, N), pd.reshape(-1, CZ), recip, wo, livet)
    grad, inter = bwd(x, up, at, lg, rg, p, o, g, wq, wk, wv, wg, we, wl.T, wr.T)
    return by_row(grad), by_row(inter)


def solution(mesh):
    rows = P("dep", "res", None)
    in_specs = (rows, P("dep", "res"), P("res", "dep", None), rows) + (P(),) * 8
    return jax.shard_map(on_device, mesh=mesh, in_specs=in_specs, out_specs=(rows, rows), check_vma=False)
```

```python
import functools

import jax
import jax.numpy as jnp
from jax import lax
from jax.experimental import pallas as pl
from jax.experimental.pallas import tpu as pltpu
from jax.sharding import PartitionSpec as P

F = 256
H = 8
DH = 32
N = 512
CW = 32
CZ = 128
EPS = 1e-05
BIG = 1e9
f32 = jnp.float32
bf16 = jnp.bfloat16
SCALE = DH ** (-0.5)
NT = (((1,), (1,)), ((), ()))


def mm(a, b):
    return jnp.dot(a, b, preferred_element_type=f32)


def mmt(a, b):
    return lax.dot_general(a, b, NT, preferred_element_type=f32)


def norm(v, axis):
    c = v - jnp.mean(v, axis, keepdims=True)
    inv = lax.rsqrt(jnp.mean(c * c, axis, keepdims=True) + EPS)
    return c * inv, inv


def spread(rows, h, extra):
    top = (h % 4) * DH
    parts = []
    if top:
        parts.append(jnp.zeros((top, N), bf16))
    parts.append(rows)
    if top < 96:
        parts.append(jnp.zeros((96 - top, N), bf16))
    parts.append(extra)
    return jnp.concatenate(parts, axis=0)


MESH = pl.DeviceIdType.MESH


def remote(src, dst, send, recv, dep, res):
    return pltpu.make_async_remote_copy(src_ref=src, dst_ref=dst, send_sem=send, recv_sem=recv,
                                        device_id={"dep": dep, "res": res}, device_id_type=MESH)


def hail(peers):
    bar = pltpu.get_barrier_semaphore()
    for dep, res in peers:
        pl.semaphore_signal(bar, inc=1, device_id={"dep": dep, "res": res}, device_id_type=MESH)


def gather_all(count):
    pl.semaphore_wait(pltpu.get_barrier_semaphore(), count)


def greet(peers):
    hail(peers)
    gather_all(len(peers))


def fwd_kernel(hx, ux, px, present, wq, wk, wv, wg, we, wl, wr,
               x_ref, p_ref, o_ref, g_ref, a_ref, l_ref, r_ref, q_ref, v_ref, kt_ref, up_out, pd_out, rc_ref, live_out,
               wt, bias_s, st_s, live_in, xbuf, lbuf, livet, jbuf, mine, ustage, pstage,
               xs, xr, us, ur, ps, pr, ls, lr, js, jr, own):
    k = pl.program_id(0)
    d = lax.axis_index("dep")
    r = lax.axis_index("res")

    def dep_at(n):
        return lax.rem(d + n, 8)

    def res_at(n):
        return lax.rem(r + n, 16)

    def x_copy(c, n):
        return remote(hx.at[dep_at(n), c], xbuf.at[c, d], xs.at[c, n], xr.at[c, n], dep_at(n), r)

    def up_copy(c, n):
        return remote(ux.at[dep_at(n), c], up_out.at[d, c], us.at[c, n], ur.at[c, n], dep_at(n), r)

    def pd_copy(n):
        return remote(px.at[dep_at(n)], pd_out.at[d], ps.at[n], pr.at[n], dep_at(n), r)

    def live_copy(n):
        return remote(live_in, lbuf.at[d], ls.at[n], lr.at[n], dep_at(n), r)

    def row_copy(n):
        return remote(mine, jbuf.at[r], js.at[n], jr.at[n], d, res_at(n))

    def own_x(c):
        return pltpu.make_async_copy(hx.at[d, c], xbuf.at[c, d], own.at[c])

    own_up = pltpu.make_async_copy(ux.at[d, pl.ds(0, 2)], ustage, own.at[4])
    own_pd = pltpu.make_async_copy(px.at[d], pstage, own.at[5])
    own_up2 = pltpu.make_async_copy(ustage, up_out.at[d], own.at[6])
    own_pd2 = pltpu.make_async_copy(pstage, pd_out.at[d], own.at[7])

    @pl.when(k == 0)
    def _():
        for c in range(4):
            own_x(c).start()
        own_up.start()
        own_pd.start()
        hail([(dep_at(n), r) for n in range(1, 8)] + [(d, res_at(n)) for n in range(1, 16)])
        for n, w in enumerate((wq, wv, wg, we)):
            wt[n] = w[...].T
        held = jnp.concatenate([present[...].astype(f32), jnp.zeros((64, 96), f32)], axis=1).astype(bf16)
        live_in[...] = held
        lbuf[d] = held
        gather_all(22)
        for n in range(1, 8):
            live_copy(n).start()
        for n in range(1, 8):
            x_copy(0, n).start()
        for n in range(1, 8):
            live_copy(n).wait_recv()
        live = lbuf[...].reshape(N, 128).astype(f32)
        bias_s[...] = ((live - 1.0) * BIG).astype(bf16)
        livet[...] = live.T
        rows = [livet[pl.ds(4 * d + n, 1), :] for n in range(4)]
        held = jnp.concatenate(rows + [jnp.zeros((4, N), f32)], axis=0)
        mine[...] = held
        live_out[...] = held
        jbuf[r] = held
        for n in range(1, 16):
            row_copy(n).start()
        for n in range(1, 8):
            x_copy(0, n).wait_send()
        for n in range(1, 8):
            x_copy(1, n).start()

    @pl.when(k == 1)
    def _():
        for n in range(1, 8):
            pd_copy(n).start()
        own_up.wait()
        own_pd.wait()
        own_up2.start()
        own_pd2.start()

    @pl.when(k == 2)
    def _():
        for n in range(1, 8):
            up_copy(1, n).start()

    @pl.when(k == 3)
    def _():
        for n in range(1, 16):
            row_copy(n).wait_recv()
        counts = mm(jbuf[...].reshape(128, N).astype(bf16), lbuf[...].reshape(N, 128))
        rec = 1.0 / (0.001 + counts)
        for n in range(8):
            pieces = []
            for j in range(8):
                at = 16 * n + 8 * (j // 4) + j % 4
                pieces.append(rec[at:at + 1, :CW])
            rc_ref[n:n + 1, :] = jnp.concatenate(pieces, axis=1)

    own_x(k).wait()
    for n in range(1, 8):
        x_copy(k, n).wait_recv()
    xin = xbuf[k].reshape(N, F)
    x_ref[...] = xin.reshape(x_ref.shape)
    xhat, _ = norm(xin.astype(f32), 1)
    xb = xhat.astype(bf16)
    xbt = xb.T
    qt = (mm(wt[0], xbt) * SCALE).astype(bf16)
    vt = mm(wt[1], xbt).astype(bf16)
    kk = mm(xb, wk[...]).astype(bf16)
    gt = jax.nn.sigmoid(mm(wt[2], xbt))
    q_ref[0] = qt.T
    v_ref[0] = vt.T
    kt_ref[0] = kk.T
    g_ref[0] = gt
    extra = (lax.broadcasted_iota(jnp.int32, (128, N), 0) == 4 * d + k).astype(f32).astype(bf16)
    bias = bias_s[...]
    PIECE = 128

    def operands(h):
        grp = h // 4
        return jnp.concatenate([kk[:, 128 * grp:128 * grp + 128], bias], axis=1), spread(qt[DH * h:DH * h + DH], h, extra)

    def score(ops, h, i):
        val = mm(ops[0][i:i + PIECE], ops[1])
        st_s[h % 2, i:i + PIECE, :] = val
        return jnp.max(val, 0, keepdims=True)

    def blend(h):
        o_ref[0, DH * h:DH * h + DH, :] = mm(vt[DH * h:DH * h + DH], p_ref[0, h])

    ops = operands(0)
    peak = functools.reduce(jnp.maximum, [score(ops, 0, i) for i in range(0, N, PIECE)])
    def push_x(at, c):
        @pl.when(k == at)
        def _():
            for n in range(1, 8):
                x_copy(c, n).start()

    def push_up(at, c):
        @pl.when(k == at)
        def _():
            for n in range(1, 8):
                up_copy(c, n).start()

    for h in range(H):
        if h == 2:
            push_x(0, 2)
        if h == 4:
            push_up(1, 0)
        if h == 5:
            push_x(0, 3)
        b = h % 2
        if h + 1 < H:
            ops = operands(h + 1)
        nxt = []
        tot = jnp.zeros((1, N), f32)
        for i in range(0, N, PIECE):
            if h + 1 < H:
                nxt.append(score(ops, h + 1, i))
            e = jnp.exp(st_s[b, i:i + PIECE, :] - peak)
            st_s[b, i:i + PIECE, :] = e
            tot = tot + jnp.sum(e, 0, keepdims=True)
        if h:
            blend(h - 1)
        inv = 1.0 / tot
        for i in range(0, N, PIECE):
            p_ref[0, h, i:i + PIECE, :] = (st_s[b, i:i + PIECE, :] * inv).astype(bf16)
        if nxt:
            peak = functools.reduce(jnp.maximum, nxt)
    blend(H - 1)
    gated = (gt * o_ref[0]).astype(bf16)
    up = mm(wt[3], gated)
    after = (xin.T.astype(f32) + up).astype(bf16)
    a_ref[0] = after
    yhat, _ = norm(after.astype(f32), 0)
    yb = yhat.astype(bf16)
    live = livet[pl.ds(4 * d + k, 1), :]
    l_ref[0] = (mm(wl[...], yb) * live).astype(bf16)
    r_ref[0] = (mm(wr[...], yb) * live).astype(bf16)

    @pl.when(k == 3)
    def _():
        for n in range(1, 8):
            pd_copy(n).wait_recv()
            for c in range(2):
                up_copy(c, n).wait_recv()
        own_up2.wait()
        own_pd2.wait()
        for n in range(1, 8):
            live_copy(n).wait_send()
            pd_copy(n).wait_send()
            for c in range(2):
                up_copy(c, n).wait_send()
            for c in range(1, 4):
                x_copy(c, n).wait_send()
        for n in range(1, 16):
            row_copy(n).wait_send()


def bwd_kernel(x_ref, ua_ref, ub_ref, at_ref, lg_ref, rg_ref, p_ref, o_ref, g_ref, q_ref, v_ref, kt_ref, wq, wk, wv, wg, we, wl, wr,
               out_g, out_i, ds_s, acc_q, acc_v, acc_t, dt_s, sbuf, ss, rs, own):
    k = pl.program_id(0)
    d = lax.axis_index("dep")
    r = lax.axis_index("res")
    outs = (out_g, out_i)

    def dep_at(n):
        return lax.rem(d + n, 8)

    def send(which, c, n):
        return remote(sbuf.at[which, c, dep_at(n)], outs[which].at[d, c],
                      ss.at[which, c, n], rs.at[which, c, n], dep_at(n), r)

    def keep(which, c):
        return pltpu.make_async_copy(sbuf.at[which, c, d], outs[which].at[d, c], own.at[which, c])

    def ship(which, c, value):
        sbuf[which, c] = value.T.reshape(8, 64, F)
        for n in range(1, 8):
            send(which, c, n).start()
        keep(which, c).start()

    @pl.when(k == 0)
    def _():
        wlt, wrt = wl[...].T, wr[...].T
        greet([(dep_at(n), r) for n in range(1, 8)])
        for c in range(4):
            yhat, yinv = norm(at_ref[c].astype(f32), 0)
            dy = mm(wlt, lg_ref[c]) + mm(wrt, rg_ref[c])
            m1 = jnp.mean(dy, 0, keepdims=True)
            m2 = jnp.mean(dy * yhat, 0, keepdims=True)
            upt = (ua_ref if c < 2 else ub_ref)[:, c % 2].reshape(N, F).T.astype(f32)
            dt_s[c] = (yinv * (dy - m1 - yhat * m2) + upt).astype(bf16)
            ship(1, c, dt_s[c])

    xin = x_ref[...].reshape(N, F)
    q = q_ref[0]
    v = v_ref[0]
    kt = kt_ref[0]
    gt = g_ref[0]
    ot = o_ref[0]
    dt = dt_s[k]
    dg = mm(we[...], dt).astype(bf16).astype(f32)
    dot_ = (dg * gt).astype(bf16)
    dpre = (dg * ot * gt * (1.0 - gt)).astype(bf16)
    prod = dot_.astype(f32) * ot
    row = lax.broadcasted_iota(jnp.int32, (128, N), 0)
    col = lax.broadcasted_iota(jnp.int32, (N, 128), 1)
    ones = (col < 2).astype(f32).astype(bf16)
    lane = lax.broadcasted_iota(jnp.int32, (N, F), 1) // DH
    zero = jnp.zeros((), bf16)

    def back(h):
        sl = slice(DH * h, DH * h + DH)
        acc_q[sl, :] = mm(kt[sl], ds_s[h])

    def dops(h):
        grp = h // 4
        sl = slice(DH * h, DH * h + DH)
        dd = -jnp.sum(prod[sl], 0, keepdims=True)
        hi = dd.astype(bf16).astype(f32)
        lo = dd - hi
        extra = jnp.where(row == 0, hi, jnp.where(row == 1, lo, 0.0)).astype(bf16)
        return jnp.concatenate([v[:, 128 * grp:128 * grp + 128], ones], axis=1), spread(dot_[sl], h, extra)

    def wide_v(h):
        sl = slice(DH * h, DH * h + DH)
        acc_v[sl, :] = mmt(dot_[sl], p_ref[0, h])

    def tall_k(h, i):
        ext = mm(ds_s[h, i:i + 256, :], jnp.where(lane == h, q, zero))
        if h:
            acc_t[i:i + 256, :] += ext
        else:
            acc_t[i:i + 256, :] = ext

    for h in range(H):
        ops = dops(h)
        for i in range(0, N, 256):
            dp = mm(ops[0][i:i + 256], ops[1])
            ds_s[h, i:i + 256, :] = (p_ref[0, h, i:i + 256, :].astype(f32) * dp).astype(bf16)
            if h:
                tall_k(h - 1, i)
        wide_v(h)
        if h:
            back(h - 1)
    back(H - 1)
    for i in range(0, N, 256):
        tall_k(H - 1, i)
    dq = (acc_q[...].astype(bf16).astype(f32) * SCALE).astype(bf16)
    dx = (mm(wq[...], dq) + mm(wg[...], dpre)
          + mmt(wk[...], acc_t[...].astype(bf16)) + mm(wv[...], acc_v[...].astype(bf16)))
    dx = dx.astype(bf16).astype(f32)
    xt = xin.T.astype(f32)
    xh, inv = norm(xt, 0)
    m1 = jnp.mean(dx, 0, keepdims=True)
    m2 = jnp.mean(dx * xh, 0, keepdims=True)
    dln = (inv * (dx - m1 - xh * m2)).astype(bf16)
    out = (dt.astype(f32) + dln.astype(f32)).astype(bf16)
    ship(0, k, out)

    @pl.when(k == 3)
    def _():
        for which in range(2):
            for c in range(4):
                keep(which, c).wait()
                for n in range(1, 8):
                    send(which, c, n).wait_recv()
                    send(which, c, n).wait_send()


def whole(shape):
    return pl.BlockSpec(shape, lambda k: (0,) * len(shape))


def percol(shape):
    return pl.BlockSpec((1, *shape), lambda k: (k,) + (0,) * len(shape))


COLS = pl.BlockSpec((8, 1, 64, F), lambda k: (0, k, 0, 0))
ANY = pl.BlockSpec(memory_space=pl.ANY)


def fwd(hx, ux, px, live, wq, wk, wv, wg, we, wl, wr):
    sd = jax.ShapeDtypeStruct
    V = pltpu.VMEM
    dma = pltpu.SemaphoreType.DMA
    return pl.pallas_call(
        fwd_kernel,
        grid=(4,),
        in_specs=[ANY] * 3 + [whole((64, CW))] + [whole((F, F))] * 5 + [whole((CW, F))] * 2,
        out_specs=[COLS, percol((H, N, N)), percol((F, N)), percol((F, N)), percol((F, N)), percol((CW, N)),
                   percol((CW, N)), percol((N, F)), percol((N, F)), percol((F, N)), ANY, ANY, whole((8, 256)), whole((8, N))],
        out_shape=[sd((8, 4, 64, F), bf16), sd((4, H, N, N), bf16), sd((4, F, N), f32), sd((4, F, N), f32),
                   sd((4, F, N), bf16), sd((4, CW, N), bf16), sd((4, CW, N), bf16),
                   sd((4, N, F), bf16), sd((4, N, F), bf16), sd((4, F, N), bf16), sd((8, 2, 64, F), bf16), sd(px.shape, bf16), sd((8, 256), f32), sd((8, N), f32)],
        scratch_shapes=[V((4, F, F), bf16), V((N, 128), bf16), V((2, N, N), f32), V((64, 128), bf16), V((4, 8, 64, F), bf16),
                        V((8, 64, 128), bf16), V((128, N), f32), V((16, 8, N), f32), V((8, N), f32), V((2, 64, F), bf16),
                        V(px.shape[1:], bf16), dma((4, 8)), dma((4, 8)), dma((4, 8)), dma((4, 8))] + [dma((8,))] * 4 + [dma((16,))] * 2 + [dma((8,))],
        compiler_params=pltpu.CompilerParams(vmem_limit_bytes=60 * 1024 * 1024, collective_id=2, has_side_effects=True,
                                             dimension_semantics=("arbitrary",)),
        name="attention_forward",
    )(hx, ux, px, live, wq, wk, wv, wg, we, wl, wr)


def bwd(x, ua, ub, at, lg, rg, p, o, g, q, v, kt, wq, wk, wv, wg, we, wl, wr):
    sd = jax.ShapeDtypeStruct
    V = pltpu.VMEM
    dma = pltpu.SemaphoreType.DMA
    return pl.pallas_call(
        bwd_kernel,
        grid=(4,),
        in_specs=[COLS, whole((8, 2, 64, F)), whole((8, 2, 64, F)), whole((4, F, N)), whole((4, CW, N)), whole((4, CW, N)), percol((H, N, N)), percol((F, N)),
                  percol((F, N)), percol((N, F)), percol((N, F)), percol((F, N))] + [whole((F, F))] * 5 + [whole((CW, F))] * 2,
        out_specs=[ANY, ANY],
        out_shape=[sd((8, 4, 64, F), bf16)] * 2,
        scratch_shapes=[V((H, N, N), bf16), V((F, N), f32), V((F, N), f32), V((N, F), f32), V((4, F, N), bf16), V((2, 4, 8, 64, F), bf16),
                        dma((2, 4, 8)), dma((2, 4, 8)), dma((2, 4))],
        compiler_params=pltpu.CompilerParams(vmem_limit_bytes=60 * 1024 * 1024, collective_id=3, has_side_effects=True,
                                             dimension_semantics=("arbitrary",)),
        name="attention_backward",
    )(x, ua, ub, at, lg, rg, p, o, g, q, v, kt, wq, wk, wv, wg, we, wl, wr)


def opm_kernel(lt, rt, pd, rc, wo, live, ux, lo, ro, up,
               perm, oc1, oc2, lbuf, rbuf, lsend, lrecv, psend, precv, rsend, rrecv, both, lkeep, lacc,
               ls, lr, rs, rr, fs, fr, ps, pr, s2, r2, s3, r3, us, ur, own):
    d = lax.axis_index("dep")
    r = lax.axis_index("res")
    xl, z = d // 4, lax.rem(d, 4)
    y, xh, core = r // 4, lax.rem(r // 2, 2), lax.rem(r, 2)

    def dep_of(flip, step):
        return 4 * lax.rem(xl + flip, 2) + lax.rem(z + step + 4, 4)

    def chip_of(flip, step):
        return 2 * lax.rem(y + step + 4, 4) + lax.rem(xh + flip, 2)

    def res_of(flip, step):
        return 2 * chip_of(flip, step) + core

    partner = 2 * chip_of(0, 0) + 1 - core
    greet([(lax.rem(d + n, 8), r) for n in range(1, 8)]
          + [(d, res_of(0, n)) for n in range(1, 4)] + [(d, res_of(1, 0)), (d, partner)])

    def left_copy(n):
        if n == 0:
            return remote(lt, lbuf.at[d], ls.at[0], lr.at[0], dep_of(1, 0), r)
        if n < 4:
            return remote(lt, lbuf.at[d], ls.at[n], lr.at[n], dep_of(0, n), r)
        slot = dep_of(1, 0)
        return remote(lbuf.at[slot], lbuf.at[slot], ls.at[n], lr.at[n], dep_of(0, n - 3), r)

    def right_copy(n):
        if n == 0:
            return remote(rt, rbuf.at[r], rs.at[0], rr.at[0], d, res_of(1, 0))
        if n < 4:
            return remote(rt, rbuf.at[r], rs.at[n], rr.at[n], d, res_of(0, n))
        slot = res_of(1, 0)
        return remote(rbuf.at[slot], rbuf.at[slot], rs.at[n], rr.at[n], d, res_of(0, n - 3))

    def across(n):
        if n == 7:
            return remote(rt, rbuf.at[r], fs.at[7], fr.at[7], d, partner)
        slot = res_of(1, 0) if n == 0 else res_of(0, -n) if n < 4 else res_of(1, 3 - n)
        return remote(rbuf.at[slot], rbuf.at[slot], fs.at[n], fr.at[n], d, partner)

    def up_copy(n):
        dep = lax.rem(d + n, 8)
        return remote(ux.at[dep, pl.ds(2, 2)], up.at[d], us.at[n], ur.at[n], dep, r)

    own_up = pltpu.make_async_copy(ux.at[d, pl.ds(2, 2)], up.at[d], own)
    own_up.start()
    for n in range(4):
        left_copy(n).start()
        right_copy(n).start()
    across(7).start()
    lbuf[d] = lt[...]
    rbuf[r] = rt[...]

    a = lax.broadcasted_iota(jnp.int32, (1024, 1024), 0)
    b = lax.broadcasted_iota(jnp.int32, (1024, 1024), 1)
    hit = ((a // CW) == (b % CW)) & ((a % CW) == (b // CW))
    perm[...] = hit.astype(f32).astype(bf16)

    def outer_step(n, carry):
        at = pl.multiple_of(256 * n, 256)
        zz = (mmt(wo[...], pd[pl.ds(at, 256), :]) * rc[pl.ds(n, 1), :]).astype(bf16)
        rows = []
        for j in range(8):
            rows.append(jnp.concatenate([zz[CW * c:CW * c + CW, CW * j:CW * j + CW] for c in range(CW)], axis=1))
        yy = mm(jnp.concatenate(rows, axis=0), perm[...]).astype(bf16)
        oc1[pl.ds(at, 256), :] = yy
        oc2[:, pl.ds(at, 256)] = yy.T

        @pl.when(n == 1)
        def _():
            left_copy(0).wait_recv()
            for i in range(4, 7):
                left_copy(i).start()

        @pl.when(n == 2)
        def _():
            right_copy(0).wait_recv()
            for i in range(4, 7):
                right_copy(i).start()
            across(0).start()

        @pl.when(n == 6)
        def _():
            for i in range(1, 8):
                up_copy(i).start()

        @pl.when(n == 5)
        def _():
            for i in range(1, 4):
                right_copy(i).wait_recv()
                across(i).start()
        return carry

    lax.fori_loop(0, 8, outer_step, 0)
    for n in range(1, 7):
        left_copy(n).wait_recv()
    for n in range(4, 7):
        right_copy(n).wait_recv()
        across(n).start()

    order = [(1, 1), (1, 2), (1, 3), (1, 0), (0, 1), (0, 2), (0, 3), (0, 0)]

    def pass_over(i):
        return remote(psend.at[i], precv.at[i], ps.at[i], pr.at[i], d, partner)

    def right_part(i):
        target = res_of(1, 0) if i == 3 else res_of(0, order[i][1])
        return remote(rsend.at[i], rrecv.at[i], s2.at[i], r2.at[i], d, target)

    def left_part(i):
        target = dep_of(1, 0) if i == 3 else dep_of(0, order[i][1])
        return remote(lsend.at[i], lrecv.at[i], s3.at[i], r3.at[i], target, r)

    mine = pl.ds(pl.multiple_of(128 * core, 128), 128)
    theirs = pl.ds(pl.multiple_of(128 * (1 - core), 128), 128)
    lall = lbuf[...].reshape(1024, N)
    for i, (flip, step) in enumerate(order):
        at = pl.multiple_of(256 * chip_of(flip, step), 256)
        both[i] = mm(oc1[pl.ds(at, 256), :], lall)
        psend[i] = both[i, theirs, :].astype(bf16)
        pass_over(i).start()
    for i in range(8):
        pass_over(i).wait_recv()
        own = both[i, mine, :] + precv[i].astype(f32)
        if i in (3, 7):
            both[i, mine, :] = own
        else:
            rsend[i] = own.astype(bf16)
            right_part(i).start()
    for n in range(8):
        across(n).wait_recv()
    rall = rbuf[...].reshape(2048, N)
    for i, (flip, step) in enumerate(order):
        at = pl.multiple_of(128 * dep_of(flip, step), 128)
        own = mm(oc2[pl.ds(at, 128), :], rall)
        if i == 3:
            lkeep[...] = own
        elif i == 7:
            lacc[...] = own
        else:
            lsend[i] = own.astype(bf16)
            left_part(i).start()
    for i in range(3):
        right_part(i).wait_recv()
    rsend[3] = (both[3, mine, :] + jnp.sum(rrecv[0:3].astype(f32), 0)).astype(bf16)
    right_part(3).start()
    for i in range(3):
        left_part(i).wait_recv()
    lsend[3] = (lkeep[...] + jnp.sum(lrecv[0:3].astype(f32), 0)).astype(bf16)
    left_part(3).start()
    for i in range(3, 7):
        right_part(i).wait_recv()
    racc = both[7, mine, :] + jnp.sum(rrecv[3:7].astype(f32), 0)
    for n in range(4):
        ro[n] = (racc[CW * n:CW * n + CW, :] * live[n:n + 1, :]).astype(bf16)
    for i in range(3, 7):
        left_part(i).wait_recv()
    lsum = lacc[...] + jnp.sum(lrecv[3:7].astype(f32), 0)
    for n in range(4):
        lo[n] = (lsum[CW * n:CW * n + CW, :] * live[n:n + 1, :]).astype(bf16)
    own_up.wait()
    for n in range(1, 8):
        up_copy(n).wait_recv()
        up_copy(n).wait_send()
    for n in range(7):
        left_copy(n).wait_send()
        right_copy(n).wait_send()
        right_part(n).wait_send()
        left_part(n).wait_send()
    for n in range(8):
        across(n).wait_send()
        pass_over(n).wait_send()


def opm(lt, rt, pd, rc, wo, live, ux):
    sd = jax.ShapeDtypeStruct
    vm = pl.BlockSpec(memory_space=pltpu.VMEM)
    chunk = (128, N)
    V = pltpu.VMEM
    dma = pltpu.SemaphoreType.DMA((8,))
    return pl.pallas_call(
        opm_kernel,
        in_specs=[vm] * 6 + [ANY],
        out_specs=[vm] * 3,
        out_shape=[sd((4, CW, N), bf16)] * 2 + [sd((8, 2, 64, F), bf16)],
        scratch_shapes=[V((1024, 1024), bf16), V((2048, 1024), bf16), V((1024, 2048), bf16),
                        V((8, *chunk), bf16), V((16, *chunk), bf16)] + [V((8, *chunk), bf16)] * 6
        + [V((8, 256, N), f32)] + [V(chunk, f32)] * 2 + [dma] * 14 + [pltpu.SemaphoreType.DMA],
        compiler_params=pltpu.CompilerParams(vmem_limit_bytes=60 * 1024 * 1024, collective_id=1, has_side_effects=True),
        name="outer_product",
    )(lt, rt, pd, rc, wo, live, ux)


def on_device(msa, present, pair, upstream, wq, wk, wv, wg, we, wl, wr, wo):
    def by_column(a):
        return a.transpose(1, 0, 2).reshape(8, 4, 64, F)

    def by_row(a):
        return a.reshape(32, 64, F).transpose(1, 0, 2)

    pd = pair.reshape(32, 2, 8, 4, CZ).transpose(2, 1, 3, 0, 4)
    ux = by_column(upstream)
    x, p, o, g, at, lt, rt, q, v, kt, ua, pd, recip, livet = fwd(
        by_column(msa), ux, pd, present, wq, wk, wv, wg, we, wl.T, wr.T)
    lg, rg, ub = opm(lt.reshape(4 * CW, N), rt.reshape(4 * CW, N), pd.reshape(-1, CZ), recip, wo, livet, ux)
    grad, inter = bwd(x, ua, ub, at, lg, rg, p, o, g, q, v, kt, wq, wk, wv, wg, we, wl.T, wr.T)
    return by_row(grad), by_row(inter)


def solution(mesh):
    rows = P("dep", "res", None)
    in_specs = (rows, P("dep", "res"), P("res", "dep", None), rows) + (P(),) * 8
    return jax.shard_map(on_device, mesh=mesh, in_specs=in_specs, out_specs=(rows, rows), check_vma=False)
```

```python
import functools

import jax
import jax.numpy as jnp
from jax import lax
from jax.experimental import pallas as pl
from jax.experimental.pallas import tpu as pltpu
from jax.sharding import PartitionSpec as P

F = 256
H = 8
DH = 32
N = 512
CW = 32
CZ = 128
EPS = 1e-05
BIG = 1e9
f32 = jnp.float32
bf16 = jnp.bfloat16
SCALE = DH ** (-0.5)
NT = (((1,), (1,)), ((), ()))


def mm(a, b):
    return jnp.dot(a, b, preferred_element_type=f32)


def mmt(a, b):
    return lax.dot_general(a, b, NT, preferred_element_type=f32)


def norm(v, axis):
    c = v - jnp.mean(v, axis, keepdims=True)
    inv = lax.rsqrt(jnp.mean(c * c, axis, keepdims=True) + EPS)
    return c * inv, inv


def spread(rows, h, extra):
    top = (h % 4) * DH
    parts = []
    if top:
        parts.append(jnp.zeros((top, N), bf16))
    parts.append(rows)
    if top < 96:
        parts.append(jnp.zeros((96 - top, N), bf16))
    parts.append(extra)
    return jnp.concatenate(parts, axis=0)


MESH = pl.DeviceIdType.MESH


def remote(src, dst, send, recv, dep, res):
    return pltpu.make_async_remote_copy(src_ref=src, dst_ref=dst, send_sem=send, recv_sem=recv,
                                        device_id={"dep": dep, "res": res}, device_id_type=MESH)


def hail(peers):
    bar = pltpu.get_barrier_semaphore()
    for dep, res in peers:
        pl.semaphore_signal(bar, inc=1, device_id={"dep": dep, "res": res}, device_id_type=MESH)


def gather_all(count):
    pl.semaphore_wait(pltpu.get_barrier_semaphore(), count)


def greet(peers):
    hail(peers)
    gather_all(len(peers))


def fwd_kernel(x_in, u_in, pair_in, present, wq, wk, wv, wg, we, wl, wr,
               x_ref, p_ref, o_ref, g_ref, a_ref, l_ref, r_ref, q_ref, v_ref, kt_ref, up_out, ut_out, pd_out, rc_ref, live_out,
               wt, bias_s, st_s, live_in, hx, ux, px, xbuf, lbuf, livet, jbuf, mine,
               xs, xr, us, ur, ps, pr, ls, lr, js, jr, own):
    k = pl.program_id(0)
    d = lax.axis_index("dep")
    r = lax.axis_index("res")

    def dep_at(n):
        return lax.rem(d + n, 8)

    def res_at(n):
        return lax.rem(r + n, 16)

    def x_copy(c, n):
        return remote(hx.at[dep_at(n), c], xbuf.at[c, d], xs.at[c, n], xr.at[c, n], dep_at(n), r)

    def up_copy(c, n):
        return remote(ux.at[dep_at(n), c], up_out.at[d, c], us.at[c, n], ur.at[c, n], dep_at(n), r)

    def pd_copy(n):
        return remote(px.at[:, dep_at(n)], pd_out.at[d], ps.at[n], pr.at[n], dep_at(n), r)

    def live_copy(n):
        return remote(live_in, lbuf.at[d], ls.at[n], lr.at[n], dep_at(n), r)

    def row_copy(n):
        return remote(mine, jbuf.at[r], js.at[n], jr.at[n], d, res_at(n))

    own_up = pltpu.make_async_copy(ux.at[d, pl.ds(0, 2)], up_out.at[d], own.at[0])
    own_pd = pltpu.make_async_copy(px.at[:, d], pd_out.at[d], own.at[1])
    later_up = pltpu.make_async_copy(ux.at[:, pl.ds(2, 2)], ut_out, own.at[2])

    @pl.when(k == 0)
    def _():
        hail([(dep_at(n), r) for n in range(1, 8)] + [(d, res_at(n)) for n in range(1, 16)])
        hx[...] = jnp.transpose(x_in[...], (1, 0, 2)).reshape(hx.shape)
        flat = jnp.concatenate([present[...].astype(f32), jnp.zeros((CW, 64), f32)], axis=1)
        held = jnp.concatenate([flat, jnp.zeros((96, 128), f32)], axis=0).T[:64].astype(bf16)
        live_in[...] = held
        lbuf[d] = held
        gather_all(22)
        for n in range(1, 8):
            live_copy(n).start()
        for n in range(1, 8):
            x_copy(0, n).start()
        for c in range(4):
            xbuf[c, d] = hx[d, c]
        for n, w in enumerate((wq, wv, wg, we)):
            wt[n] = w[...].T
        px[...] = jnp.transpose(pair_in[...], (1, 0, 2)).reshape(px.shape)
        ux[...] = jnp.transpose(u_in[...], (1, 0, 2)).reshape(ux.shape)
        for n in range(1, 8):
            live_copy(n).wait_recv()
        live = lbuf[...].reshape(N, 128).astype(f32)
        bias_s[...] = ((live - 1.0) * BIG).astype(bf16)
        livet[...] = live.T
        rows = [livet[pl.ds(4 * d + n, 1), :] for n in range(4)]
        held = jnp.concatenate(rows + [jnp.zeros((4, N), f32)], axis=0)
        mine[...] = held
        live_out[...] = held
        jbuf[r] = held
        for n in range(1, 16):
            row_copy(n).start()
        for n in range(1, 8):
            x_copy(0, n).wait_send()
        for n in range(1, 8):
            x_copy(1, n).start()

    @pl.when(k == 1)
    def _():
        for n in range(1, 8):
            pd_copy(n).start()
        own_up.start()
        own_pd.start()
        later_up.start()

    @pl.when(k == 2)
    def _():
        for n in range(1, 8):
            up_copy(1, n).start()

    @pl.when(k == 3)
    def _():
        for n in range(1, 16):
            row_copy(n).wait_recv()
        counts = mm(jbuf[...].reshape(128, N).astype(bf16), lbuf[...].reshape(N, 128))
        rec = 1.0 / (0.001 + counts)
        for n in range(8):
            pieces = []
            for j in range(8):
                at = 16 * n + 8 * (j // 4) + j % 4
                pieces.append(rec[at:at + 1, :CW])
            rc_ref[n:n + 1, :] = jnp.concatenate(pieces, axis=1)

    for n in range(1, 8):
        x_copy(k, n).wait_recv()
    xin = xbuf[k].reshape(N, F)
    x_ref[...] = xin.reshape(x_ref.shape)
    xhat, _ = norm(xin.astype(f32), 1)
    xb = xhat.astype(bf16)
    xbt = xb.T
    qt = (mm(wt[0], xbt) * SCALE).astype(bf16)
    vt = mm(wt[1], xbt).astype(bf16)
    kk = mm(xb, wk[...]).astype(bf16)
    gt = jax.nn.sigmoid(mm(wt[2], xbt))
    q_ref[0] = qt.T
    v_ref[0] = vt.T
    kt_ref[0] = kk.T
    g_ref[0] = gt
    extra = (lax.broadcasted_iota(jnp.int32, (128, N), 0) == 4 * d + k).astype(f32).astype(bf16)
    bias = bias_s[...]
    PIECE = 128

    def operands(h):
        grp = h // 4
        return jnp.concatenate([kk[:, 128 * grp:128 * grp + 128], bias], axis=1), spread(qt[DH * h:DH * h + DH], h, extra)

    def score(ops, h, i):
        val = mm(ops[0][i:i + PIECE], ops[1])
        st_s[h % 2, i:i + PIECE, :] = val
        return jnp.max(val, 0, keepdims=True)

    def blend(h):
        o_ref[0, DH * h:DH * h + DH, :] = mm(vt[DH * h:DH * h + DH], p_ref[0, h])

    ops = operands(0)
    peak = functools.reduce(jnp.maximum, [score(ops, 0, i) for i in range(0, N, PIECE)])
    def push_x(at, c):
        @pl.when(k == at)
        def _():
            for n in range(1, 8):
                x_copy(c, n).start()

    def push_up(at, c):
        @pl.when(k == at)
        def _():
            for n in range(1, 8):
                up_copy(c, n).start()

    for h in range(H):
        if h == 2:
            push_x(0, 2)
        if h == 4:
            push_up(1, 0)
        if h == 5:
            push_x(0, 3)
        b = h % 2
        if h + 1 < H:
            ops = operands(h + 1)
        nxt = []
        tot = jnp.zeros((1, N), f32)
        for i in range(0, N, PIECE):
            if h + 1 < H:
                nxt.append(score(ops, h + 1, i))
            e = jnp.exp(st_s[b, i:i + PIECE, :] - peak)
            st_s[b, i:i + PIECE, :] = e
            tot = tot + jnp.sum(e, 0, keepdims=True)
        if h:
            blend(h - 1)
        inv = 1.0 / tot
        for i in range(0, N, PIECE):
            p_ref[0, h, i:i + PIECE, :] = (st_s[b, i:i + PIECE, :] * inv).astype(bf16)
        if nxt:
            peak = functools.reduce(jnp.maximum, nxt)
    blend(H - 1)
    gated = (gt * o_ref[0]).astype(bf16)
    up = mm(wt[3], gated)
    after = (xin.T.astype(f32) + up).astype(bf16)
    a_ref[0] = after
    yhat, _ = norm(after.astype(f32), 0)
    yb = yhat.astype(bf16)
    live = livet[pl.ds(4 * d + k, 1), :]
    l_ref[0] = (mm(wl[...], yb) * live).astype(bf16)
    r_ref[0] = (mm(wr[...], yb) * live).astype(bf16)

    @pl.when(k == 3)
    def _():
        for n in range(1, 8):
            pd_copy(n).wait_recv()
            for c in range(2):
                up_copy(c, n).wait_recv()
        own_up.wait()
        own_pd.wait()
        later_up.wait()
        for n in range(1, 8):
            live_copy(n).wait_send()
            pd_copy(n).wait_send()
            for c in range(2):
                up_copy(c, n).wait_send()
            for c in range(1, 4):
                x_copy(c, n).wait_send()
        for n in range(1, 16):
            row_copy(n).wait_send()


def bwd_kernel(x_ref, ua_ref, ub_ref, at_ref, lg_ref, rg_ref, p_ref, o_ref, g_ref, q_ref, v_ref, kt_ref, wq, wk, wv, wg, we, wl, wr,
               out_g, out_i, ds_s, acc_q, acc_v, acc_t, dt_s, sbuf, ss, rs, own):
    k = pl.program_id(0)
    d = lax.axis_index("dep")
    r = lax.axis_index("res")
    outs = (out_g, out_i)

    def dep_at(n):
        return lax.rem(d + n, 8)

    def send(which, c, n):
        return remote(sbuf.at[which, c, dep_at(n)], outs[which].at[d, c],
                      ss.at[which, c, n], rs.at[which, c, n], dep_at(n), r)

    def keep(which, c):
        return pltpu.make_async_copy(sbuf.at[which, c, d], outs[which].at[d, c], own.at[which, c])

    def ship(which, c, value):
        sbuf[which, c] = value.T.reshape(8, 64, F)
        for n in range(1, 8):
            send(which, c, n).start()
        keep(which, c).start()

    @pl.when(k == 0)
    def _():
        wlt, wrt = wl[...].T, wr[...].T
        greet([(dep_at(n), r) for n in range(1, 8)])
        for c in range(4):
            yhat, yinv = norm(at_ref[c].astype(f32), 0)
            dy = mm(wlt, lg_ref[c]) + mm(wrt, rg_ref[c])
            m1 = jnp.mean(dy, 0, keepdims=True)
            m2 = jnp.mean(dy * yhat, 0, keepdims=True)
            upt = (ua_ref if c < 2 else ub_ref)[:, c % 2].reshape(N, F).T.astype(f32)
            dt_s[c] = (yinv * (dy - m1 - yhat * m2) + upt).astype(bf16)
            ship(1, c, dt_s[c])

    xin = x_ref[...].reshape(N, F)
    q = q_ref[0]
    v = v_ref[0]
    kt = kt_ref[0]
    gt = g_ref[0]
    ot = o_ref[0]
    dt = dt_s[k]
    dg = mm(we[...], dt).astype(bf16).astype(f32)
    dot_ = (dg * gt).astype(bf16)
    dpre = (dg * ot * gt * (1.0 - gt)).astype(bf16)
    prod = dot_.astype(f32) * ot
    row = lax.broadcasted_iota(jnp.int32, (128, N), 0)
    col = lax.broadcasted_iota(jnp.int32, (N, 128), 1)
    ones = (col < 2).astype(f32).astype(bf16)
    lane = lax.broadcasted_iota(jnp.int32, (N, F), 1) // DH
    zero = jnp.zeros((), bf16)

    def back(h):
        sl = slice(DH * h, DH * h + DH)
        acc_q[sl, :] = mm(kt[sl], ds_s[h])

    def dops(h):
        grp = h // 4
        sl = slice(DH * h, DH * h + DH)
        dd = -jnp.sum(prod[sl], 0, keepdims=True)
        hi = dd.astype(bf16).astype(f32)
        lo = dd - hi
        extra = jnp.where(row == 0, hi, jnp.where(row == 1, lo, 0.0)).astype(bf16)
        return jnp.concatenate([v[:, 128 * grp:128 * grp + 128], ones], axis=1), spread(dot_[sl], h, extra)

    def wide_v(h):
        sl = slice(DH * h, DH * h + DH)
        acc_v[sl, :] = mmt(dot_[sl], p_ref[0, h])

    def tall_k(h, i):
        ext = mm(ds_s[h, i:i + 256, :], jnp.where(lane == h, q, zero))
        if h:
            acc_t[i:i + 256, :] += ext
        else:
            acc_t[i:i + 256, :] = ext

    for h in range(H):
        ops = dops(h)
        for i in range(0, N, 256):
            dp = mm(ops[0][i:i + 256], ops[1])
            ds_s[h, i:i + 256, :] = (p_ref[0, h, i:i + 256, :].astype(f32) * dp).astype(bf16)
            if h:
                tall_k(h - 1, i)
        wide_v(h)
        if h:
            back(h - 1)
    back(H - 1)
    for i in range(0, N, 256):
        tall_k(H - 1, i)
    dq = (acc_q[...].astype(bf16).astype(f32) * SCALE).astype(bf16)
    dx = (mm(wq[...], dq) + mm(wg[...], dpre)
          + mmt(wk[...], acc_t[...].astype(bf16)) + mm(wv[...], acc_v[...].astype(bf16)))
    dx = dx.astype(bf16).astype(f32)
    xt = xin.T.astype(f32)
    xh, inv = norm(xt, 0)
    m1 = jnp.mean(dx, 0, keepdims=True)
    m2 = jnp.mean(dx * xh, 0, keepdims=True)
    dln = (inv * (dx - m1 - xh * m2)).astype(bf16)
    out = (dt.astype(f32) + dln.astype(f32)).astype(bf16)
    ship(0, k, out)

    @pl.when(k == 3)
    def _():
        for which in range(2):
            for c in range(4):
                keep(which, c).wait()
                for n in range(1, 8):
                    send(which, c, n).wait_recv()
                    send(which, c, n).wait_send()


def whole(shape):
    return pl.BlockSpec(shape, lambda k: (0,) * len(shape))


def percol(shape):
    return pl.BlockSpec((1, *shape), lambda k: (k,) + (0,) * len(shape))


COLS = pl.BlockSpec((8, 1, 64, F), lambda k: (0, k, 0, 0))
ANY = pl.BlockSpec(memory_space=pl.ANY)


def fwd(msa, upstream, pair, live, wq, wk, wv, wg, we, wl, wr):
    sd = jax.ShapeDtypeStruct
    V = pltpu.VMEM
    dma = pltpu.SemaphoreType.DMA
    return pl.pallas_call(
        fwd_kernel,
        grid=(4,),
        in_specs=[whole((64, 32, F))] * 2 + [whole((32, 64, CZ)), whole((CW, 64))] + [whole((F, F))] * 5 + [whole((CW, F))] * 2,
        out_specs=[COLS, percol((H, N, N)), percol((F, N)), percol((F, N)), percol((F, N)), percol((CW, N)),
                   percol((CW, N)), percol((N, F)), percol((N, F)), percol((F, N)), ANY, ANY, ANY, whole((8, 256)), whole((8, N))],
        out_shape=[sd((8, 4, 64, F), bf16), sd((4, H, N, N), bf16), sd((4, F, N), f32), sd((4, F, N), f32),
                   sd((4, F, N), bf16), sd((4, CW, N), bf16), sd((4, CW, N), bf16),
                   sd((4, N, F), bf16), sd((4, N, F), bf16), sd((4, F, N), bf16), sd((8, 2, 64, F), bf16), sd((8, 2, 64, F), bf16), sd((8, 2, 4, CW, CZ), bf16), sd((8, 256), f32), sd((8, N), f32)],
        scratch_shapes=[V((4, F, F), bf16), V((N, 128), bf16), V((2, N, N), f32), V((64, 128), bf16), V((8, 4, 64, F), bf16), V((8, 4, 64, F), bf16), V((2, 8, 4, CW, CZ), bf16), V((4, 8, 64, F), bf16),
                        V((8, 64, 128), bf16), V((128, N), f32), V((16, 8, N), f32), V((8, N), f32),
                        dma((4, 8)), dma((4, 8)), dma((4, 8)), dma((4, 8))] + [dma((8,))] * 4 + [dma((16,))] * 2 + [dma((8,))],
        compiler_params=pltpu.CompilerParams(vmem_limit_bytes=60 * 1024 * 1024, collective_id=2, has_side_effects=True,
                                             dimension_semantics=("arbitrary",)),
        name="attention_forward",
    )(msa, upstream, pair, live, wq, wk, wv, wg, we, wl, wr)


def bwd(x, ua, ub, at, lg, rg, p, o, g, q, v, kt, wq, wk, wv, wg, we, wl, wr):
    sd = jax.ShapeDtypeStruct
    V = pltpu.VMEM
    dma = pltpu.SemaphoreType.DMA
    return pl.pallas_call(
        bwd_kernel,
        grid=(4,),
        in_specs=[COLS, whole((8, 2, 64, F)), whole((8, 2, 64, F)), whole((4, F, N)), whole((4, CW, N)), whole((4, CW, N)), percol((H, N, N)), percol((F, N)),
                  percol((F, N)), percol((N, F)), percol((N, F)), percol((F, N))] + [whole((F, F))] * 5 + [whole((CW, F))] * 2,
        out_specs=[ANY, ANY],
        out_shape=[sd((8, 4, 64, F), bf16)] * 2,
        scratch_shapes=[V((H, N, N), bf16), V((F, N), f32), V((F, N), f32), V((N, F), f32), V((4, F, N), bf16), V((2, 4, 8, 64, F), bf16),
                        dma((2, 4, 8)), dma((2, 4, 8)), dma((2, 4))],
        compiler_params=pltpu.CompilerParams(vmem_limit_bytes=60 * 1024 * 1024, collective_id=3, has_side_effects=True,
                                             dimension_semantics=("arbitrary",)),
        name="attention_backward",
    )(x, ua, ub, at, lg, rg, p, o, g, q, v, kt, wq, wk, wv, wg, we, wl, wr)


def opm_kernel(lt, rt, pd, rc, wo, live, ux, lo, ro, up,
               perm, oc1, oc2, lbuf, rbuf, lsend, lrecv, psend, precv, rsend, rrecv, both, lkeep, lacc,
               ls, lr, rs, rr, fs, fr, ps, pr, s2, r2, s3, r3, us, ur, own):
    d = lax.axis_index("dep")
    r = lax.axis_index("res")
    xl, z = d // 4, lax.rem(d, 4)
    y, xh, core = r // 4, lax.rem(r // 2, 2), lax.rem(r, 2)

    def dep_of(flip, step):
        return 4 * lax.rem(xl + flip, 2) + lax.rem(z + step + 4, 4)

    def chip_of(flip, step):
        return 2 * lax.rem(y + step + 4, 4) + lax.rem(xh + flip, 2)

    def res_of(flip, step):
        return 2 * chip_of(flip, step) + core

    partner = 2 * chip_of(0, 0) + 1 - core
    greet([(lax.rem(d + n, 8), r) for n in range(1, 8)]
          + [(d, res_of(0, n)) for n in range(1, 4)] + [(d, res_of(1, 0)), (d, partner)])

    def left_copy(n):
        if n == 0:
            return remote(lt, lbuf.at[d], ls.at[0], lr.at[0], dep_of(1, 0), r)
        if n < 4:
            return remote(lt, lbuf.at[d], ls.at[n], lr.at[n], dep_of(0, n), r)
        slot = dep_of(1, 0)
        return remote(lbuf.at[slot], lbuf.at[slot], ls.at[n], lr.at[n], dep_of(0, n - 3), r)

    def right_copy(n):
        if n == 0:
            return remote(rt, rbuf.at[r], rs.at[0], rr.at[0], d, res_of(1, 0))
        if n < 4:
            return remote(rt, rbuf.at[r], rs.at[n], rr.at[n], d, res_of(0, n))
        slot = res_of(1, 0)
        return remote(rbuf.at[slot], rbuf.at[slot], rs.at[n], rr.at[n], d, res_of(0, n - 3))

    def across(n):
        if n == 7:
            return remote(rt, rbuf.at[r], fs.at[7], fr.at[7], d, partner)
        slot = res_of(1, 0) if n == 0 else res_of(0, -n) if n < 4 else res_of(1, 3 - n)
        return remote(rbuf.at[slot], rbuf.at[slot], fs.at[n], fr.at[n], d, partner)

    def up_copy(n):
        dep = lax.rem(d + n, 8)
        return remote(ux.at[dep], up.at[d], us.at[n], ur.at[n], dep, r)

    own_up = pltpu.make_async_copy(ux.at[d], up.at[d], own)
    own_up.start()
    for n in range(4):
        left_copy(n).start()
        right_copy(n).start()
    across(7).start()
    lbuf[d] = lt[...]
    rbuf[r] = rt[...]

    a = lax.broadcasted_iota(jnp.int32, (1024, 1024), 0)
    b = lax.broadcasted_iota(jnp.int32, (1024, 1024), 1)
    hit = ((a // CW) == (b % CW)) & ((a % CW) == (b // CW))
    perm[...] = hit.astype(f32).astype(bf16)

    def outer_step(n, carry):
        at = pl.multiple_of(256 * n, 256)
        zz = (mmt(wo[...], pd[pl.ds(at, 256), :]) * rc[pl.ds(n, 1), :]).astype(bf16)
        rows = []
        for j in range(8):
            rows.append(jnp.concatenate([zz[CW * c:CW * c + CW, CW * j:CW * j + CW] for c in range(CW)], axis=1))
        yy = mm(jnp.concatenate(rows, axis=0), perm[...]).astype(bf16)
        oc1[pl.ds(at, 256), :] = yy
        oc2[:, pl.ds(at, 256)] = yy.T

        @pl.when(n == 1)
        def _():
            left_copy(0).wait_recv()
            for i in range(4, 7):
                left_copy(i).start()

        @pl.when(n == 2)
        def _():
            right_copy(0).wait_recv()
            for i in range(4, 7):
                right_copy(i).start()
            across(0).start()

        @pl.when(n == 6)
        def _():
            for i in range(1, 8):
                up_copy(i).start()

        @pl.when(n == 5)
        def _():
            for i in range(1, 4):
                right_copy(i).wait_recv()
                across(i).start()
        return carry

    lax.fori_loop(0, 8, outer_step, 0)
    for n in range(1, 7):
        left_copy(n).wait_recv()
    for n in range(4, 7):
        right_copy(n).wait_recv()
        across(n).start()

    order = [(1, 1), (1, 2), (1, 3), (1, 0), (0, 1), (0, 2), (0, 3), (0, 0)]

    def pass_over(i):
        return remote(psend.at[i], precv.at[i], ps.at[i], pr.at[i], d, partner)

    def right_part(i):
        target = res_of(1, 0) if i == 3 else res_of(0, order[i][1])
        return remote(rsend.at[i], rrecv.at[i], s2.at[i], r2.at[i], d, target)

    def left_part(i):
        target = dep_of(1, 0) if i == 3 else dep_of(0, order[i][1])
        return remote(lsend.at[i], lrecv.at[i], s3.at[i], r3.at[i], target, r)

    mine = pl.ds(pl.multiple_of(128 * core, 128), 128)
    theirs = pl.ds(pl.multiple_of(128 * (1 - core), 128), 128)
    lall = lbuf[...].reshape(1024, N)
    for i, (flip, step) in enumerate(order):
        at = pl.multiple_of(256 * chip_of(flip, step), 256)
        both[i] = mm(oc1[pl.ds(at, 256), :], lall)
        psend[i] = both[i, theirs, :].astype(bf16)
        pass_over(i).start()
    for i in range(8):
        pass_over(i).wait_recv()
        own = both[i, mine, :] + precv[i].astype(f32)
        if i in (3, 7):
            both[i, mine, :] = own
        else:
            rsend[i] = own.astype(bf16)
            right_part(i).start()
    for n in range(8):
        across(n).wait_recv()
    rall = rbuf[...].reshape(2048, N)
    for i, (flip, step) in enumerate(order):
        at = pl.multiple_of(128 * dep_of(flip, step), 128)
        own = mm(oc2[pl.ds(at, 128), :], rall)
        if i == 3:
            lkeep[...] = own
        elif i == 7:
            lacc[...] = own
        else:
            lsend[i] = own.astype(bf16)
            left_part(i).start()
    for i in range(3):
        right_part(i).wait_recv()
    rsend[3] = (both[3, mine, :] + jnp.sum(rrecv[0:3].astype(f32), 0)).astype(bf16)
    right_part(3).start()
    for i in range(3):
        left_part(i).wait_recv()
    lsend[3] = (lkeep[...] + jnp.sum(lrecv[0:3].astype(f32), 0)).astype(bf16)
    left_part(3).start()
    for i in range(3, 7):
        right_part(i).wait_recv()
    racc = both[7, mine, :] + jnp.sum(rrecv[3:7].astype(f32), 0)
    for n in range(4):
        ro[n] = (racc[CW * n:CW * n + CW, :] * live[n:n + 1, :]).astype(bf16)
    for i in range(3, 7):
        left_part(i).wait_recv()
    lsum = lacc[...] + jnp.sum(lrecv[3:7].astype(f32), 0)
    for n in range(4):
        lo[n] = (lsum[CW * n:CW * n + CW, :] * live[n:n + 1, :]).astype(bf16)
    own_up.wait()
    for n in range(1, 8):
        up_copy(n).wait_recv()
        up_copy(n).wait_send()
    for n in range(7):
        left_copy(n).wait_send()
        right_copy(n).wait_send()
        right_part(n).wait_send()
        left_part(n).wait_send()
    for n in range(8):
        across(n).wait_send()
        pass_over(n).wait_send()


def opm(lt, rt, pd, rc, wo, live, ux):
    sd = jax.ShapeDtypeStruct
    vm = pl.BlockSpec(memory_space=pltpu.VMEM)
    chunk = (128, N)
    V = pltpu.VMEM
    dma = pltpu.SemaphoreType.DMA((8,))
    return pl.pallas_call(
        opm_kernel,
        in_specs=[vm] * 6 + [ANY],
        out_specs=[vm] * 3,
        out_shape=[sd((4, CW, N), bf16)] * 2 + [sd((8, 2, 64, F), bf16)],
        scratch_shapes=[V((1024, 1024), bf16), V((2048, 1024), bf16), V((1024, 2048), bf16),
                        V((8, *chunk), bf16), V((16, *chunk), bf16)] + [V((8, *chunk), bf16)] * 6
        + [V((8, 256, N), f32)] + [V(chunk, f32)] * 2 + [dma] * 14 + [pltpu.SemaphoreType.DMA],
        compiler_params=pltpu.CompilerParams(vmem_limit_bytes=60 * 1024 * 1024, collective_id=1, has_side_effects=True),
        name="outer_product",
    )(lt, rt, pd, rc, wo, live, ux)


def on_device(msa, present, pair, upstream, wq, wk, wv, wg, we, wl, wr, wo):
    def by_row(a):
        return a.reshape(32, 64, F).transpose(1, 0, 2)

    x, p, o, g, at, lt, rt, q, v, kt, ua, ut, pd, recip, livet = fwd(
        msa, upstream, pair, present.T, wq, wk, wv, wg, we, wl.T, wr.T)
    lg, rg, ub = opm(lt.reshape(4 * CW, N), rt.reshape(4 * CW, N), pd.reshape(-1, CZ), recip, wo, livet, ut)
    grad, inter = bwd(x, ua, ub, at, lg, rg, p, o, g, q, v, kt, wq, wk, wv, wg, we, wl.T, wr.T)
    return by_row(grad), by_row(inter)


def solution(mesh):
    rows = P("dep", "res", None)
    in_specs = (rows, P("dep", "res"), P("res", "dep", None), rows) + (P(),) * 8
    return jax.shard_map(on_device, mesh=mesh, in_specs=in_specs, out_specs=(rows, rows), check_vma=False)
```

```python
import functools

import jax
import jax.numpy as jnp
from jax import lax
from jax.experimental import pallas as pl
from jax.experimental.pallas import tpu as pltpu
from jax.sharding import PartitionSpec as P

F = 256
H = 8
DH = 32
N = 512
CW = 32
CZ = 128
EPS = 1e-05
BIG = 1e9
f32 = jnp.float32
bf16 = jnp.bfloat16
SCALE = DH ** (-0.5)
NT = (((1,), (1,)), ((), ()))


def mm(a, b):
    return jnp.dot(a, b, preferred_element_type=f32)


def mmt(a, b):
    return lax.dot_general(a, b, NT, preferred_element_type=f32)


def norm(v, axis):
    c = v - jnp.mean(v, axis, keepdims=True)
    inv = lax.rsqrt(jnp.mean(c * c, axis, keepdims=True) + EPS)
    return c * inv, inv


def spread(rows, h, extra):
    top = (h % 4) * DH
    parts = []
    if top:
        parts.append(jnp.zeros((top, N), bf16))
    parts.append(rows)
    if top < 96:
        parts.append(jnp.zeros((96 - top, N), bf16))
    parts.append(extra)
    return jnp.concatenate(parts, axis=0)


MESH = pl.DeviceIdType.MESH


def remote(src, dst, send, recv, dep, res):
    return pltpu.make_async_remote_copy(src_ref=src, dst_ref=dst, send_sem=send, recv_sem=recv,
                                        device_id={"dep": dep, "res": res}, device_id_type=MESH)


def hail(peers):
    bar = pltpu.get_barrier_semaphore()
    for dep, res in peers:
        pl.semaphore_signal(bar, inc=1, device_id={"dep": dep, "res": res}, device_id_type=MESH)


def gather_all(count):
    pl.semaphore_wait(pltpu.get_barrier_semaphore(), count)


def greet(peers):
    hail(peers)
    gather_all(len(peers))


def fwd_kernel(x_in, u_in, pair_in, present, wq, wk, wv, wg, we, wl, wr,
               x_ref, p_out, o_ref, g_ref, a_ref, l_ref, r_ref, q_ref, v_ref, kt_ref, ut_out, pd_out, rc_ref, live_out,
               wt, bias_s, st_s, p_buf, live_in, hx, ux, px, xbuf, lbuf, livet, jbuf, mine,
               xs, xr, ps, pr, ls, lr, js, jr, own, p_sem):
    k = pl.program_id(0)
    d = lax.axis_index("dep")
    r = lax.axis_index("res")

    def dep_at(n):
        return lax.rem(d + n, 8)

    def res_at(n):
        return lax.rem(r + n, 16)

    def x_copy(c, n):
        return remote(hx.at[dep_at(n), c], xbuf.at[c, d], xs.at[c, n], xr.at[c, n], dep_at(n), r)

    def pd_copy(n):
        return remote(px.at[:, dep_at(n)], pd_out.at[d], ps.at[n], pr.at[n], dep_at(n), r)

    def live_copy(n):
        return remote(live_in, lbuf.at[d], ls.at[n], lr.at[n], dep_at(n), r)

    def row_copy(n):
        return remote(mine, jbuf.at[r], js.at[n], jr.at[n], d, res_at(n))

    own_pd = pltpu.make_async_copy(px.at[:, d], pd_out.at[d], own.at[1])
    later_up = pltpu.make_async_copy(ux, ut_out, own.at[2])

    half = lax.rem(k, 2)

    def p_copy(at, h):
        return pltpu.make_async_copy(p_buf.at[lax.rem(at, 2), h], p_out.at[at, h], p_sem.at[lax.rem(at, 2), h])

    @pl.when(k > 1)
    def _():
        for h in range(H):
            p_copy(k - 2, h).wait()

    @pl.when(k == 0)
    def _():
        hail([(dep_at(n), r) for n in range(1, 8)] + [(d, res_at(n)) for n in range(1, 16)])
        hx[...] = jnp.transpose(x_in[...], (1, 0, 2)).reshape(hx.shape)
        flat = jnp.concatenate([present[...].astype(f32), jnp.zeros((CW, 64), f32)], axis=1)
        held = jnp.concatenate([flat, jnp.zeros((96, 128), f32)], axis=0).T[:64].astype(bf16)
        live_in[...] = held
        lbuf[d] = held
        gather_all(22)
        for n in range(1, 8):
            live_copy(n).start()
        for n in range(1, 8):
            x_copy(0, n).start()
        for c in range(4):
            xbuf[c, d] = hx[d, c]
        for n, w in enumerate((wq, wv, wg, we)):
            wt[n] = w[...].T
        px[...] = jnp.transpose(pair_in[...], (1, 0, 2)).reshape(px.shape)
        ux[...] = jnp.transpose(u_in[...], (1, 0, 2)).reshape(ux.shape)
        for n in range(1, 8):
            live_copy(n).wait_recv()
        live = lbuf[...].reshape(N, 128).astype(f32)
        bias_s[...] = ((live - 1.0) * BIG).astype(bf16)
        livet[...] = live.T
        rows = [livet[pl.ds(4 * d + n, 1), :] for n in range(4)]
        held = jnp.concatenate(rows + [jnp.zeros((4, N), f32)], axis=0)
        mine[...] = held
        live_out[...] = held
        jbuf[r] = held
        for n in range(1, 16):
            row_copy(n).start()
        for n in range(1, 8):
            x_copy(0, n).wait_send()
        for n in range(1, 8):
            x_copy(1, n).start()

    @pl.when(k == 1)
    def _():
        for n in range(1, 8):
            pd_copy(n).start()
        own_pd.start()
        later_up.start()

    @pl.when(k == 3)
    def _():
        for n in range(1, 16):
            row_copy(n).wait_recv()
        counts = mm(jbuf[...].reshape(128, N).astype(bf16), lbuf[...].reshape(N, 128))
        rec = 1.0 / (0.001 + counts)
        for n in range(8):
            pieces = []
            for j in range(8):
                at = 16 * n + 8 * (j // 4) + j % 4
                pieces.append(rec[at:at + 1, :CW])
            rc_ref[n:n + 1, :] = jnp.concatenate(pieces, axis=1)

    for n in range(1, 8):
        x_copy(k, n).wait_recv()
    xin = xbuf[k].reshape(N, F)
    x_ref[...] = xin.reshape(x_ref.shape)
    xhat, _ = norm(xin.astype(f32), 1)
    xb = xhat.astype(bf16)
    xbt = xb.T
    qt = (mm(wt[0], xbt) * SCALE).astype(bf16)
    vt = mm(wt[1], xbt).astype(bf16)
    kk = mm(xb, wk[...]).astype(bf16)
    gt = jax.nn.sigmoid(mm(wt[2], xbt))
    q_ref[0] = qt.T
    v_ref[0] = vt.T
    kt_ref[0] = kk.T
    g_ref[0] = gt
    extra = (lax.broadcasted_iota(jnp.int32, (128, N), 0) == 4 * d + k).astype(f32).astype(bf16)
    bias = bias_s[...]
    PIECE = 128

    def operands(h):
        grp = h // 4
        return jnp.concatenate([kk[:, 128 * grp:128 * grp + 128], bias], axis=1), spread(qt[DH * h:DH * h + DH], h, extra)

    def score(ops, h, i):
        val = mm(ops[0][i:i + PIECE], ops[1])
        st_s[h % 2, i:i + PIECE, :] = val
        return jnp.max(val, 0, keepdims=True)

    def blend(h):
        o_ref[0, DH * h:DH * h + DH, :] = mm(vt[DH * h:DH * h + DH], p_buf[half, h])

    ops = operands(0)
    peak = functools.reduce(jnp.maximum, [score(ops, 0, i) for i in range(0, N, PIECE)])
    def push_x(at, c):
        @pl.when(k == at)
        def _():
            for n in range(1, 8):
                x_copy(c, n).start()

    for h in range(H):
        if h == 2:
            push_x(0, 2)
        if h == 5:
            push_x(0, 3)
        b = h % 2
        if h + 1 < H:
            ops = operands(h + 1)
        nxt = []
        tot = jnp.zeros((1, N), f32)
        for i in range(0, N, PIECE):
            if h + 1 < H:
                nxt.append(score(ops, h + 1, i))
            e = jnp.exp(st_s[b, i:i + PIECE, :] - peak)
            st_s[b, i:i + PIECE, :] = e
            tot = tot + jnp.sum(e, 0, keepdims=True)
        if h:
            blend(h - 1)
        inv = 1.0 / tot
        for i in range(0, N, PIECE):
            p_buf[half, h, i:i + PIECE, :] = (st_s[b, i:i + PIECE, :] * inv).astype(bf16)
        p_copy(k, h).start()
        if nxt:
            peak = functools.reduce(jnp.maximum, nxt)
    blend(H - 1)
    gated = (gt * o_ref[0]).astype(bf16)
    up = mm(wt[3], gated)
    after = (xin.T.astype(f32) + up).astype(bf16)
    a_ref[0] = after
    yhat, _ = norm(after.astype(f32), 0)
    yb = yhat.astype(bf16)
    live = livet[pl.ds(4 * d + k, 1), :]
    l_ref[0] = (mm(wl[...], yb) * live).astype(bf16)
    r_ref[0] = (mm(wr[...], yb) * live).astype(bf16)

    @pl.when(k == 3)
    def _():
        for n in range(1, 8):
            pd_copy(n).wait_recv()
        own_pd.wait()
        later_up.wait()
        for h in range(H):
            p_copy(2, h).wait()
            p_copy(3, h).wait()
        for n in range(1, 8):
            live_copy(n).wait_send()
            pd_copy(n).wait_send()
            for c in range(1, 4):
                x_copy(c, n).wait_send()
        for n in range(1, 16):
            row_copy(n).wait_send()


def bwd_kernel(x_ref, up_ref, at_ref, lg_ref, rg_ref, p_in, o_ref, g_ref, q_ref, v_ref, kt_ref, wq, wk, wv, wg, we, wl, wr,
               out_g, out_i, p_buf, ds_s, acc_q, acc_v, acc_t, dt_s, sbuf, ss, rs, own, p_sem):
    k = pl.program_id(0)
    d = lax.axis_index("dep")
    r = lax.axis_index("res")
    outs = (out_g, out_i)

    def dep_at(n):
        return lax.rem(d + n, 8)

    def send(which, c, n):
        return remote(sbuf.at[which, c, dep_at(n)], outs[which].at[d, c],
                      ss.at[which, c, n], rs.at[which, c, n], dep_at(n), r)

    def keep(which, c):
        return pltpu.make_async_copy(sbuf.at[which, c, d], outs[which].at[d, c], own.at[which, c])

    def ship(which, c, value):
        sbuf[which, c] = value.T.reshape(8, 64, F)
        for n in range(1, 8):
            send(which, c, n).start()
        keep(which, c).start()

    half = lax.rem(k, 2)

    def p_copy(at):
        return pltpu.make_async_copy(p_in.at[at], p_buf.at[lax.rem(at, 2)], p_sem.at[lax.rem(at, 2)])

    @pl.when(k == 0)
    def _():
        p_copy(0).start()
        p_copy(1).start()
        wlt, wrt = wl[...].T, wr[...].T
        greet([(dep_at(n), r) for n in range(1, 8)])
        for c in range(4):
            yhat, yinv = norm(at_ref[c].astype(f32), 0)
            dy = mm(wlt, lg_ref[c]) + mm(wrt, rg_ref[c])
            m1 = jnp.mean(dy, 0, keepdims=True)
            m2 = jnp.mean(dy * yhat, 0, keepdims=True)
            upt = up_ref[:, c].reshape(N, F).T.astype(f32)
            dt_s[c] = (yinv * (dy - m1 - yhat * m2) + upt).astype(bf16)
            ship(1, c, dt_s[c])

    p_copy(k).wait()
    xin = x_ref[...].reshape(N, F)
    q = q_ref[0]
    v = v_ref[0]
    kt = kt_ref[0]
    gt = g_ref[0]
    ot = o_ref[0]
    dt = dt_s[k]
    dg = mm(we[...], dt).astype(bf16).astype(f32)
    dot_ = (dg * gt).astype(bf16)
    dpre = (dg * ot * gt * (1.0 - gt)).astype(bf16)
    prod = dot_.astype(f32) * ot
    row = lax.broadcasted_iota(jnp.int32, (128, N), 0)
    col = lax.broadcasted_iota(jnp.int32, (N, 128), 1)
    ones = (col < 2).astype(f32).astype(bf16)
    lane = lax.broadcasted_iota(jnp.int32, (N, F), 1) // DH
    zero = jnp.zeros((), bf16)

    def back(h):
        sl = slice(DH * h, DH * h + DH)
        acc_q[sl, :] = mm(kt[sl], ds_s[h])

    def dops(h):
        grp = h // 4
        sl = slice(DH * h, DH * h + DH)
        dd = -jnp.sum(prod[sl], 0, keepdims=True)
        hi = dd.astype(bf16).astype(f32)
        lo = dd - hi
        extra = jnp.where(row == 0, hi, jnp.where(row == 1, lo, 0.0)).astype(bf16)
        return jnp.concatenate([v[:, 128 * grp:128 * grp + 128], ones], axis=1), spread(dot_[sl], h, extra)

    def wide_v(h):
        sl = slice(DH * h, DH * h + DH)
        acc_v[sl, :] = mmt(dot_[sl], p_buf[half, h])

    def tall_k(h, i):
        ext = mm(ds_s[h, i:i + 256, :], jnp.where(lane == h, q, zero))
        if h:
            acc_t[i:i + 256, :] += ext
        else:
            acc_t[i:i + 256, :] = ext

    for h in range(H):
        ops = dops(h)
        for i in range(0, N, 256):
            dp = mm(ops[0][i:i + 256], ops[1])
            ds_s[h, i:i + 256, :] = (p_buf[half, h, i:i + 256, :].astype(f32) * dp).astype(bf16)
            if h:
                tall_k(h - 1, i)
        wide_v(h)
        if h:
            back(h - 1)
    back(H - 1)
    for i in range(0, N, 256):
        tall_k(H - 1, i)
    dq = (acc_q[...].astype(bf16).astype(f32) * SCALE).astype(bf16)
    dx = (mm(wq[...], dq) + mm(wg[...], dpre)
          + mmt(wk[...], acc_t[...].astype(bf16)) + mm(wv[...], acc_v[...].astype(bf16)))
    dx = dx.astype(bf16).astype(f32)
    xt = xin.T.astype(f32)
    xh, inv = norm(xt, 0)
    m1 = jnp.mean(dx, 0, keepdims=True)
    m2 = jnp.mean(dx * xh, 0, keepdims=True)
    dln = (inv * (dx - m1 - xh * m2)).astype(bf16)
    out = (dt.astype(f32) + dln.astype(f32)).astype(bf16)
    ship(0, k, out)

    @pl.when(k < 2)
    def _():
        p_copy(k + 2).start()

    @pl.when(k == 3)
    def _():
        for which in range(2):
            for c in range(4):
                keep(which, c).wait()
                for n in range(1, 8):
                    send(which, c, n).wait_recv()
                    send(which, c, n).wait_send()


def whole(shape):
    return pl.BlockSpec(shape, lambda k: (0,) * len(shape))


def percol(shape):
    return pl.BlockSpec((1, *shape), lambda k: (k,) + (0,) * len(shape))


COLS = pl.BlockSpec((8, 1, 64, F), lambda k: (0, k, 0, 0))
ANY = pl.BlockSpec(memory_space=pl.ANY)


def fwd(msa, upstream, pair, live, wq, wk, wv, wg, we, wl, wr):
    sd = jax.ShapeDtypeStruct
    V = pltpu.VMEM
    dma = pltpu.SemaphoreType.DMA
    return pl.pallas_call(
        fwd_kernel,
        grid=(4,),
        in_specs=[whole((64, 32, F))] * 2 + [whole((32, 64, CZ)), whole((CW, 64))] + [whole((F, F))] * 5 + [whole((CW, F))] * 2,
        out_specs=[COLS, ANY, percol((F, N)), percol((F, N)), percol((F, N)), percol((CW, N)),
                   percol((CW, N)), percol((N, F)), percol((N, F)), percol((F, N)), ANY, ANY, whole((8, 256)), whole((8, N))],
        out_shape=[sd((8, 4, 64, F), bf16), sd((4, H, N, N), bf16), sd((4, F, N), f32), sd((4, F, N), f32),
                   sd((4, F, N), bf16), sd((4, CW, N), bf16), sd((4, CW, N), bf16),
                   sd((4, N, F), bf16), sd((4, N, F), bf16), sd((4, F, N), bf16), sd((8, 4, 64, F), bf16), sd((8, 2, 4, CW, CZ), bf16), sd((8, 256), f32), sd((8, N), f32)],
        scratch_shapes=[V((4, F, F), bf16), V((N, 128), bf16), V((2, N, N), f32), V((2, H, N, N), bf16), V((64, 128), bf16), V((8, 4, 64, F), bf16), V((8, 4, 64, F), bf16), V((2, 8, 4, CW, CZ), bf16), V((4, 8, 64, F), bf16),
                        V((8, 64, 128), bf16), V((128, N), f32), V((16, 8, N), f32), V((8, N), f32),
                        dma((4, 8)), dma((4, 8))] + [dma((8,))] * 4 + [dma((16,))] * 2 + [dma((8,)), dma((2, 8))],
        compiler_params=pltpu.CompilerParams(vmem_limit_bytes=60 * 1024 * 1024, collective_id=2, has_side_effects=True,
                                             dimension_semantics=("arbitrary",)),
        name="attention_forward",
    )(msa, upstream, pair, live, wq, wk, wv, wg, we, wl, wr)


def bwd(x, up, at, lg, rg, p, o, g, q, v, kt, wq, wk, wv, wg, we, wl, wr):
    sd = jax.ShapeDtypeStruct
    V = pltpu.VMEM
    dma = pltpu.SemaphoreType.DMA
    return pl.pallas_call(
        bwd_kernel,
        grid=(4,),
        in_specs=[COLS, whole((8, 4, 64, F)), whole((4, F, N)), whole((4, CW, N)), whole((4, CW, N)), ANY, percol((F, N)),
                  percol((F, N)), percol((N, F)), percol((N, F)), percol((F, N))] + [whole((F, F))] * 5 + [whole((CW, F))] * 2,
        out_specs=[ANY, ANY],
        out_shape=[sd((8, 4, 64, F), bf16)] * 2,
        scratch_shapes=[V((2, H, N, N), bf16), V((H, N, N), bf16), V((F, N), f32), V((F, N), f32), V((N, F), f32), V((4, F, N), bf16), V((2, 4, 8, 64, F), bf16),
                        dma((2, 4, 8)), dma((2, 4, 8)), dma((2, 4)), dma((2,))],
        compiler_params=pltpu.CompilerParams(vmem_limit_bytes=60 * 1024 * 1024, collective_id=3, has_side_effects=True,
                                             dimension_semantics=("arbitrary",)),
        name="attention_backward",
    )(x, up, at, lg, rg, p, o, g, q, v, kt, wq, wk, wv, wg, we, wl, wr)


def opm_kernel(lt, rt, pd, rc, wo, live, ux, lo, ro, up,
               perm, oc1, oc2, lbuf, rbuf, lsend, lrecv, psend, precv, rsend, rrecv, both, lkeep, lacc,
               ls, lr, rs, rr, fs, fr, ps, pr, s2, r2, s3, r3, us, ur, own):
    d = lax.axis_index("dep")
    r = lax.axis_index("res")
    xl, z = d // 4, lax.rem(d, 4)
    y, xh, core = r // 4, lax.rem(r // 2, 2), lax.rem(r, 2)

    def dep_of(flip, step):
        return 4 * lax.rem(xl + flip, 2) + lax.rem(z + step + 4, 4)

    def chip_of(flip, step):
        return 2 * lax.rem(y + step + 4, 4) + lax.rem(xh + flip, 2)

    def res_of(flip, step):
        return 2 * chip_of(flip, step) + core

    partner = 2 * chip_of(0, 0) + 1 - core
    greet([(lax.rem(d + n, 8), r) for n in range(1, 8)]
          + [(d, res_of(0, n)) for n in range(1, 4)] + [(d, res_of(1, 0)), (d, partner)])

    def left_copy(n):
        if n == 0:
            return remote(lt, lbuf.at[d], ls.at[0], lr.at[0], dep_of(1, 0), r)
        if n < 4:
            return remote(lt, lbuf.at[d], ls.at[n], lr.at[n], dep_of(0, n), r)
        slot = dep_of(1, 0)
        return remote(lbuf.at[slot], lbuf.at[slot], ls.at[n], lr.at[n], dep_of(0, n - 3), r)

    def right_copy(n):
        if n == 0:
            return remote(rt, rbuf.at[r], rs.at[0], rr.at[0], d, res_of(1, 0))
        if n < 4:
            return remote(rt, rbuf.at[r], rs.at[n], rr.at[n], d, res_of(0, n))
        slot = res_of(1, 0)
        return remote(rbuf.at[slot], rbuf.at[slot], rs.at[n], rr.at[n], d, res_of(0, n - 3))

    def across(n):
        if n == 7:
            return remote(rt, rbuf.at[r], fs.at[7], fr.at[7], d, partner)
        slot = res_of(1, 0) if n == 0 else res_of(0, -n) if n < 4 else res_of(1, 3 - n)
        return remote(rbuf.at[slot], rbuf.at[slot], fs.at[n], fr.at[n], d, partner)

    def up_copy(n):
        dep = lax.rem(d + n, 8)
        return remote(ux.at[dep], up.at[d], us.at[n], ur.at[n], dep, r)

    own_up = pltpu.make_async_copy(ux.at[d], up.at[d], own)
    own_up.start()
    for n in range(4):
        left_copy(n).start()
        right_copy(n).start()
    across(7).start()
    lbuf[d] = lt[...]
    rbuf[r] = rt[...]

    a = lax.broadcasted_iota(jnp.int32, (1024, 1024), 0)
    b = lax.broadcasted_iota(jnp.int32, (1024, 1024), 1)
    hit = ((a // CW) == (b % CW)) & ((a % CW) == (b // CW))
    perm[...] = hit.astype(f32).astype(bf16)

    def outer_step(n, carry):
        at = pl.multiple_of(256 * n, 256)
        zz = (mmt(wo[...], pd[pl.ds(at, 256), :]) * rc[pl.ds(n, 1), :]).astype(bf16)
        rows = []
        for j in range(8):
            rows.append(jnp.concatenate([zz[CW * c:CW * c + CW, CW * j:CW * j + CW] for c in range(CW)], axis=1))
        yy = mm(jnp.concatenate(rows, axis=0), perm[...]).astype(bf16)
        oc1[pl.ds(at, 256), :] = yy
        oc2[:, pl.ds(at, 256)] = yy.T

        @pl.when(n == 1)
        def _():
            left_copy(0).wait_recv()
            for i in range(4, 7):
                left_copy(i).start()

        @pl.when(n == 2)
        def _():
            right_copy(0).wait_recv()
            for i in range(4, 7):
                right_copy(i).start()
            across(0).start()

        @pl.when(n == 6)
        def _():
            for i in range(1, 8):
                up_copy(i).start()

        @pl.when(n == 5)
        def _():
            for i in range(1, 4):
                right_copy(i).wait_recv()
                across(i).start()
        return carry

    lax.fori_loop(0, 8, outer_step, 0)
    for n in range(1, 7):
        left_copy(n).wait_recv()
    for n in range(4, 7):
        right_copy(n).wait_recv()
        across(n).start()

    order = [(1, 1), (1, 2), (1, 3), (1, 0), (0, 1), (0, 2), (0, 3), (0, 0)]

    def pass_over(i):
        return remote(psend.at[i], precv.at[i], ps.at[i], pr.at[i], d, partner)

    def right_part(i):
        target = res_of(1, 0) if i == 3 else res_of(0, order[i][1])
        return remote(rsend.at[i], rrecv.at[i], s2.at[i], r2.at[i], d, target)

    def left_part(i):
        target = dep_of(1, 0) if i == 3 else dep_of(0, order[i][1])
        return remote(lsend.at[i], lrecv.at[i], s3.at[i], r3.at[i], target, r)

    mine = pl.ds(pl.multiple_of(128 * core, 128), 128)
    theirs = pl.ds(pl.multiple_of(128 * (1 - core), 128), 128)
    lall = lbuf[...].reshape(1024, N)
    for i, (flip, step) in enumerate(order):
        at = pl.multiple_of(256 * chip_of(flip, step), 256)
        both[i] = mm(oc1[pl.ds(at, 256), :], lall)
        psend[i] = both[i, theirs, :].astype(bf16)
        pass_over(i).start()
    for i in range(8):
        pass_over(i).wait_recv()
        own = both[i, mine, :] + precv[i].astype(f32)
        if i in (3, 7):
            both[i, mine, :] = own
        else:
            rsend[i] = own.astype(bf16)
            right_part(i).start()
    for n in range(8):
        across(n).wait_recv()
    rall = rbuf[...].reshape(2048, N)
    for i, (flip, step) in enumerate(order):
        at = pl.multiple_of(128 * dep_of(flip, step), 128)
        own = mm(oc2[pl.ds(at, 128), :], rall)
        if i == 3:
            lkeep[...] = own
        elif i == 7:
            lacc[...] = own
        else:
            lsend[i] = own.astype(bf16)
            left_part(i).start()
    for i in range(3):
        right_part(i).wait_recv()
    rsend[3] = (both[3, mine, :] + jnp.sum(rrecv[0:3].astype(f32), 0)).astype(bf16)
    right_part(3).start()
    for i in range(3):
        left_part(i).wait_recv()
    lsend[3] = (lkeep[...] + jnp.sum(lrecv[0:3].astype(f32), 0)).astype(bf16)
    left_part(3).start()
    for i in range(3, 7):
        right_part(i).wait_recv()
    racc = both[7, mine, :] + jnp.sum(rrecv[3:7].astype(f32), 0)
    for n in range(4):
        ro[n] = (racc[CW * n:CW * n + CW, :] * live[n:n + 1, :]).astype(bf16)
    for i in range(3, 7):
        left_part(i).wait_recv()
    lsum = lacc[...] + jnp.sum(lrecv[3:7].astype(f32), 0)
    for n in range(4):
        lo[n] = (lsum[CW * n:CW * n + CW, :] * live[n:n + 1, :]).astype(bf16)
    own_up.wait()
    for n in range(1, 8):
        up_copy(n).wait_recv()
        up_copy(n).wait_send()
    for n in range(7):
        left_copy(n).wait_send()
        right_copy(n).wait_send()
        right_part(n).wait_send()
        left_part(n).wait_send()
    for n in range(8):
        across(n).wait_send()
        pass_over(n).wait_send()


def opm(lt, rt, pd, rc, wo, live, ux):
    sd = jax.ShapeDtypeStruct
    vm = pl.BlockSpec(memory_space=pltpu.VMEM)
    chunk = (128, N)
    V = pltpu.VMEM
    dma = pltpu.SemaphoreType.DMA((8,))
    return pl.pallas_call(
        opm_kernel,
        in_specs=[vm] * 6 + [ANY],
        out_specs=[vm] * 3,
        out_shape=[sd((4, CW, N), bf16)] * 2 + [sd((8, 4, 64, F), bf16)],
        scratch_shapes=[V((1024, 1024), bf16), V((2048, 1024), bf16), V((1024, 2048), bf16),
                        V((8, *chunk), bf16), V((16, *chunk), bf16)] + [V((8, *chunk), bf16)] * 6
        + [V((8, 256, N), f32)] + [V(chunk, f32)] * 2 + [dma] * 14 + [pltpu.SemaphoreType.DMA],
        compiler_params=pltpu.CompilerParams(vmem_limit_bytes=60 * 1024 * 1024, collective_id=1, has_side_effects=True),
        name="outer_product",
    )(lt, rt, pd, rc, wo, live, ux)


def on_device(msa, present, pair, upstream, wq, wk, wv, wg, we, wl, wr, wo):
    def by_row(a):
        return a.reshape(32, 64, F).transpose(1, 0, 2)

    x, p, o, g, at, lt, rt, q, v, kt, ut, pd, recip, livet = fwd(
        msa, upstream, pair, present.T, wq, wk, wv, wg, we, wl.T, wr.T)
    lg, rg, up = opm(lt.reshape(4 * CW, N), rt.reshape(4 * CW, N), pd.reshape(-1, CZ), recip, wo, livet, ut)
    grad, inter = bwd(x, up, at, lg, rg, p, o, g, q, v, kt, wq, wk, wv, wg, we, wl.T, wr.T)
    return by_row(grad), by_row(inter)


def solution(mesh):
    rows = P("dep", "res", None)
    in_specs = (rows, P("dep", "res"), P("res", "dep", None), rows) + (P(),) * 8
    return jax.shard_map(on_device, mesh=mesh, in_specs=in_specs, out_specs=(rows, rows), check_vma=False)
```

```python
import functools

import jax
import jax.numpy as jnp
from jax import lax
from jax.experimental import pallas as pl
from jax.experimental.pallas import tpu as pltpu
from jax.sharding import PartitionSpec as P

F = 256
H = 8
DH = 32
N = 512
CW = 32
CZ = 128
EPS = 1e-05
BIG = 1e9
f32 = jnp.float32
bf16 = jnp.bfloat16
SCALE = DH ** (-0.5)
NT = (((1,), (1,)), ((), ()))


def mm(a, b):
    return jnp.dot(a, b, preferred_element_type=f32)


def mmt(a, b):
    return lax.dot_general(a, b, NT, preferred_element_type=f32)


def norm(v, axis):
    c = v - jnp.mean(v, axis, keepdims=True)
    inv = lax.rsqrt(jnp.mean(c * c, axis, keepdims=True) + EPS)
    return c * inv, inv


def spread(rows, h, extra):
    top = (h % 4) * DH
    parts = []
    if top:
        parts.append(jnp.zeros((top, N), bf16))
    parts.append(rows)
    if top < 96:
        parts.append(jnp.zeros((96 - top, N), bf16))
    parts.append(extra)
    return jnp.concatenate(parts, axis=0)


MESH = pl.DeviceIdType.MESH


def remote(src, dst, send, recv, dep, res):
    return pltpu.make_async_remote_copy(src_ref=src, dst_ref=dst, send_sem=send, recv_sem=recv,
                                        device_id={"dep": dep, "res": res}, device_id_type=MESH)


def hail(peers):
    bar = pltpu.get_barrier_semaphore()
    for dep, res in peers:
        pl.semaphore_signal(bar, inc=1, device_id={"dep": dep, "res": res}, device_id_type=MESH)


def gather_all(count):
    pl.semaphore_wait(pltpu.get_barrier_semaphore(), count)


def greet(peers):
    hail(peers)
    gather_all(len(peers))


def fwd_kernel(x_in, u_in, pair_in, present, wq, wk, wv, wg, we, wl, wr,
               x_ref, p_out, o_ref, g_ref, a_ref, l_ref, r_ref, q_ref, v_ref, kt_ref, up_out, ut_out, pd_out, rc_ref, live_out,
               wt, bias_s, st_s, p_buf, live_in, hx, ux, px, xbuf, lbuf, livet, jbuf, mine,
               xs, xr, us, ur, ps, pr, ls, lr, js, jr, own, p_sem):
    k = pl.program_id(0)
    d = lax.axis_index("dep")
    r = lax.axis_index("res")

    def dep_at(n):
        return lax.rem(d + n, 8)

    def res_at(n):
        return lax.rem(r + n, 16)

    def x_copy(c, n):
        return remote(hx.at[dep_at(n), c], xbuf.at[c, d], xs.at[c, n], xr.at[c, n], dep_at(n), r)

    def up_copy(c, n):
        return remote(ux.at[dep_at(n), c], up_out.at[d, c], us.at[c, n], ur.at[c, n], dep_at(n), r)

    def pd_copy(n):
        return remote(px.at[:, dep_at(n)], pd_out.at[d], ps.at[n], pr.at[n], dep_at(n), r)

    def live_copy(n):
        return remote(live_in, lbuf.at[d], ls.at[n], lr.at[n], dep_at(n), r)

    def row_copy(n):
        return remote(mine, jbuf.at[r], js.at[n], jr.at[n], d, res_at(n))

    own_up = pltpu.make_async_copy(ux.at[d, pl.ds(0, 2)], up_out.at[d], own.at[0])
    own_pd = pltpu.make_async_copy(px.at[:, d], pd_out.at[d], own.at[1])
    later_up = pltpu.make_async_copy(ux.at[:, pl.ds(2, 2)], ut_out, own.at[2])

    half = lax.rem(k, 2)

    def p_copy(at, h):
        return pltpu.make_async_copy(p_buf.at[lax.rem(at, 2), h], p_out.at[at, h], p_sem.at[lax.rem(at, 2), h])

    @pl.when(k > 1)
    def _():
        for h in range(H):
            p_copy(k - 2, h).wait()

    @pl.when(k == 0)
    def _():
        hail([(dep_at(n), r) for n in range(1, 8)] + [(d, res_at(n)) for n in range(1, 16)])
        hx[...] = jnp.transpose(x_in[...], (1, 0, 2)).reshape(hx.shape)
        flat = jnp.concatenate([present[...].astype(f32), jnp.zeros((CW, 64), f32)], axis=1)
        held = jnp.concatenate([flat, jnp.zeros((96, 128), f32)], axis=0).T[:64].astype(bf16)
        live_in[...] = held
        lbuf[d] = held
        gather_all(22)
        for n in range(1, 8):
            live_copy(n).start()
        for n in range(1, 8):
            x_copy(0, n).start()
        for c in range(4):
            xbuf[c, d] = hx[d, c]
        for n, w in enumerate((wq, wv, wg, we)):
            wt[n] = w[...].T
        px[...] = jnp.transpose(pair_in[...], (1, 0, 2)).reshape(px.shape)
        ux[...] = jnp.transpose(u_in[...], (1, 0, 2)).reshape(ux.shape)
        for n in range(1, 8):
            live_copy(n).wait_recv()
        live = lbuf[...].reshape(N, 128).astype(f32)
        bias_s[...] = ((live - 1.0) * BIG).astype(bf16)
        livet[...] = live.T
        rows = [livet[pl.ds(4 * d + n, 1), :] for n in range(4)]
        held = jnp.concatenate(rows + [jnp.zeros((4, N), f32)], axis=0)
        mine[...] = held
        live_out[...] = held
        jbuf[r] = held
        for n in range(1, 16):
            row_copy(n).start()
        for n in range(1, 8):
            x_copy(0, n).wait_send()
        for n in range(1, 8):
            x_copy(1, n).start()

    @pl.when(k == 1)
    def _():
        for n in range(1, 8):
            pd_copy(n).start()
        own_up.start()
        own_pd.start()
        later_up.start()

    @pl.when(k == 2)
    def _():
        for n in range(1, 8):
            up_copy(1, n).start()

    @pl.when(k == 3)
    def _():
        for n in range(1, 16):
            row_copy(n).wait_recv()
        counts = mm(jbuf[...].reshape(128, N).astype(bf16), lbuf[...].reshape(N, 128))
        rec = 1.0 / (0.001 + counts)
        for n in range(8):
            pieces = []
            for j in range(8):
                at = 16 * n + 8 * (j // 4) + j % 4
                pieces.append(rec[at:at + 1, :CW])
            rc_ref[n:n + 1, :] = jnp.concatenate(pieces, axis=1)

    for n in range(1, 8):
        x_copy(k, n).wait_recv()
    xin = xbuf[k].reshape(N, F)
    x_ref[...] = xin.reshape(x_ref.shape)
    xhat, _ = norm(xin.astype(f32), 1)
    xb = xhat.astype(bf16)
    xbt = xb.T
    qt = (mm(wt[0], xbt) * SCALE).astype(bf16)
    vt = mm(wt[1], xbt).astype(bf16)
    kk = mm(xb, wk[...]).astype(bf16)
    gt = jax.nn.sigmoid(mm(wt[2], xbt))
    q_ref[0] = qt.T
    v_ref[0] = vt.T
    kt_ref[0] = kk.T
    g_ref[0] = gt
    extra = (lax.broadcasted_iota(jnp.int32, (128, N), 0) == 4 * d + k).astype(f32).astype(bf16)
    bias = bias_s[...]
    PIECE = 128

    def operands(h):
        grp = h // 4
        return jnp.concatenate([kk[:, 128 * grp:128 * grp + 128], bias], axis=1), spread(qt[DH * h:DH * h + DH], h, extra)

    def score(ops, h, i):
        val = mm(ops[0][i:i + PIECE], ops[1])
        st_s[h % 2, i:i + PIECE, :] = val
        return jnp.max(val, 0, keepdims=True)

    def blend(h):
        o_ref[0, DH * h:DH * h + DH, :] = mm(vt[DH * h:DH * h + DH], p_buf[half, h])

    ops = operands(0)
    peak = functools.reduce(jnp.maximum, [score(ops, 0, i) for i in range(0, N, PIECE)])
    def push_x(at, c):
        @pl.when(k == at)
        def _():
            for n in range(1, 8):
                x_copy(c, n).start()

    def push_up(at, c):
        @pl.when(k == at)
        def _():
            for n in range(1, 8):
                up_copy(c, n).start()

    for h in range(H):
        if h == 2:
            push_x(0, 2)
        if h == 4:
            push_up(1, 0)
        if h == 5:
            push_x(0, 3)
        b = h % 2
        if h + 1 < H:
            ops = operands(h + 1)
        nxt = []
        tot = jnp.zeros((1, N), f32)
        for i in range(0, N, PIECE):
            if h + 1 < H:
                nxt.append(score(ops, h + 1, i))
            e = jnp.exp(st_s[b, i:i + PIECE, :] - peak)
            st_s[b, i:i + PIECE, :] = e
            tot = tot + jnp.sum(e, 0, keepdims=True)
        if h:
            blend(h - 1)
        inv = 1.0 / tot
        for i in range(0, N, PIECE):
            p_buf[half, h, i:i + PIECE, :] = (st_s[b, i:i + PIECE, :] * inv).astype(bf16)
        p_copy(k, h).start()
        if nxt:
            peak = functools.reduce(jnp.maximum, nxt)
    blend(H - 1)
    gated = (gt * o_ref[0]).astype(bf16)
    up = mm(wt[3], gated)
    after = (xin.T.astype(f32) + up).astype(bf16)
    a_ref[0] = after
    yhat, _ = norm(after.astype(f32), 0)
    yb = yhat.astype(bf16)
    live = livet[pl.ds(4 * d + k, 1), :]
    l_ref[0] = (mm(wl[...], yb) * live).astype(bf16)
    r_ref[0] = (mm(wr[...], yb) * live).astype(bf16)

    @pl.when(k == 3)
    def _():
        for n in range(1, 8):
            pd_copy(n).wait_recv()
            for c in range(2):
                up_copy(c, n).wait_recv()
        own_up.wait()
        own_pd.wait()
        later_up.wait()
        for h in range(H):
            p_copy(2, h).wait()
            p_copy(3, h).wait()
        for n in range(1, 8):
            live_copy(n).wait_send()
            pd_copy(n).wait_send()
            for c in range(2):
                up_copy(c, n).wait_send()
            for c in range(1, 4):
                x_copy(c, n).wait_send()
        for n in range(1, 16):
            row_copy(n).wait_send()


def bwd_kernel(x_ref, ua_ref, ub_ref, at_ref, lg_ref, rg_ref, p_in, o_ref, g_ref, q_ref, v_ref, kt_ref, wq, wk, wv, wg, we, wl, wr,
               out_g, out_i, p_buf, ds_s, acc_q, acc_v, acc_t, dt_s, sbuf, ss, rs, own, p_sem):
    k = pl.program_id(0)
    d = lax.axis_index("dep")
    r = lax.axis_index("res")
    outs = (out_g, out_i)

    def dep_at(n):
        return lax.rem(d + n, 8)

    def send(which, c, n):
        return remote(sbuf.at[which, c, dep_at(n)], outs[which].at[d, c],
                      ss.at[which, c, n], rs.at[which, c, n], dep_at(n), r)

    def keep(which, c):
        return pltpu.make_async_copy(sbuf.at[which, c, d], outs[which].at[d, c], own.at[which, c])

    def ship(which, c, value):
        sbuf[which, c] = value.T.reshape(8, 64, F)
        for n in range(1, 8):
            send(which, c, n).start()
        keep(which, c).start()

    half = lax.rem(k, 2)

    def p_copy(at):
        return pltpu.make_async_copy(p_in.at[at], p_buf.at[lax.rem(at, 2)], p_sem.at[lax.rem(at, 2)])

    @pl.when(k == 0)
    def _():
        p_copy(0).start()
        p_copy(1).start()
        wlt, wrt = wl[...].T, wr[...].T
        greet([(dep_at(n), r) for n in range(1, 8)])
        for c in range(4):
            yhat, yinv = norm(at_ref[c].astype(f32), 0)
            dy = mm(wlt, lg_ref[c]) + mm(wrt, rg_ref[c])
            m1 = jnp.mean(dy, 0, keepdims=True)
            m2 = jnp.mean(dy * yhat, 0, keepdims=True)
            upt = (ua_ref if c < 2 else ub_ref)[:, c % 2].reshape(N, F).T.astype(f32)
            dt_s[c] = (yinv * (dy - m1 - yhat * m2) + upt).astype(bf16)
            ship(1, c, dt_s[c])

    p_copy(k).wait()
    xin = x_ref[...].reshape(N, F)
    q = q_ref[0]
    v = v_ref[0]
    kt = kt_ref[0]
    gt = g_ref[0]
    ot = o_ref[0]
    dt = dt_s[k]
    dg = mm(we[...], dt).astype(bf16).astype(f32)
    dot_ = (dg * gt).astype(bf16)
    dpre = (dg * ot * gt * (1.0 - gt)).astype(bf16)
    prod = dot_.astype(f32) * ot
    row = lax.broadcasted_iota(jnp.int32, (128, N), 0)
    col = lax.broadcasted_iota(jnp.int32, (N, 128), 1)
    ones = (col < 2).astype(f32).astype(bf16)
    lane = lax.broadcasted_iota(jnp.int32, (N, F), 1) // DH
    zero = jnp.zeros((), bf16)

    def back(h):
        sl = slice(DH * h, DH * h + DH)
        acc_q[sl, :] = mm(kt[sl], ds_s[h])

    def dops(h):
        grp = h // 4
        sl = slice(DH * h, DH * h + DH)
        dd = -jnp.sum(prod[sl], 0, keepdims=True)
        hi = dd.astype(bf16).astype(f32)
        lo = dd - hi
        extra = jnp.where(row == 0, hi, jnp.where(row == 1, lo, 0.0)).astype(bf16)
        return jnp.concatenate([v[:, 128 * grp:128 * grp + 128], ones], axis=1), spread(dot_[sl], h, extra)

    def wide_v(h):
        sl = slice(DH * h, DH * h + DH)
        acc_v[sl, :] = mmt(dot_[sl], p_buf[half, h])

    def tall_k(h, i):
        ext = mm(ds_s[h, i:i + 256, :], jnp.where(lane == h, q, zero))
        if h:
            acc_t[i:i + 256, :] += ext
        else:
            acc_t[i:i + 256, :] = ext

    for h in range(H):
        ops = dops(h)
        for i in range(0, N, 256):
            dp = mm(ops[0][i:i + 256], ops[1])
            ds_s[h, i:i + 256, :] = (p_buf[half, h, i:i + 256, :].astype(f32) * dp).astype(bf16)
            if h:
                tall_k(h - 1, i)
        wide_v(h)
        if h:
            back(h - 1)
    back(H - 1)
    for i in range(0, N, 256):
        tall_k(H - 1, i)
    dq = (acc_q[...].astype(bf16).astype(f32) * SCALE).astype(bf16)
    dx = (mm(wq[...], dq) + mm(wg[...], dpre)
          + mmt(wk[...], acc_t[...].astype(bf16)) + mm(wv[...], acc_v[...].astype(bf16)))
    dx = dx.astype(bf16).astype(f32)
    xt = xin.T.astype(f32)
    xh, inv = norm(xt, 0)
    m1 = jnp.mean(dx, 0, keepdims=True)
    m2 = jnp.mean(dx * xh, 0, keepdims=True)
    dln = (inv * (dx - m1 - xh * m2)).astype(bf16)
    out = (dt.astype(f32) + dln.astype(f32)).astype(bf16)
    ship(0, k, out)

    @pl.when(k < 2)
    def _():
        p_copy(k + 2).start()

    @pl.when(k == 3)
    def _():
        for which in range(2):
            for c in range(4):
                keep(which, c).wait()
                for n in range(1, 8):
                    send(which, c, n).wait_recv()
                    send(which, c, n).wait_send()


def whole(shape):
    return pl.BlockSpec(shape, lambda k: (0,) * len(shape))


def percol(shape):
    return pl.BlockSpec((1, *shape), lambda k: (k,) + (0,) * len(shape))


COLS = pl.BlockSpec((8, 1, 64, F), lambda k: (0, k, 0, 0))
ANY = pl.BlockSpec(memory_space=pl.ANY)


def fwd(msa, upstream, pair, live, wq, wk, wv, wg, we, wl, wr):
    sd = jax.ShapeDtypeStruct
    V = pltpu.VMEM
    dma = pltpu.SemaphoreType.DMA
    return pl.pallas_call(
        fwd_kernel,
        grid=(4,),
        in_specs=[whole((64, 32, F))] * 2 + [whole((32, 64, CZ)), whole((CW, 64))] + [whole((F, F))] * 5 + [whole((CW, F))] * 2,
        out_specs=[COLS, ANY, percol((F, N)), percol((F, N)), percol((F, N)), percol((CW, N)),
                   percol((CW, N)), percol((N, F)), percol((N, F)), percol((F, N)), ANY, ANY, ANY, whole((8, 256)), whole((8, N))],
        out_shape=[sd((8, 4, 64, F), bf16), sd((4, H, N, N), bf16), sd((4, F, N), f32), sd((4, F, N), f32),
                   sd((4, F, N), bf16), sd((4, CW, N), bf16), sd((4, CW, N), bf16),
                   sd((4, N, F), bf16), sd((4, N, F), bf16), sd((4, F, N), bf16), sd((8, 2, 64, F), bf16), sd((8, 2, 64, F), bf16), sd((8, 2, 4, CW, CZ), bf16), sd((8, 256), f32), sd((8, N), f32)],
        scratch_shapes=[V((4, F, F), bf16), V((N, 128), bf16), V((2, N, N), f32), V((2, H, N, N), bf16), V((64, 128), bf16), V((8, 4, 64, F), bf16), V((8, 4, 64, F), bf16), V((2, 8, 4, CW, CZ), bf16), V((4, 8, 64, F), bf16),
                        V((8, 64, 128), bf16), V((128, N), f32), V((16, 8, N), f32), V((8, N), f32),
                        dma((4, 8)), dma((4, 8)), dma((4, 8)), dma((4, 8))] + [dma((8,))] * 4 + [dma((16,))] * 2 + [dma((8,)), dma((2, 8))],
        compiler_params=pltpu.CompilerParams(vmem_limit_bytes=60 * 1024 * 1024, collective_id=2, has_side_effects=True,
                                             dimension_semantics=("arbitrary",)),
        name="attention_forward",
    )(msa, upstream, pair, live, wq, wk, wv, wg, we, wl, wr)


def bwd(x, ua, ub, at, lg, rg, p, o, g, q, v, kt, wq, wk, wv, wg, we, wl, wr):
    sd = jax.ShapeDtypeStruct
    V = pltpu.VMEM
    dma = pltpu.SemaphoreType.DMA
    return pl.pallas_call(
        bwd_kernel,
        grid=(4,),
        in_specs=[COLS, whole((8, 2, 64, F)), whole((8, 2, 64, F)), whole((4, F, N)), whole((4, CW, N)), whole((4, CW, N)), ANY, percol((F, N)),
                  percol((F, N)), percol((N, F)), percol((N, F)), percol((F, N))] + [whole((F, F))] * 5 + [whole((CW, F))] * 2,
        out_specs=[ANY, ANY],
        out_shape=[sd((8, 4, 64, F), bf16)] * 2,
        scratch_shapes=[V((2, H, N, N), bf16), V((H, N, N), bf16), V((F, N), f32), V((F, N), f32), V((N, F), f32), V((4, F, N), bf16), V((2, 4, 8, 64, F), bf16),
                        dma((2, 4, 8)), dma((2, 4, 8)), dma((2, 4)), dma((2,))],
        compiler_params=pltpu.CompilerParams(vmem_limit_bytes=60 * 1024 * 1024, collective_id=3, has_side_effects=True,
                                             dimension_semantics=("arbitrary",)),
        name="attention_backward",
    )(x, ua, ub, at, lg, rg, p, o, g, q, v, kt, wq, wk, wv, wg, we, wl, wr)


def opm_kernel(lt, rt, pd, rc, wo, live, ux, lo, ro, up,
               perm, oc1, oc2, lbuf, rbuf, lsend, lrecv, psend, precv, rsend, rrecv, both, lkeep, lacc,
               ls, lr, rs, rr, fs, fr, ps, pr, s2, r2, s3, r3, us, ur, own):
    d = lax.axis_index("dep")
    r = lax.axis_index("res")
    xl, z = d // 4, lax.rem(d, 4)
    y, xh, core = r // 4, lax.rem(r // 2, 2), lax.rem(r, 2)

    def dep_of(flip, step):
        return 4 * lax.rem(xl + flip, 2) + lax.rem(z + step + 4, 4)

    def chip_of(flip, step):
        return 2 * lax.rem(y + step + 4, 4) + lax.rem(xh + flip, 2)

    def res_of(flip, step):
        return 2 * chip_of(flip, step) + core

    partner = 2 * chip_of(0, 0) + 1 - core
    greet([(lax.rem(d + n, 8), r) for n in range(1, 8)]
          + [(d, res_of(0, n)) for n in range(1, 4)] + [(d, res_of(1, 0)), (d, partner)])

    def left_copy(n):
        if n == 0:
            return remote(lt, lbuf.at[d], ls.at[0], lr.at[0], dep_of(1, 0), r)
        if n < 4:
            return remote(lt, lbuf.at[d], ls.at[n], lr.at[n], dep_of(0, n), r)
        slot = dep_of(1, 0)
        return remote(lbuf.at[slot], lbuf.at[slot], ls.at[n], lr.at[n], dep_of(0, n - 3), r)

    def right_copy(n):
        if n == 0:
            return remote(rt, rbuf.at[r], rs.at[0], rr.at[0], d, res_of(1, 0))
        if n < 4:
            return remote(rt, rbuf.at[r], rs.at[n], rr.at[n], d, res_of(0, n))
        slot = res_of(1, 0)
        return remote(rbuf.at[slot], rbuf.at[slot], rs.at[n], rr.at[n], d, res_of(0, n - 3))

    def across(n):
        if n == 7:
            return remote(rt, rbuf.at[r], fs.at[7], fr.at[7], d, partner)
        slot = res_of(1, 0) if n == 0 else res_of(0, -n) if n < 4 else res_of(1, 3 - n)
        return remote(rbuf.at[slot], rbuf.at[slot], fs.at[n], fr.at[n], d, partner)

    def up_copy(n):
        dep = lax.rem(d + n, 8)
        return remote(ux.at[dep], up.at[d], us.at[n], ur.at[n], dep, r)

    own_up = pltpu.make_async_copy(ux.at[d], up.at[d], own)
    own_up.start()
    for n in range(4):
        left_copy(n).start()
        right_copy(n).start()
    across(7).start()
    lbuf[d] = lt[...]
    rbuf[r] = rt[...]

    a = lax.broadcasted_iota(jnp.int32, (1024, 1024), 0)
    b = lax.broadcasted_iota(jnp.int32, (1024, 1024), 1)
    hit = ((a // CW) == (b % CW)) & ((a % CW) == (b // CW))
    perm[...] = hit.astype(f32).astype(bf16)

    def outer_step(n, carry):
        at = pl.multiple_of(256 * n, 256)
        zz = (mmt(wo[...], pd[pl.ds(at, 256), :]) * rc[pl.ds(n, 1), :]).astype(bf16)
        rows = []
        for j in range(8):
            rows.append(jnp.concatenate([zz[CW * c:CW * c + CW, CW * j:CW * j + CW] for c in range(CW)], axis=1))
        yy = mm(jnp.concatenate(rows, axis=0), perm[...]).astype(bf16)
        oc1[pl.ds(at, 256), :] = yy
        oc2[:, pl.ds(at, 256)] = yy.T

        @pl.when(n == 1)
        def _():
            left_copy(0).wait_recv()
            for i in range(4, 7):
                left_copy(i).start()

        @pl.when(n == 2)
        def _():
            right_copy(0).wait_recv()
            for i in range(4, 7):
                right_copy(i).start()
            across(0).start()

        @pl.when(n == 5)
        def _():
            for i in range(1, 4):
                right_copy(i).wait_recv()
                across(i).start()
        return carry

    lax.fori_loop(0, 8, outer_step, 0)
    for n in range(1, 7):
        left_copy(n).wait_recv()
    for n in range(1, 8):
        up_copy(n).start()
    for n in range(4, 7):
        right_copy(n).wait_recv()
        across(n).start()

    order = [(1, 1), (1, 2), (1, 3), (1, 0), (0, 1), (0, 2), (0, 3), (0, 0)]

    def pass_over(i):
        return remote(psend.at[i], precv.at[i], ps.at[i], pr.at[i], d, partner)

    def right_part(i):
        target = res_of(1, 0) if i == 3 else res_of(0, order[i][1])
        return remote(rsend.at[i], rrecv.at[i], s2.at[i], r2.at[i], d, target)

    def left_part(i):
        target = dep_of(1, 0) if i == 3 else dep_of(0, order[i][1])
        return remote(lsend.at[i], lrecv.at[i], s3.at[i], r3.at[i], target, r)

    mine = pl.ds(pl.multiple_of(128 * core, 128), 128)
    theirs = pl.ds(pl.multiple_of(128 * (1 - core), 128), 128)
    lall = lbuf[...].reshape(1024, N)
    for i, (flip, step) in enumerate(order):
        at = pl.multiple_of(256 * chip_of(flip, step), 256)
        both[i] = mm(oc1[pl.ds(at, 256), :], lall)
        psend[i] = both[i, theirs, :].astype(bf16)
        pass_over(i).start()
    for i in range(8):
        pass_over(i).wait_recv()
        own = both[i, mine, :] + precv[i].astype(f32)
        if i in (3, 7):
            both[i, mine, :] = own
        else:
            rsend[i] = own.astype(bf16)
            right_part(i).start()
    for n in range(8):
        across(n).wait_recv()
    rall = rbuf[...].reshape(2048, N)
    for i, (flip, step) in enumerate(order):
        at = pl.multiple_of(128 * dep_of(flip, step), 128)
        own = mm(oc2[pl.ds(at, 128), :], rall)
        if i == 3:
            lkeep[...] = own
        elif i == 7:
            lacc[...] = own
        else:
            lsend[i] = own.astype(bf16)
            left_part(i).start()
    for i in range(3):
        right_part(i).wait_recv()
    rsend[3] = (both[3, mine, :] + jnp.sum(rrecv[0:3].astype(f32), 0)).astype(bf16)
    right_part(3).start()
    for i in range(3):
        left_part(i).wait_recv()
    lsend[3] = (lkeep[...] + jnp.sum(lrecv[0:3].astype(f32), 0)).astype(bf16)
    left_part(3).start()
    for i in range(3, 7):
        right_part(i).wait_recv()
    racc = both[7, mine, :] + jnp.sum(rrecv[3:7].astype(f32), 0)
    for n in range(4):
        ro[n] = (racc[CW * n:CW * n + CW, :] * live[n:n + 1, :]).astype(bf16)
    for i in range(3, 7):
        left_part(i).wait_recv()
    lsum = lacc[...] + jnp.sum(lrecv[3:7].astype(f32), 0)
    for n in range(4):
        lo[n] = (lsum[CW * n:CW * n + CW, :] * live[n:n + 1, :]).astype(bf16)
    own_up.wait()
    for n in range(1, 8):
        up_copy(n).wait_recv()
        up_copy(n).wait_send()
    for n in range(7):
        left_copy(n).wait_send()
        right_copy(n).wait_send()
        right_part(n).wait_send()
        left_part(n).wait_send()
    for n in range(8):
        across(n).wait_send()
        pass_over(n).wait_send()


def opm(lt, rt, pd, rc, wo, live, ux):
    sd = jax.ShapeDtypeStruct
    vm = pl.BlockSpec(memory_space=pltpu.VMEM)
    chunk = (128, N)
    V = pltpu.VMEM
    dma = pltpu.SemaphoreType.DMA((8,))
    return pl.pallas_call(
        opm_kernel,
        in_specs=[vm] * 6 + [ANY],
        out_specs=[vm] * 3,
        out_shape=[sd((4, CW, N), bf16)] * 2 + [sd((8, 2, 64, F), bf16)],
        scratch_shapes=[V((1024, 1024), bf16), V((2048, 1024), bf16), V((1024, 2048), bf16),
                        V((8, *chunk), bf16), V((16, *chunk), bf16)] + [V((8, *chunk), bf16)] * 6
        + [V((8, 256, N), f32)] + [V(chunk, f32)] * 2 + [dma] * 14 + [pltpu.SemaphoreType.DMA],
        compiler_params=pltpu.CompilerParams(vmem_limit_bytes=60 * 1024 * 1024, collective_id=1, has_side_effects=True),
        name="outer_product",
    )(lt, rt, pd, rc, wo, live, ux)


def on_device(msa, present, pair, upstream, wq, wk, wv, wg, we, wl, wr, wo):
    def by_row(a):
        return a.reshape(32, 64, F).transpose(1, 0, 2)

    x, p, o, g, at, lt, rt, q, v, kt, ua, ut, pd, recip, livet = fwd(
        msa, upstream, pair, present.T, wq, wk, wv, wg, we, wl.T, wr.T)
    lg, rg, ub = opm(lt.reshape(4 * CW, N), rt.reshape(4 * CW, N), pd.reshape(-1, CZ), recip, wo, livet, ut)
    grad, inter = bwd(x, ua, ub, at, lg, rg, p, o, g, q, v, kt, wq, wk, wv, wg, we, wl.T, wr.T)
    return by_row(grad), by_row(inter)


def solution(mesh):
    rows = P("dep", "res", None)
    in_specs = (rows, P("dep", "res"), P("res", "dep", None), rows) + (P(),) * 8
    return jax.shard_map(on_device, mesh=mesh, in_specs=in_specs, out_specs=(rows, rows), check_vma=False)
```

```python
import functools

import jax
import jax.numpy as jnp
from jax import lax
from jax.experimental import pallas as pl
from jax.experimental.pallas import tpu as pltpu
from jax.sharding import PartitionSpec as P

F = 256
H = 8
DH = 32
N = 512
CW = 32
CZ = 128
EPS = 1e-05
BIG = 1e9
f32 = jnp.float32
bf16 = jnp.bfloat16
SCALE = DH ** (-0.5)
NT = (((1,), (1,)), ((), ()))


def mm(a, b):
    return jnp.dot(a, b, preferred_element_type=f32)


def mmt(a, b):
    return lax.dot_general(a, b, NT, preferred_element_type=f32)


def norm(v, axis):
    c = v - jnp.mean(v, axis, keepdims=True)
    inv = lax.rsqrt(jnp.mean(c * c, axis, keepdims=True) + EPS)
    return c * inv, inv


def spread(rows, h, extra):
    top = (h % 4) * DH
    parts = []
    if top:
        parts.append(jnp.zeros((top, N), bf16))
    parts.append(rows)
    if top < 96:
        parts.append(jnp.zeros((96 - top, N), bf16))
    parts.append(extra)
    return jnp.concatenate(parts, axis=0)


MESH = pl.DeviceIdType.MESH


def remote(src, dst, send, recv, dep, res):
    return pltpu.make_async_remote_copy(src_ref=src, dst_ref=dst, send_sem=send, recv_sem=recv,
                                        device_id={"dep": dep, "res": res}, device_id_type=MESH)


def hail(peers):
    bar = pltpu.get_barrier_semaphore()
    for dep, res in peers:
        pl.semaphore_signal(bar, inc=1, device_id={"dep": dep, "res": res}, device_id_type=MESH)


def gather_all(count):
    pl.semaphore_wait(pltpu.get_barrier_semaphore(), count)


def greet(peers):
    hail(peers)
    gather_all(len(peers))


def fwd_kernel(x_in, u_in, pair_in, present, wq, wk, wv, wg, we, wl, wr,
               x_ref, p_out, o_ref, g_ref, a_ref, l_ref, r_ref, q_ref, v_ref, kt_ref, up_out, ut_out, pd_out, rc_ref, live_out,
               wt, bias_s, st_s, p_buf, live_in, hx, ux, px, xbuf, lbuf, livet, jbuf, mine,
               xs, xr, us, ur, ps, pr, ls, lr, js, jr, own, p_sem):
    k = pl.program_id(0)
    d = lax.axis_index("dep")
    r = lax.axis_index("res")

    def dep_at(n):
        return lax.rem(d + n, 8)

    def res_at(n):
        return lax.rem(r + n, 16)

    def x_copy(c, n):
        return remote(hx.at[dep_at(n), c], xbuf.at[c, d], xs.at[c, n], xr.at[c, n], dep_at(n), r)

    def up_copy(c, n):
        return remote(ux.at[dep_at(n), c], up_out.at[d, c], us.at[c, n], ur.at[c, n], dep_at(n), r)

    def pd_copy(n):
        return remote(px.at[:, dep_at(n)], pd_out.at[d], ps.at[n], pr.at[n], dep_at(n), r)

    def live_copy(n):
        return remote(live_in, lbuf.at[d], ls.at[n], lr.at[n], dep_at(n), r)

    def row_copy(n):
        return remote(mine, jbuf.at[r], js.at[n], jr.at[n], d, res_at(n))

    own_up = pltpu.make_async_copy(ux.at[d, pl.ds(0, 2)], up_out.at[d], own.at[0])
    own_pd = pltpu.make_async_copy(px.at[:, d], pd_out.at[d], own.at[1])
    later_up = pltpu.make_async_copy(ux.at[:, pl.ds(2, 2)], ut_out, own.at[2])

    half = lax.rem(k, 2)

    def p_copy(at, h):
        return pltpu.make_async_copy(p_buf.at[lax.rem(at, 2), h], p_out.at[at, h], p_sem.at[lax.rem(at, 2), h])

    @pl.when(k > 1)
    def _():
        for h in range(H):
            p_copy(k - 2, h).wait()

    @pl.when(k == 0)
    def _():
        hail([(dep_at(n), r) for n in range(1, 8)] + [(d, res_at(n)) for n in range(1, 16)])
        hx[...] = jnp.transpose(x_in[...], (1, 0, 2)).reshape(hx.shape)
        flat = jnp.concatenate([present[...].astype(f32), jnp.zeros((CW, 64), f32)], axis=1)
        held = jnp.concatenate([flat, jnp.zeros((96, 128), f32)], axis=0).T[:64].astype(bf16)
        live_in[...] = held
        lbuf[d] = held
        gather_all(22)
        for n in range(1, 8):
            live_copy(n).start()
        for n in range(1, 8):
            x_copy(0, n).start()
        for c in range(4):
            xbuf[c, d] = hx[d, c]
        for n, w in enumerate((wq, wv, wg, we)):
            wt[n] = w[...].T
        px[...] = jnp.transpose(pair_in[...], (1, 0, 2)).reshape(px.shape)
        ux[...] = jnp.transpose(u_in[...], (1, 0, 2)).reshape(ux.shape)
        for n in range(1, 8):
            live_copy(n).wait_recv()
        live = lbuf[...].reshape(N, 128).astype(f32)
        bias_s[...] = ((live - 1.0) * BIG).astype(bf16)
        livet[...] = live.T
        rows = [livet[pl.ds(4 * d + n, 1), :] for n in range(4)]
        held = jnp.concatenate(rows + [jnp.zeros((4, N), f32)], axis=0)
        mine[...] = held
        live_out[...] = held
        jbuf[r] = held
        for n in range(1, 8):
            x_copy(0, n).wait_send()
        for n in range(1, 8):
            x_copy(1, n).start()

    @pl.when(k == 1)
    def _():
        for n in range(1, 16):
            row_copy(n).start()
        for n in range(1, 8):
            pd_copy(n).start()
        own_up.start()
        own_pd.start()
        later_up.start()

    @pl.when(k == 2)
    def _():
        for n in range(1, 8):
            up_copy(1, n).start()

    @pl.when(k == 3)
    def _():
        for n in range(1, 16):
            row_copy(n).wait_recv()
        counts = mm(jbuf[...].reshape(128, N).astype(bf16), lbuf[...].reshape(N, 128))
        rec = 1.0 / (0.001 + counts)
        for n in range(8):
            pieces = []
            for j in range(8):
                at = 16 * n + 8 * (j // 4) + j % 4
                pieces.append(rec[at:at + 1, :CW])
            rc_ref[n:n + 1, :] = jnp.concatenate(pieces, axis=1)

    for n in range(1, 8):
        x_copy(k, n).wait_recv()
    xin = xbuf[k].reshape(N, F)
    x_ref[...] = xin.reshape(x_ref.shape)
    xhat, _ = norm(xin.astype(f32), 1)
    xb = xhat.astype(bf16)
    xbt = xb.T
    qt = (mm(wt[0], xbt) * SCALE).astype(bf16)
    vt = mm(wt[1], xbt).astype(bf16)
    kk = mm(xb, wk[...]).astype(bf16)
    gt = jax.nn.sigmoid(mm(wt[2], xbt))
    q_ref[0] = qt.T
    v_ref[0] = vt.T
    kt_ref[0] = kk.T
    g_ref[0] = gt
    extra = (lax.broadcasted_iota(jnp.int32, (128, N), 0) == 4 * d + k).astype(f32).astype(bf16)
    bias = bias_s[...]
    PIECE = 128

    def operands(h):
        grp = h // 4
        return jnp.concatenate([kk[:, 128 * grp:128 * grp + 128], bias], axis=1), spread(qt[DH * h:DH * h + DH], h, extra)

    def score(ops, h, i):
        val = mm(ops[0][i:i + PIECE], ops[1])
        st_s[h % 2, i:i + PIECE, :] = val
        return jnp.max(val, 0, keepdims=True)

    def blend(h):
        o_ref[0, DH * h:DH * h + DH, :] = mm(vt[DH * h:DH * h + DH], p_buf[half, h])

    ops = operands(0)
    peak = functools.reduce(jnp.maximum, [score(ops, 0, i) for i in range(0, N, PIECE)])
    def push_x(at, c):
        @pl.when(k == at)
        def _():
            for n in range(1, 8):
                x_copy(c, n).start()

    def push_up(at, c):
        @pl.when(k == at)
        def _():
            for n in range(1, 8):
                up_copy(c, n).start()

    for h in range(H):
        if h == 2:
            push_x(0, 2)
        if h == 4:
            push_up(1, 0)
        if h == 5:
            push_x(0, 3)
        b = h % 2
        if h + 1 < H:
            ops = operands(h + 1)
        nxt = []
        tot = jnp.zeros((1, N), f32)
        for i in range(0, N, PIECE):
            if h + 1 < H:
                nxt.append(score(ops, h + 1, i))
            e = jnp.exp(st_s[b, i:i + PIECE, :] - peak)
            st_s[b, i:i + PIECE, :] = e
            tot = tot + jnp.sum(e, 0, keepdims=True)
        if h:
            blend(h - 1)
        inv = 1.0 / tot
        for i in range(0, N, PIECE):
            p_buf[half, h, i:i + PIECE, :] = (st_s[b, i:i + PIECE, :] * inv).astype(bf16)
        p_copy(k, h).start()
        if nxt:
            peak = functools.reduce(jnp.maximum, nxt)
    blend(H - 1)
    gated = (gt * o_ref[0]).astype(bf16)
    up = mm(wt[3], gated)
    after = (xin.T.astype(f32) + up).astype(bf16)
    a_ref[0] = after
    yhat, _ = norm(after.astype(f32), 0)
    yb = yhat.astype(bf16)
    live = livet[pl.ds(4 * d + k, 1), :]
    l_ref[0] = (mm(wl[...], yb) * live).astype(bf16)
    r_ref[0] = (mm(wr[...], yb) * live).astype(bf16)

    @pl.when(k == 3)
    def _():
        for n in range(1, 8):
            pd_copy(n).wait_recv()
            for c in range(2):
                up_copy(c, n).wait_recv()
        own_up.wait()
        own_pd.wait()
        later_up.wait()
        for h in range(H):
            p_copy(2, h).wait()
            p_copy(3, h).wait()
        for n in range(1, 8):
            live_copy(n).wait_send()
            pd_copy(n).wait_send()
            for c in range(2):
                up_copy(c, n).wait_send()
            for c in range(1, 4):
                x_copy(c, n).wait_send()
        for n in range(1, 16):
            row_copy(n).wait_send()


def bwd_kernel(x_ref, ua_ref, ub_ref, at_ref, lg_ref, rg_ref, p_in, o_ref, g_ref, q_ref, v_ref, kt_ref, wq, wk, wv, wg, we, wl, wr,
               out_g, out_i, p_buf, ds_s, acc_q, acc_v, acc_t, dt_s, sbuf, ss, rs, own, p_sem):
    k = pl.program_id(0)
    d = lax.axis_index("dep")
    r = lax.axis_index("res")
    outs = (out_g, out_i)

    def dep_at(n):
        return lax.rem(d + n, 8)

    def send(which, c, n):
        return remote(sbuf.at[which, c, dep_at(n)], outs[which].at[d, c],
                      ss.at[which, c, n], rs.at[which, c, n], dep_at(n), r)

    def keep(which, c):
        return pltpu.make_async_copy(sbuf.at[which, c, d], outs[which].at[d, c], own.at[which, c])

    def ship(which, c, value):
        sbuf[which, c] = value.T.reshape(8, 64, F)
        for n in range(1, 8):
            send(which, c, n).start()
        keep(which, c).start()

    half = lax.rem(k, 2)

    def p_copy(at):
        return pltpu.make_async_copy(p_in.at[at], p_buf.at[lax.rem(at, 2)], p_sem.at[lax.rem(at, 2)])

    @pl.when(k == 0)
    def _():
        p_copy(0).start()
        p_copy(1).start()
        hail([(dep_at(n), r) for n in range(1, 8)])
        wlt, wrt = wl[...].T, wr[...].T
        gather_all(7)
        for c in range(4):
            yhat, yinv = norm(at_ref[c].astype(f32), 0)
            dy = mm(wlt, lg_ref[c]) + mm(wrt, rg_ref[c])
            m1 = jnp.mean(dy, 0, keepdims=True)
            m2 = jnp.mean(dy * yhat, 0, keepdims=True)
            upt = (ua_ref if c < 2 else ub_ref)[:, c % 2].reshape(N, F).T.astype(f32)
            dt_s[c] = (yinv * (dy - m1 - yhat * m2) + upt).astype(bf16)
            ship(1, c, dt_s[c])

    p_copy(k).wait()
    xin = x_ref[...].reshape(N, F)
    q = q_ref[0]
    v = v_ref[0]
    kt = kt_ref[0]
    gt = g_ref[0]
    ot = o_ref[0]
    dt = dt_s[k]
    dg = mm(we[...], dt).astype(bf16).astype(f32)
    dot_ = (dg * gt).astype(bf16)
    dpre = (dg * ot * gt * (1.0 - gt)).astype(bf16)
    prod = dot_.astype(f32) * ot
    row = lax.broadcasted_iota(jnp.int32, (128, N), 0)
    col = lax.broadcasted_iota(jnp.int32, (N, 128), 1)
    ones = (col < 2).astype(f32).astype(bf16)
    lane = lax.broadcasted_iota(jnp.int32, (N, F), 1) // DH
    zero = jnp.zeros((), bf16)

    def back(h):
        sl = slice(DH * h, DH * h + DH)
        acc_q[sl, :] = mm(kt[sl], ds_s[h])

    def dops(h):
        grp = h // 4
        sl = slice(DH * h, DH * h + DH)
        dd = -jnp.sum(prod[sl], 0, keepdims=True)
        hi = dd.astype(bf16).astype(f32)
        lo = dd - hi
        extra = jnp.where(row == 0, hi, jnp.where(row == 1, lo, 0.0)).astype(bf16)
        return jnp.concatenate([v[:, 128 * grp:128 * grp + 128], ones], axis=1), spread(dot_[sl], h, extra)

    def wide_v(h):
        sl = slice(DH * h, DH * h + DH)
        acc_v[sl, :] = mmt(dot_[sl], p_buf[half, h])

    def tall_k(h, i):
        ext = mm(ds_s[h, i:i + 256, :], jnp.where(lane == h, q, zero))
        if h:
            acc_t[i:i + 256, :] += ext
        else:
            acc_t[i:i + 256, :] = ext

    for h in range(H):
        ops = dops(h)
        for i in range(0, N, 256):
            dp = mm(ops[0][i:i + 256], ops[1])
            ds_s[h, i:i + 256, :] = (p_buf[half, h, i:i + 256, :].astype(f32) * dp).astype(bf16)
            if h:
                tall_k(h - 1, i)
        wide_v(h)
        if h:
            back(h - 1)
    back(H - 1)
    for i in range(0, N, 256):
        tall_k(H - 1, i)
    dq = (acc_q[...].astype(bf16).astype(f32) * SCALE).astype(bf16)
    dx = (mm(wq[...], dq) + mm(wg[...], dpre)
          + mmt(wk[...], acc_t[...].astype(bf16)) + mm(wv[...], acc_v[...].astype(bf16)))
    dx = dx.astype(bf16).astype(f32)
    xt = xin.T.astype(f32)
    xh, inv = norm(xt, 0)
    m1 = jnp.mean(dx, 0, keepdims=True)
    m2 = jnp.mean(dx * xh, 0, keepdims=True)
    dln = (inv * (dx - m1 - xh * m2)).astype(bf16)
    out = (dt.astype(f32) + dln.astype(f32)).astype(bf16)
    ship(0, k, out)

    @pl.when(k < 2)
    def _():
        p_copy(k + 2).start()

    @pl.when(k == 3)
    def _():
        for which in range(2):
            for c in range(4):
                keep(which, c).wait()
                for n in range(1, 8):
                    send(which, c, n).wait_recv()
                    send(which, c, n).wait_send()


def whole(shape):
    return pl.BlockSpec(shape, lambda k: (0,) * len(shape))


def percol(shape):
    return pl.BlockSpec((1, *shape), lambda k: (k,) + (0,) * len(shape))


COLS = pl.BlockSpec((8, 1, 64, F), lambda k: (0, k, 0, 0))
ANY = pl.BlockSpec(memory_space=pl.ANY)


def fwd(msa, upstream, pair, live, wq, wk, wv, wg, we, wl, wr):
    sd = jax.ShapeDtypeStruct
    V = pltpu.VMEM
    dma = pltpu.SemaphoreType.DMA
    return pl.pallas_call(
        fwd_kernel,
        grid=(4,),
        in_specs=[whole((64, 32, F))] * 2 + [whole((32, 64, CZ)), whole((CW, 64))] + [whole((F, F))] * 5 + [whole((CW, F))] * 2,
        out_specs=[COLS, ANY, percol((F, N)), percol((F, N)), percol((F, N)), percol((CW, N)),
                   percol((CW, N)), percol((N, F)), percol((N, F)), percol((F, N)), ANY, ANY, ANY, whole((8, 256)), whole((8, N))],
        out_shape=[sd((8, 4, 64, F), bf16), sd((4, H, N, N), bf16), sd((4, F, N), f32), sd((4, F, N), f32),
                   sd((4, F, N), bf16), sd((4, CW, N), bf16), sd((4, CW, N), bf16),
                   sd((4, N, F), bf16), sd((4, N, F), bf16), sd((4, F, N), bf16), sd((8, 2, 64, F), bf16), sd((8, 2, 64, F), bf16), sd((8, 2, 4, CW, CZ), bf16), sd((8, 256), f32), sd((8, N), f32)],
        scratch_shapes=[V((4, F, F), bf16), V((N, 128), bf16), V((2, N, N), f32), V((2, H, N, N), bf16), V((64, 128), bf16), V((8, 4, 64, F), bf16), V((8, 4, 64, F), bf16), V((2, 8, 4, CW, CZ), bf16), V((4, 8, 64, F), bf16),
                        V((8, 64, 128), bf16), V((128, N), f32), V((16, 8, N), f32), V((8, N), f32),
                        dma((4, 8)), dma((4, 8)), dma((4, 8)), dma((4, 8))] + [dma((8,))] * 4 + [dma((16,))] * 2 + [dma((8,)), dma((2, 8))],
        compiler_params=pltpu.CompilerParams(vmem_limit_bytes=60 * 1024 * 1024, collective_id=2, has_side_effects=True,
                                             dimension_semantics=("arbitrary",)),
        name="attention_forward",
    )(msa, upstream, pair, live, wq, wk, wv, wg, we, wl, wr)


def bwd(x, ua, ub, at, lg, rg, p, o, g, q, v, kt, wq, wk, wv, wg, we, wl, wr):
    sd = jax.ShapeDtypeStruct
    V = pltpu.VMEM
    dma = pltpu.SemaphoreType.DMA
    return pl.pallas_call(
        bwd_kernel,
        grid=(4,),
        in_specs=[COLS, whole((8, 2, 64, F)), whole((8, 2, 64, F)), whole((4, F, N)), whole((4, CW, N)), whole((4, CW, N)), ANY, percol((F, N)),
                  percol((F, N)), percol((N, F)), percol((N, F)), percol((F, N))] + [whole((F, F))] * 5 + [whole((CW, F))] * 2,
        out_specs=[ANY, ANY],
        out_shape=[sd((8, 4, 64, F), bf16)] * 2,
        scratch_shapes=[V((2, H, N, N), bf16), V((H, N, N), bf16), V((F, N), f32), V((F, N), f32), V((N, F), f32), V((4, F, N), bf16), V((2, 4, 8, 64, F), bf16),
                        dma((2, 4, 8)), dma((2, 4, 8)), dma((2, 4)), dma((2,))],
        compiler_params=pltpu.CompilerParams(vmem_limit_bytes=60 * 1024 * 1024, collective_id=3, has_side_effects=True,
                                             dimension_semantics=("arbitrary",)),
        name="attention_backward",
    )(x, ua, ub, at, lg, rg, p, o, g, q, v, kt, wq, wk, wv, wg, we, wl, wr)


def opm_kernel(lt, rt, pd, rc, wo, live, ux, lo, ro, up,
               perm, oc1, oc2, lbuf, rbuf, lsend, lrecv, psend, precv, rsend, rrecv, both, lkeep, lacc,
               ls, lr, rs, rr, fs, fr, ps, pr, s2, r2, s3, r3, us, ur, own):
    d = lax.axis_index("dep")
    r = lax.axis_index("res")
    xl, z = d // 4, lax.rem(d, 4)
    y, xh, core = r // 4, lax.rem(r // 2, 2), lax.rem(r, 2)

    def dep_of(flip, step):
        return 4 * lax.rem(xl + flip, 2) + lax.rem(z + step + 4, 4)

    def chip_of(flip, step):
        return 2 * lax.rem(y + step + 4, 4) + lax.rem(xh + flip, 2)

    def res_of(flip, step):
        return 2 * chip_of(flip, step) + core

    partner = 2 * chip_of(0, 0) + 1 - core
    greet([(lax.rem(d + n, 8), r) for n in range(1, 8)]
          + [(d, res_of(0, n)) for n in range(1, 4)] + [(d, res_of(1, 0)), (d, partner)])

    def left_copy(n):
        if n == 0:
            return remote(lt, lbuf.at[d], ls.at[0], lr.at[0], dep_of(1, 0), r)
        if n < 4:
            return remote(lt, lbuf.at[d], ls.at[n], lr.at[n], dep_of(0, n), r)
        slot = dep_of(1, 0)
        return remote(lbuf.at[slot], lbuf.at[slot], ls.at[n], lr.at[n], dep_of(0, n - 3), r)

    def right_copy(n):
        if n == 0:
            return remote(rt, rbuf.at[r], rs.at[0], rr.at[0], d, res_of(1, 0))
        if n < 4:
            return remote(rt, rbuf.at[r], rs.at[n], rr.at[n], d, res_of(0, n))
        slot = res_of(1, 0)
        return remote(rbuf.at[slot], rbuf.at[slot], rs.at[n], rr.at[n], d, res_of(0, n - 3))

    def across(n):
        if n == 7:
            return remote(rt, rbuf.at[r], fs.at[7], fr.at[7], d, partner)
        slot = res_of(1, 0) if n == 0 else res_of(0, -n) if n < 4 else res_of(1, 3 - n)
        return remote(rbuf.at[slot], rbuf.at[slot], fs.at[n], fr.at[n], d, partner)

    def up_copy(n):
        dep = lax.rem(d + n, 8)
        return remote(ux.at[dep], up.at[d], us.at[n], ur.at[n], dep, r)

    own_up = pltpu.make_async_copy(ux.at[d], up.at[d], own)
    own_up.start()
    for n in range(4):
        left_copy(n).start()
        right_copy(n).start()
    across(7).start()
    lbuf[d] = lt[...]
    rbuf[r] = rt[...]

    a = lax.broadcasted_iota(jnp.int32, (1024, 1024), 0)
    b = lax.broadcasted_iota(jnp.int32, (1024, 1024), 1)
    hit = ((a // CW) == (b % CW)) & ((a % CW) == (b // CW))
    perm[...] = hit.astype(f32).astype(bf16)

    def outer_step(n, carry):
        at = pl.multiple_of(256 * n, 256)
        zz = (mmt(wo[...], pd[pl.ds(at, 256), :]) * rc[pl.ds(n, 1), :]).astype(bf16)
        rows = []
        for j in range(8):
            rows.append(jnp.concatenate([zz[CW * c:CW * c + CW, CW * j:CW * j + CW] for c in range(CW)], axis=1))
        yy = mm(jnp.concatenate(rows, axis=0), perm[...]).astype(bf16)
        oc1[pl.ds(at, 256), :] = yy
        oc2[:, pl.ds(at, 256)] = yy.T

        @pl.when(n == 1)
        def _():
            left_copy(0).wait_recv()
            for i in range(4, 7):
                left_copy(i).start()

        @pl.when(n == 2)
        def _():
            right_copy(0).wait_recv()
            for i in range(4, 7):
                right_copy(i).start()
            across(0).start()

        @pl.when(n == 5)
        def _():
            for i in range(1, 4):
                right_copy(i).wait_recv()
                across(i).start()
        return carry

    lax.fori_loop(0, 8, outer_step, 0)
    for n in range(1, 7):
        left_copy(n).wait_recv()
    for n in range(1, 8):
        up_copy(n).start()
    for n in range(4, 7):
        right_copy(n).wait_recv()
        across(n).start()

    order = [(1, 1), (1, 2), (1, 3), (1, 0), (0, 1), (0, 2), (0, 3), (0, 0)]

    def pass_over(i):
        return remote(psend.at[i], precv.at[i], ps.at[i], pr.at[i], d, partner)

    def right_part(i):
        target = res_of(1, 0) if i == 3 else res_of(0, order[i][1])
        return remote(rsend.at[i], rrecv.at[i], s2.at[i], r2.at[i], d, target)

    def left_part(i):
        target = dep_of(1, 0) if i == 3 else dep_of(0, order[i][1])
        return remote(lsend.at[i], lrecv.at[i], s3.at[i], r3.at[i], target, r)

    mine = pl.ds(pl.multiple_of(128 * core, 128), 128)
    theirs = pl.ds(pl.multiple_of(128 * (1 - core), 128), 128)
    def right_mm(i):
        at = pl.multiple_of(256 * chip_of(*order[i]), 256)
        both[i] = mm(oc1[pl.ds(at, 256), :], lbuf[...].reshape(1024, N))
        psend[i] = both[i, theirs, :].astype(bf16)
        pass_over(i).start()

    def right_send(i):
        pass_over(i).wait_recv()
        own = both[i, mine, :] + precv[i].astype(f32)
        if i in (3, 7):
            both[i, mine, :] = own
        else:
            rsend[i] = own.astype(bf16)
            right_part(i).start()

    def left_mm(i):
        at = pl.multiple_of(128 * dep_of(*order[i]), 128)
        own = mm(oc2[pl.ds(at, 128), :], rbuf[...].reshape(2048, N))
        if i == 3:
            lkeep[...] = own
        elif i == 7:
            lacc[...] = own
        else:
            lsend[i] = own.astype(bf16)
            left_part(i).start()

    for grp in (range(4), range(4, 8)):
        for i in grp:
            right_mm(i)
        if grp[0] == 0:
            for n in range(8):
                across(n).wait_recv()
        for i in grp:
            left_mm(i)
        for i in grp:
            right_send(i)
    for i in range(3):
        right_part(i).wait_recv()
    rsend[3] = (both[3, mine, :] + jnp.sum(rrecv[0:3].astype(f32), 0)).astype(bf16)
    right_part(3).start()
    for i in range(3):
        left_part(i).wait_recv()
    lsend[3] = (lkeep[...] + jnp.sum(lrecv[0:3].astype(f32), 0)).astype(bf16)
    left_part(3).start()
    for i in range(3, 7):
        right_part(i).wait_recv()
    racc = both[7, mine, :] + jnp.sum(rrecv[3:7].astype(f32), 0)
    for n in range(4):
        ro[n] = (racc[CW * n:CW * n + CW, :] * live[n:n + 1, :]).astype(bf16)
    for i in range(3, 7):
        left_part(i).wait_recv()
    lsum = lacc[...] + jnp.sum(lrecv[3:7].astype(f32), 0)
    for n in range(4):
        lo[n] = (lsum[CW * n:CW * n + CW, :] * live[n:n + 1, :]).astype(bf16)
    own_up.wait()
    for n in range(1, 8):
        up_copy(n).wait_recv()
        up_copy(n).wait_send()
    for n in range(7):
        left_copy(n).wait_send()
        right_copy(n).wait_send()
        right_part(n).wait_send()
        left_part(n).wait_send()
    for n in range(8):
        across(n).wait_send()
        pass_over(n).wait_send()


def opm(lt, rt, pd, rc, wo, live, ux):
    sd = jax.ShapeDtypeStruct
    vm = pl.BlockSpec(memory_space=pltpu.VMEM)
    chunk = (128, N)
    V = pltpu.VMEM
    dma = pltpu.SemaphoreType.DMA((8,))
    return pl.pallas_call(
        opm_kernel,
        in_specs=[vm] * 6 + [ANY],
        out_specs=[vm] * 3,
        out_shape=[sd((4, CW, N), bf16)] * 2 + [sd((8, 2, 64, F), bf16)],
        scratch_shapes=[V((1024, 1024), bf16), V((2048, 1024), bf16), V((1024, 2048), bf16),
                        V((8, *chunk), bf16), V((16, *chunk), bf16)] + [V((8, *chunk), bf16)] * 6
        + [V((8, 256, N), f32)] + [V(chunk, f32)] * 2 + [dma] * 14 + [pltpu.SemaphoreType.DMA],
        compiler_params=pltpu.CompilerParams(vmem_limit_bytes=60 * 1024 * 1024, collective_id=1, has_side_effects=True),
        name="outer_product",
    )(lt, rt, pd, rc, wo, live, ux)


def on_device(msa, present, pair, upstream, wq, wk, wv, wg, we, wl, wr, wo):
    def by_row(a):
        return a.reshape(32, 64, F).transpose(1, 0, 2)

    x, p, o, g, at, lt, rt, q, v, kt, ua, ut, pd, recip, livet = fwd(
        msa, upstream, pair, present.T, wq, wk, wv, wg, we, wl.T, wr.T)
    lg, rg, ub = opm(lt.reshape(4 * CW, N), rt.reshape(4 * CW, N), pd.reshape(-1, CZ), recip, wo, livet, ut)
    grad, inter = bwd(x, ua, ub, at, lg, rg, p, o, g, q, v, kt, wq, wk, wv, wg, we, wl.T, wr.T)
    return by_row(grad), by_row(inter)


def solution(mesh):
    rows = P("dep", "res", None)
    in_specs = (rows, P("dep", "res"), P("res", "dep", None), rows) + (P(),) * 8
    return jax.shard_map(on_device, mesh=mesh, in_specs=in_specs, out_specs=(rows, rows), check_vma=False)
```

```python
import functools

import jax
import jax.numpy as jnp
from jax import lax
from jax.experimental import pallas as pl
from jax.experimental.pallas import tpu as pltpu
from jax.sharding import PartitionSpec as P

F = 256
H = 8
DH = 32
N = 512
CW = 32
CZ = 128
EPS = 1e-05
BIG = 1e9
f32 = jnp.float32
bf16 = jnp.bfloat16
SCALE = DH ** (-0.5)
NT = (((1,), (1,)), ((), ()))


def mm(a, b):
    return jnp.dot(a, b, preferred_element_type=f32)


def mmt(a, b):
    return lax.dot_general(a, b, NT, preferred_element_type=f32)


def norm(v, axis):
    c = v - jnp.mean(v, axis, keepdims=True)
    inv = lax.rsqrt(jnp.mean(c * c, axis, keepdims=True) + EPS)
    return c * inv, inv


def spread(rows, h, extra):
    top = (h % 4) * DH
    parts = []
    if top:
        parts.append(jnp.zeros((top, N), bf16))
    parts.append(rows)
    if top < 96:
        parts.append(jnp.zeros((96 - top, N), bf16))
    parts.append(extra)
    return jnp.concatenate(parts, axis=0)


MESH = pl.DeviceIdType.MESH


def remote(src, dst, send, recv, dep, res):
    return pltpu.make_async_remote_copy(src_ref=src, dst_ref=dst, send_sem=send, recv_sem=recv,
                                        device_id={"dep": dep, "res": res}, device_id_type=MESH)


def hail(peers):
    bar = pltpu.get_barrier_semaphore()
    for dep, res in peers:
        pl.semaphore_signal(bar, inc=1, device_id={"dep": dep, "res": res}, device_id_type=MESH)


def gather_all(count):
    pl.semaphore_wait(pltpu.get_barrier_semaphore(), count)


def greet(peers):
    hail(peers)
    gather_all(len(peers))


def fwd_kernel(x_in, u_in, pair_in, present, wq, wk, wv, wg, we, wl, wr,
               x_ref, p_out, o_ref, g_ref, a_ref, l_ref, r_ref, q_ref, v_ref, kt_ref, up_out, ut_out, pd_out, rc_ref, live_out,
               wt, bias_s, st_s, p_buf, live_in, u_buf, pair_buf, hx, ux, px, xbuf, lbuf, livet, jbuf, mine,
               xs, xr, us, ur, ps, pr, ls, lr, js, jr, own, p_sem):
    k = pl.program_id(0)
    d = lax.axis_index("dep")
    r = lax.axis_index("res")

    def dep_at(n):
        return lax.rem(d + n, 8)

    def res_at(n):
        return lax.rem(r + n, 16)

    def x_copy(c, n):
        return remote(hx.at[dep_at(n), c], xbuf.at[c, d], xs.at[c, n], xr.at[c, n], dep_at(n), r)

    def up_copy(c, n):
        return remote(ux.at[dep_at(n), c], up_out.at[d, c], us.at[c, n], ur.at[c, n], dep_at(n), r)

    def pd_copy(n):
        return remote(px.at[:, dep_at(n)], pd_out.at[d], ps.at[n], pr.at[n], dep_at(n), r)

    def live_copy(n):
        return remote(live_in, lbuf.at[d], ls.at[n], lr.at[n], dep_at(n), r)

    def row_copy(n):
        return remote(mine, jbuf.at[r], js.at[n], jr.at[n], d, res_at(n))

    own_up = pltpu.make_async_copy(ux.at[d, pl.ds(0, 2)], up_out.at[d], own.at[0])
    own_pd = pltpu.make_async_copy(px.at[:, d], pd_out.at[d], own.at[1])
    load_up = pltpu.make_async_copy(u_in, u_buf, own.at[3])
    load_pd = pltpu.make_async_copy(pair_in, pair_buf, own.at[4])
    later_up = pltpu.make_async_copy(ux.at[:, pl.ds(2, 2)], ut_out, own.at[2])

    half = lax.rem(k, 2)

    def p_copy(at, h):
        return pltpu.make_async_copy(p_buf.at[lax.rem(at, 2), h], p_out.at[at, h], p_sem.at[lax.rem(at, 2), h])

    @pl.when(k > 1)
    def _():
        for h in range(H):
            p_copy(k - 2, h).wait()

    @pl.when(k == 0)
    def _():
        hail([(dep_at(n), r) for n in range(1, 8)] + [(d, res_at(n)) for n in range(1, 16)])
        load_pd.start()
        load_up.start()
        hx[...] = jnp.transpose(x_in[...], (1, 0, 2)).reshape(hx.shape)
        flat = jnp.concatenate([present[...].astype(f32), jnp.zeros((CW, 64), f32)], axis=1)
        held = jnp.concatenate([flat, jnp.zeros((96, 128), f32)], axis=0).T[:64].astype(bf16)
        live_in[...] = held
        lbuf[d] = held
        gather_all(22)
        for n in range(1, 8):
            live_copy(n).start()
        for n in range(1, 8):
            x_copy(0, n).start()
        for c in range(4):
            xbuf[c, d] = hx[d, c]
        for n, w in enumerate((wq, wv, wg, we)):
            wt[n] = w[...].T
        load_pd.wait()
        px[...] = jnp.transpose(pair_buf[...], (1, 0, 2)).reshape(px.shape)
        load_up.wait()
        ux[...] = jnp.transpose(u_buf[...], (1, 0, 2)).reshape(ux.shape)
        for n in range(1, 8):
            live_copy(n).wait_recv()
        live = lbuf[...].reshape(N, 128).astype(f32)
        bias_s[...] = ((live - 1.0) * BIG).astype(bf16)
        livet[...] = live.T
        rows = [livet[pl.ds(4 * d + n, 1), :] for n in range(4)]
        held = jnp.concatenate(rows + [jnp.zeros((4, N), f32)], axis=0)
        mine[...] = held
        live_out[...] = held
        jbuf[r] = held
        for n in range(1, 8):
            x_copy(0, n).wait_send()
        for n in range(1, 8):
            x_copy(1, n).start()

    @pl.when(k == 1)
    def _():
        for n in range(1, 16):
            row_copy(n).start()
        for n in range(1, 8):
            pd_copy(n).start()
        own_up.start()
        own_pd.start()
        later_up.start()

    @pl.when(k == 2)
    def _():
        for n in range(1, 8):
            up_copy(1, n).start()

    @pl.when(k == 3)
    def _():
        for n in range(1, 16):
            row_copy(n).wait_recv()
        counts = mm(jbuf[...].reshape(128, N).astype(bf16), lbuf[...].reshape(N, 128))
        rec = 1.0 / (0.001 + counts)
        for n in range(8):
            pieces = []
            for j in range(8):
                at = 16 * n + 8 * (j // 4) + j % 4
                pieces.append(rec[at:at + 1, :CW])
            rc_ref[n:n + 1, :] = jnp.concatenate(pieces, axis=1)

    for n in range(1, 8):
        x_copy(k, n).wait_recv()
    xin = xbuf[k].reshape(N, F)
    x_ref[...] = xin.reshape(x_ref.shape)
    xhat, _ = norm(xin.astype(f32), 1)
    xb = xhat.astype(bf16)
    xbt = xb.T
    qt = (mm(wt[0], xbt) * SCALE).astype(bf16)
    vt = mm(wt[1], xbt).astype(bf16)
    kk = mm(xb, wk[...]).astype(bf16)
    gt = jax.nn.sigmoid(mm(wt[2], xbt))
    q_ref[0] = qt.T
    v_ref[0] = vt.T
    kt_ref[0] = kk.T
    g_ref[0] = gt
    extra = (lax.broadcasted_iota(jnp.int32, (128, N), 0) == 4 * d + k).astype(f32).astype(bf16)
    bias = bias_s[...]
    PIECE = 128

    def operands(h):
        grp = h // 4
        return jnp.concatenate([kk[:, 128 * grp:128 * grp + 128], bias], axis=1), spread(qt[DH * h:DH * h + DH], h, extra)

    def score(ops, h, i):
        val = mm(ops[0][i:i + PIECE], ops[1])
        st_s[h % 2, i:i + PIECE, :] = val
        return jnp.max(val, 0, keepdims=True)

    def blend(h):
        o_ref[0, DH * h:DH * h + DH, :] = mm(vt[DH * h:DH * h + DH], p_buf[half, h])

    ops = operands(0)
    peak = functools.reduce(jnp.maximum, [score(ops, 0, i) for i in range(0, N, PIECE)])
    def push_x(at, c):
        @pl.when(k == at)
        def _():
            for n in range(1, 8):
                x_copy(c, n).start()

    def push_up(at, c):
        @pl.when(k == at)
        def _():
            for n in range(1, 8):
                up_copy(c, n).start()

    for h in range(H):
        if h == 2:
            push_x(0, 2)
        if h == 4:
            push_up(1, 0)
        if h == 5:
            push_x(0, 3)
        b = h % 2
        if h + 1 < H:
            ops = operands(h + 1)
        nxt = []
        tot = jnp.zeros((1, N), f32)
        for i in range(0, N, PIECE):
            if h + 1 < H:
                nxt.append(score(ops, h + 1, i))
            e = jnp.exp(st_s[b, i:i + PIECE, :] - peak)
            st_s[b, i:i + PIECE, :] = e
            tot = tot + jnp.sum(e, 0, keepdims=True)
        if h:
            blend(h - 1)
        inv = 1.0 / tot
        for i in range(0, N, PIECE):
            p_buf[half, h, i:i + PIECE, :] = (st_s[b, i:i + PIECE, :] * inv).astype(bf16)
        p_copy(k, h).start()
        if nxt:
            peak = functools.reduce(jnp.maximum, nxt)
    blend(H - 1)
    gated = (gt * o_ref[0]).astype(bf16)
    up = mm(wt[3], gated)
    after = (xin.T.astype(f32) + up).astype(bf16)
    a_ref[0] = after
    yhat, _ = norm(after.astype(f32), 0)
    yb = yhat.astype(bf16)
    live = livet[pl.ds(4 * d + k, 1), :]
    l_ref[0] = (mm(wl[...], yb) * live).astype(bf16)
    r_ref[0] = (mm(wr[...], yb) * live).astype(bf16)

    @pl.when(k == 3)
    def _():
        for n in range(1, 8):
            pd_copy(n).wait_recv()
            for c in range(2):
                up_copy(c, n).wait_recv()
        own_up.wait()
        own_pd.wait()
        later_up.wait()
        for h in range(H):
            p_copy(2, h).wait()
            p_copy(3, h).wait()
        for n in range(1, 8):
            live_copy(n).wait_send()
            pd_copy(n).wait_send()
            for c in range(2):
                up_copy(c, n).wait_send()
            for c in range(1, 4):
                x_copy(c, n).wait_send()
        for n in range(1, 16):
            row_copy(n).wait_send()


def bwd_kernel(x_ref, ua_in, ub_in, at_in, lg_ref, rg_ref, p_in, o_ref, g_ref, q_ref, v_ref, kt_ref, wq, wk, wv, wg, we, wl, wr,
               out_g, out_i, ua_ref, ub_ref, at_ref, p_buf, ds_s, acc_q, acc_v, acc_t, dt_s, sbuf, ss, rs, own, p_sem, in_sem):
    k = pl.program_id(0)
    d = lax.axis_index("dep")
    r = lax.axis_index("res")
    loads = [pltpu.make_async_copy(a, b, in_sem.at[n]) for n, (a, b) in
             enumerate(((at_in, at_ref), (ua_in, ua_ref), (ub_in, ub_ref)))]
    outs = (out_g, out_i)

    def dep_at(n):
        return lax.rem(d + n, 8)

    def send(which, c, n):
        return remote(sbuf.at[which, c, dep_at(n)], outs[which].at[d, c],
                      ss.at[which, c, n], rs.at[which, c, n], dep_at(n), r)

    def keep(which, c):
        return pltpu.make_async_copy(sbuf.at[which, c, d], outs[which].at[d, c], own.at[which, c])

    def ship(which, c, value):
        sbuf[which, c] = value.T.reshape(8, 64, F)
        for n in range(1, 8):
            send(which, c, n).start()
        keep(which, c).start()

    half = lax.rem(k, 2)

    def p_copy(at):
        return pltpu.make_async_copy(p_in.at[at], p_buf.at[lax.rem(at, 2)], p_sem.at[lax.rem(at, 2)])

    @pl.when(k == 0)
    def _():
        hail([(dep_at(n), r) for n in range(1, 8)])
        for load in loads:
            load.start()
        p_copy(0).start()
        p_copy(1).start()
        wlt, wrt = wl[...].T, wr[...].T
        gather_all(7)
        for load in loads:
            load.wait()
        for c in range(4):
            yhat, yinv = norm(at_ref[c].astype(f32), 0)
            dy = mm(wlt, lg_ref[c]) + mm(wrt, rg_ref[c])
            m1 = jnp.mean(dy, 0, keepdims=True)
            m2 = jnp.mean(dy * yhat, 0, keepdims=True)
            upt = (ua_ref if c < 2 else ub_ref)[:, c % 2].reshape(N, F).T.astype(f32)
            dt_s[c] = (yinv * (dy - m1 - yhat * m2) + upt).astype(bf16)
            ship(1, c, dt_s[c])

    p_copy(k).wait()
    xin = x_ref[...].reshape(N, F)
    q = q_ref[0]
    v = v_ref[0]
    kt = kt_ref[0]
    gt = g_ref[0]
    ot = o_ref[0]
    dt = dt_s[k]
    dg = mm(we[...], dt).astype(bf16).astype(f32)
    dot_ = (dg * gt).astype(bf16)
    dpre = (dg * ot * gt * (1.0 - gt)).astype(bf16)
    prod = dot_.astype(f32) * ot
    row = lax.broadcasted_iota(jnp.int32, (128, N), 0)
    col = lax.broadcasted_iota(jnp.int32, (N, 128), 1)
    ones = (col < 2).astype(f32).astype(bf16)
    lane = lax.broadcasted_iota(jnp.int32, (N, F), 1) // DH
    zero = jnp.zeros((), bf16)

    def back(h):
        sl = slice(DH * h, DH * h + DH)
        acc_q[sl, :] = mm(kt[sl], ds_s[h])

    def dops(h):
        grp = h // 4
        sl = slice(DH * h, DH * h + DH)
        dd = -jnp.sum(prod[sl], 0, keepdims=True)
        hi = dd.astype(bf16).astype(f32)
        lo = dd - hi
        extra = jnp.where(row == 0, hi, jnp.where(row == 1, lo, 0.0)).astype(bf16)
        return jnp.concatenate([v[:, 128 * grp:128 * grp + 128], ones], axis=1), spread(dot_[sl], h, extra)

    def wide_v(h):
        sl = slice(DH * h, DH * h + DH)
        acc_v[sl, :] = mmt(dot_[sl], p_buf[half, h])

    def tall_k(h, i):
        ext = mm(ds_s[h, i:i + 256, :], jnp.where(lane == h, q, zero))
        if h:
            acc_t[i:i + 256, :] += ext
        else:
            acc_t[i:i + 256, :] = ext

    for h in range(H):
        ops = dops(h)
        for i in range(0, N, 256):
            dp = mm(ops[0][i:i + 256], ops[1])
            ds_s[h, i:i + 256, :] = (p_buf[half, h, i:i + 256, :].astype(f32) * dp).astype(bf16)
            if h:
                tall_k(h - 1, i)
        wide_v(h)
        if h:
            back(h - 1)
    back(H - 1)
    for i in range(0, N, 256):
        tall_k(H - 1, i)
    dq = (acc_q[...].astype(bf16).astype(f32) * SCALE).astype(bf16)
    dx = (mm(wq[...], dq) + mm(wg[...], dpre)
          + mmt(wk[...], acc_t[...].astype(bf16)) + mm(wv[...], acc_v[...].astype(bf16)))
    dx = dx.astype(bf16).astype(f32)
    xt = xin.T.astype(f32)
    xh, inv = norm(xt, 0)
    m1 = jnp.mean(dx, 0, keepdims=True)
    m2 = jnp.mean(dx * xh, 0, keepdims=True)
    dln = (inv * (dx - m1 - xh * m2)).astype(bf16)
    out = (dt.astype(f32) + dln.astype(f32)).astype(bf16)
    ship(0, k, out)

    @pl.when(k < 2)
    def _():
        p_copy(k + 2).start()

    @pl.when(k == 3)
    def _():
        for which in range(2):
            for c in range(4):
                keep(which, c).wait()
                for n in range(1, 8):
                    send(which, c, n).wait_recv()
                    send(which, c, n).wait_send()


def whole(shape):
    return pl.BlockSpec(shape, lambda k: (0,) * len(shape))


def percol(shape):
    return pl.BlockSpec((1, *shape), lambda k: (k,) + (0,) * len(shape))


COLS = pl.BlockSpec((8, 1, 64, F), lambda k: (0, k, 0, 0))
ANY = pl.BlockSpec(memory_space=pl.ANY)


def fwd(msa, upstream, pair, live, wq, wk, wv, wg, we, wl, wr):
    sd = jax.ShapeDtypeStruct
    V = pltpu.VMEM
    dma = pltpu.SemaphoreType.DMA
    return pl.pallas_call(
        fwd_kernel,
        grid=(4,),
        in_specs=[whole((64, 32, F)), ANY, ANY, whole((CW, 64))] + [whole((F, F))] * 5 + [whole((CW, F))] * 2,
        out_specs=[COLS, ANY, percol((F, N)), percol((F, N)), percol((F, N)), percol((CW, N)),
                   percol((CW, N)), percol((N, F)), percol((N, F)), percol((F, N)), ANY, ANY, ANY, whole((8, 256)), whole((8, N))],
        out_shape=[sd((8, 4, 64, F), bf16), sd((4, H, N, N), bf16), sd((4, F, N), f32), sd((4, F, N), f32),
                   sd((4, F, N), bf16), sd((4, CW, N), bf16), sd((4, CW, N), bf16),
                   sd((4, N, F), bf16), sd((4, N, F), bf16), sd((4, F, N), bf16), sd((8, 2, 64, F), bf16), sd((8, 2, 64, F), bf16), sd((8, 2, 4, CW, CZ), bf16), sd((8, 256), f32), sd((8, N), f32)],
        scratch_shapes=[V((4, F, F), bf16), V((N, 128), bf16), V((2, N, N), f32), V((2, H, N, N), bf16), V((64, 128), bf16), V((64, 32, F), bf16), V((32, 64, CZ), bf16), V((8, 4, 64, F), bf16), V((8, 4, 64, F), bf16), V((2, 8, 4, CW, CZ), bf16), V((4, 8, 64, F), bf16),
                        V((8, 64, 128), bf16), V((128, N), f32), V((16, 8, N), f32), V((8, N), f32),
                        dma((4, 8)), dma((4, 8)), dma((4, 8)), dma((4, 8))] + [dma((8,))] * 4 + [dma((16,))] * 2 + [dma((8,)), dma((2, 8))],
        compiler_params=pltpu.CompilerParams(vmem_limit_bytes=60 * 1024 * 1024, collective_id=2, has_side_effects=True,
                                             dimension_semantics=("arbitrary",)),
        name="attention_forward",
    )(msa, upstream, pair, live, wq, wk, wv, wg, we, wl, wr)


def bwd(x, ua, ub, at, lg, rg, p, o, g, q, v, kt, wq, wk, wv, wg, we, wl, wr):
    sd = jax.ShapeDtypeStruct
    V = pltpu.VMEM
    dma = pltpu.SemaphoreType.DMA
    return pl.pallas_call(
        bwd_kernel,
        grid=(4,),
        in_specs=[COLS, ANY, ANY, ANY, whole((4, CW, N)), whole((4, CW, N)), ANY, percol((F, N)),
                  percol((F, N)), percol((N, F)), percol((N, F)), percol((F, N))] + [whole((F, F))] * 5 + [whole((CW, F))] * 2,
        out_specs=[ANY, ANY],
        out_shape=[sd((8, 4, 64, F), bf16)] * 2,
        scratch_shapes=[V((8, 2, 64, F), bf16), V((8, 2, 64, F), bf16), V((4, F, N), bf16), V((2, H, N, N), bf16), V((H, N, N), bf16), V((F, N), f32), V((F, N), f32), V((N, F), f32), V((4, F, N), bf16), V((2, 4, 8, 64, F), bf16),
                        dma((2, 4, 8)), dma((2, 4, 8)), dma((2, 4)), dma((2,)), dma((3,))],
        compiler_params=pltpu.CompilerParams(vmem_limit_bytes=60 * 1024 * 1024, collective_id=3, has_side_effects=True,
                                             dimension_semantics=("arbitrary",)),
        name="attention_backward",
    )(x, ua, ub, at, lg, rg, p, o, g, q, v, kt, wq, wk, wv, wg, we, wl, wr)


def opm_kernel(lt, rt, pd, rc, wo, live, ux, lo, ro, up,
               perm, oc1, oc2, lbuf, rbuf, lsend, lrecv, psend, precv, rsend, rrecv, both, lkeep, lacc,
               ls, lr, rs, rr, fs, fr, ps, pr, s2, r2, s3, r3, us, ur, own):
    d = lax.axis_index("dep")
    r = lax.axis_index("res")
    xl, z = d // 4, lax.rem(d, 4)
    y, xh, core = r // 4, lax.rem(r // 2, 2), lax.rem(r, 2)

    def dep_of(flip, step):
        return 4 * lax.rem(xl + flip, 2) + lax.rem(z + step + 4, 4)

    def chip_of(flip, step):
        return 2 * lax.rem(y + step + 4, 4) + lax.rem(xh + flip, 2)

    def res_of(flip, step):
        return 2 * chip_of(flip, step) + core

    partner = 2 * chip_of(0, 0) + 1 - core
    greet([(lax.rem(d + n, 8), r) for n in range(1, 8)]
          + [(d, res_of(0, n)) for n in range(1, 4)] + [(d, res_of(1, 0)), (d, partner)])

    def left_copy(n):
        if n == 0:
            return remote(lt, lbuf.at[d], ls.at[0], lr.at[0], dep_of(1, 0), r)
        if n < 4:
            return remote(lt, lbuf.at[d], ls.at[n], lr.at[n], dep_of(0, n), r)
        slot = dep_of(1, 0)
        return remote(lbuf.at[slot], lbuf.at[slot], ls.at[n], lr.at[n], dep_of(0, n - 3), r)

    def right_copy(n):
        if n == 0:
            return remote(rt, rbuf.at[r], rs.at[0], rr.at[0], d, res_of(1, 0))
        if n < 4:
            return remote(rt, rbuf.at[r], rs.at[n], rr.at[n], d, res_of(0, n))
        slot = res_of(1, 0)
        return remote(rbuf.at[slot], rbuf.at[slot], rs.at[n], rr.at[n], d, res_of(0, n - 3))

    def across(n):
        if n == 7:
            return remote(rt, rbuf.at[r], fs.at[7], fr.at[7], d, partner)
        slot = res_of(1, 0) if n == 0 else res_of(0, -n) if n < 4 else res_of(1, 3 - n)
        return remote(rbuf.at[slot], rbuf.at[slot], fs.at[n], fr.at[n], d, partner)

    def up_copy(n):
        dep = lax.rem(d + n, 8)
        return remote(ux.at[dep], up.at[d], us.at[n], ur.at[n], dep, r)

    own_up = pltpu.make_async_copy(ux.at[d], up.at[d], own)
    own_up.start()
    for n in range(4):
        left_copy(n).start()
        right_copy(n).start()
    across(7).start()
    lbuf[d] = lt[...]
    rbuf[r] = rt[...]

    a = lax.broadcasted_iota(jnp.int32, (1024, 1024), 0)
    b = lax.broadcasted_iota(jnp.int32, (1024, 1024), 1)
    hit = ((a // CW) == (b % CW)) & ((a % CW) == (b // CW))
    perm[...] = hit.astype(f32).astype(bf16)

    def outer_step(n, carry):
        at = pl.multiple_of(256 * n, 256)
        zz = (mmt(wo[...], pd[pl.ds(at, 256), :]) * rc[pl.ds(n, 1), :]).astype(bf16)
        rows = []
        for j in range(8):
            rows.append(jnp.concatenate([zz[CW * c:CW * c + CW, CW * j:CW * j + CW] for c in range(CW)], axis=1))
        yy = mm(jnp.concatenate(rows, axis=0), perm[...]).astype(bf16)
        oc1[pl.ds(at, 256), :] = yy
        oc2[:, pl.ds(at, 256)] = yy.T

        @pl.when(n == 1)
        def _():
            left_copy(0).wait_recv()
            for i in range(4, 7):
                left_copy(i).start()

        @pl.when(n == 2)
        def _():
            right_copy(0).wait_recv()
            for i in range(4, 7):
                right_copy(i).start()
            across(0).start()

        @pl.when(n == 5)
        def _():
            for i in range(1, 4):
                right_copy(i).wait_recv()
                across(i).start()
        return carry

    lax.fori_loop(0, 8, outer_step, 0)
    for n in range(1, 7):
        left_copy(n).wait_recv()
    for n in range(1, 8):
        up_copy(n).start()
    for n in range(4, 7):
        right_copy(n).wait_recv()
        across(n).start()

    order = [(1, 1), (1, 2), (1, 3), (1, 0), (0, 1), (0, 2), (0, 3), (0, 0)]

    def pass_over(i):
        return remote(psend.at[i], precv.at[i], ps.at[i], pr.at[i], d, partner)

    def right_part(i):
        target = res_of(1, 0) if i == 3 else res_of(0, order[i][1])
        return remote(rsend.at[i], rrecv.at[i], s2.at[i], r2.at[i], d, target)

    def left_part(i):
        target = dep_of(1, 0) if i == 3 else dep_of(0, order[i][1])
        return remote(lsend.at[i], lrecv.at[i], s3.at[i], r3.at[i], target, r)

    mine = pl.ds(pl.multiple_of(128 * core, 128), 128)
    theirs = pl.ds(pl.multiple_of(128 * (1 - core), 128), 128)
    def right_mm(i):
        at = pl.multiple_of(256 * chip_of(*order[i]), 256)
        both[i] = mm(oc1[pl.ds(at, 256), :], lbuf[...].reshape(1024, N))
        psend[i] = both[i, theirs, :].astype(bf16)
        pass_over(i).start()

    def right_send(i):
        pass_over(i).wait_recv()
        own = both[i, mine, :] + precv[i].astype(f32)
        if i in (3, 7):
            both[i, mine, :] = own
        else:
            rsend[i] = own.astype(bf16)
            right_part(i).start()

    def left_mm(i):
        at = pl.multiple_of(128 * dep_of(*order[i]), 128)
        own = mm(oc2[pl.ds(at, 128), :], rbuf[...].reshape(2048, N))
        if i == 3:
            lkeep[...] = own
        elif i == 7:
            lacc[...] = own
        else:
            lsend[i] = own.astype(bf16)
            left_part(i).start()

    for grp in (range(4), range(4, 8)):
        for i in grp:
            right_mm(i)
        if grp[0] == 0:
            for n in range(8):
                across(n).wait_recv()
        for i in grp:
            left_mm(i)
        for i in grp:
            right_send(i)
    for i in range(3):
        right_part(i).wait_recv()
    rsend[3] = (both[3, mine, :] + jnp.sum(rrecv[0:3].astype(f32), 0)).astype(bf16)
    right_part(3).start()
    for i in range(3):
        left_part(i).wait_recv()
    lsend[3] = (lkeep[...] + jnp.sum(lrecv[0:3].astype(f32), 0)).astype(bf16)
    left_part(3).start()
    for i in range(3, 7):
        right_part(i).wait_recv()
    racc = both[7, mine, :] + jnp.sum(rrecv[3:7].astype(f32), 0)
    for n in range(4):
        ro[n] = (racc[CW * n:CW * n + CW, :] * live[n:n + 1, :]).astype(bf16)
    for i in range(3, 7):
        left_part(i).wait_recv()
    lsum = lacc[...] + jnp.sum(lrecv[3:7].astype(f32), 0)
    for n in range(4):
        lo[n] = (lsum[CW * n:CW * n + CW, :] * live[n:n + 1, :]).astype(bf16)
    own_up.wait()
    for n in range(1, 8):
        up_copy(n).wait_recv()
        up_copy(n).wait_send()
    for n in range(7):
        left_copy(n).wait_send()
        right_copy(n).wait_send()
        right_part(n).wait_send()
        left_part(n).wait_send()
    for n in range(8):
        across(n).wait_send()
        pass_over(n).wait_send()


def opm(lt, rt, pd, rc, wo, live, ux):
    sd = jax.ShapeDtypeStruct
    vm = pl.BlockSpec(memory_space=pltpu.VMEM)
    chunk = (128, N)
    V = pltpu.VMEM
    dma = pltpu.SemaphoreType.DMA((8,))
    return pl.pallas_call(
        opm_kernel,
        in_specs=[vm] * 6 + [ANY],
        out_specs=[vm] * 3,
        out_shape=[sd((4, CW, N), bf16)] * 2 + [sd((8, 2, 64, F), bf16)],
        scratch_shapes=[V((1024, 1024), bf16), V((2048, 1024), bf16), V((1024, 2048), bf16),
                        V((8, *chunk), bf16), V((16, *chunk), bf16)] + [V((8, *chunk), bf16)] * 6
        + [V((8, 256, N), f32)] + [V(chunk, f32)] * 2 + [dma] * 14 + [pltpu.SemaphoreType.DMA],
        compiler_params=pltpu.CompilerParams(vmem_limit_bytes=60 * 1024 * 1024, collective_id=1, has_side_effects=True),
        name="outer_product",
    )(lt, rt, pd, rc, wo, live, ux)


def on_device(msa, present, pair, upstream, wq, wk, wv, wg, we, wl, wr, wo):
    def by_row(a):
        return a.reshape(32, 64, F).transpose(1, 0, 2)

    x, p, o, g, at, lt, rt, q, v, kt, ua, ut, pd, recip, livet = fwd(
        msa, upstream, pair, present.T, wq, wk, wv, wg, we, wl.T, wr.T)
    lg, rg, ub = opm(lt.reshape(4 * CW, N), rt.reshape(4 * CW, N), pd.reshape(-1, CZ), recip, wo, livet, ut)
    grad, inter = bwd(x, ua, ub, at, lg, rg, p, o, g, q, v, kt, wq, wk, wv, wg, we, wl.T, wr.T)
    return by_row(grad), by_row(inter)


def solution(mesh):
    rows = P("dep", "res", None)
    in_specs = (rows, P("dep", "res"), P("res", "dep", None), rows) + (P(),) * 8
    return jax.shard_map(on_device, mesh=mesh, in_specs=in_specs, out_specs=(rows, rows), check_vma=False)
```
